512 devices in a mesh: gx: 8 (over x, core), gy: 64 (over y, z).
Axes of the slice: x: 4, y: 8, z: 8, core: 2. Of those that a mesh axis runs over, the one named last changes fastest.
Arguments:
- trial: float32 [786432, 384], P(('gx', 'gy')), may hold values from -30 to 30
- resid: float32 [786432, 128], P(('gx', 'gy')), may hold values from -500 to 500
- energy: float32 [786432], P(('gx', 'gy')), may hold values from 1 to 10
- shift: float32 [128], replicated, may hold values from 0.05 to 0.5
Outputs:
- basis: float32 [786432, 128], P(('gx', 'gy'))
The draws below stay inside these ranges and needn't reach their ends.
All inputs are finite; a program needn't handle non-finite values.
Results may differ from the reference program's by a relative error of at most 0.0003.
Values sent between devices are 32-bit elements; how exact they have to be, the bound alone decides.
A program may use at most 64 MiB of HBM per device.

```python
import math
import jax
import jax.numpy as jnp
from jax import lax

KEEP = 384
NEW = 128
NPAIR = 786432


side_share = 0.01


def base_noise(key, label, height, breadth):
    subkey = jax.random.fold_in(jax.random.fold_in(key, 5101), label)
    return jax.random.truncated_normal(subkey, -5.0, 5.0, (height, breadth), jnp.float32)


def row_scale():
    place = jnp.arange(NPAIR, dtype=jnp.float32) / (NPAIR - 1)
    return jnp.exp(place * math.log(3.0))[:, None]


def energies(key):
    subkey = jax.random.fold_in(jax.random.fold_in(key, 5101), 11)
    level = jax.random.uniform(subkey, (NPAIR,), jnp.float32, 0.0, 1.0)
    return jnp.exp(level * math.log(9.99))


def shifts(key):
    subkey = jax.random.fold_in(jax.random.fold_in(key, 5101), 12)
    return jax.random.uniform(subkey, (NEW,), jnp.float32, 0.05, 0.5)


def draw_trial(key, part):
    return base_noise(key, 1, NPAIR, KEEP) * row_scale()


def draw_energy(key, part):
    return energies(key)


def draw_shift(key, part):
    return shifts(key)


def draw_resid(key, part):
    stored = base_noise(key, 1, NPAIR, KEEP)
    mixkey = jax.random.fold_in(jax.random.fold_in(key, 5101), 2)
    mixing = jax.random.truncated_normal(mixkey, -5.0, 5.0, (KEEP, NEW), jnp.float32) / math.sqrt(KEEP)
    owned = base_noise(key, 5, NPAIR, NEW)
    inside = jnp.dot(stored, mixing, precision=lax.Precision.HIGHEST, preferred_element_type=jnp.float32)
    target = jnp.clip(inside, -7.9, 7.9) + side_share * owned
    target = target * row_scale()
    return target * (energies(key)[:, None] - shifts(key)[None, :])


def setup_inputs(seed: int = 0) -> dict:
    key_list = jax.random.split(jax.random.key(seed), 5)
    return {
        "trial": draw_trial(jax.random.fold_in(key_list[4], 71), 0),
        "resid": draw_resid(jax.random.fold_in(key_list[4], 71), 0),
        "energy": draw_energy(jax.random.fold_in(key_list[4], 71), 0),
        "shift": draw_shift(jax.random.fold_in(key_list[4], 71), 0),
    }


def fdot(left, right):
    return jnp.dot(left.astype(jnp.float32), right.astype(jnp.float32), precision=lax.Precision.HIGHEST, preferred_element_type=jnp.float32)

def reference(trial, resid, energy, shift):
    count = trial.shape[0]
    work = resid / (energy[:, None] - shift[None, :])
    for sweep in range(2):
        coef = fdot(trial.T, work) / count
        work = work - fdot(trial, coef)
    gram = fdot(work.T, work) / count
    lower = jnp.linalg.cholesky(gram)
    return jax.scipy.linalg.solve_triangular(lower, work.T, lower=True).T
```

```python
import jax
import jax.numpy as jnp
from jax import lax
from jax.experimental import pallas as pl
from jax.experimental.pallas import tpu as pltpu
from jax.sharding import Mesh
from jax.sharding import PartitionSpec as P

MESH = pl.DeviceIdType.MESH
AXES = ("x", "core", "y", "z")
ROWS, KEEP, NEW = 1536, 384, 128
UNIT = 4
PAIRS = [(i, j) for i in range(4) for j in range(i, 4)]
HALF = len(PAIRS) * 128 // UNIT // 2
PLANE, LINE = 32, 8
CHUNK = HALF // PLANE
F32, BF16 = jnp.float32, jnp.bfloat16


def tdot(a, b):
    return lax.dot_general(a, b, (((0,), (0,)), ((), ())), preferred_element_type=F32)


def gram_kernel(
    trial_ref, resid_ref, energy_ref, shift_ref, total_ref, corr_ref,
    hi, lo, part, peer, held, own, line, done,
    core_sems, plane_sems, line_sems, gather_sems, spread_sems, last_sems,
):
    x, c = lax.axis_index("x"), lax.axis_index("core")
    y, z = lax.axis_index("y"), lax.axis_index("z")
    p = (1 - c) * y + c * z
    q = (1 - c) * z + c * y
    me = x * 8 + p
    other = {"x": x, "core": 1 - c, "y": y, "z": z}

    def in_plane(k):
        a, b = k // 8, k % 8
        return {"x": a, "core": c, "y": (1 - c) * b + c * y, "z": (1 - c) * z + c * b}

    def in_line(b):
        return {"x": x, "core": c, "y": (1 - c) * y + c * b, "z": (1 - c) * b + c * z}

    barrier = pltpu.get_barrier_semaphore()

    def greet_plane(j, _):
        pl.semaphore_signal(barrier, inc=1, device_id=in_plane((me + j) % PLANE), device_id_type=MESH)
        return _

    def greet_line(j, _):
        pl.semaphore_signal(barrier, inc=1, device_id=in_line((q + j) % LINE), device_id_type=MESH)
        return _

    pl.semaphore_signal(barrier, inc=1, device_id=other, device_id_type=MESH)
    lax.fori_loop(1, PLANE, greet_plane, 0)
    lax.fori_loop(1, LINE, greet_line, 0)

    shift = shift_ref[...]
    for b in range(ROWS // 128):
        rows = pl.ds(b * 128, 128)
        gap = jnp.broadcast_to(energy_ref[pl.ds(b, 1), :], (128, 128)).T - shift
        corr = resid_ref[rows, :] / gap
        corr_ref[rows, :] = corr
        trial = trial_ref[rows, :]
        high = trial.astype(BF16)
        hi[rows, :KEEP] = high
        lo[rows, :KEEP] = (trial - high.astype(F32)).astype(BF16)
        high = corr.astype(BF16)
        hi[rows, KEEP:] = high
        lo[rows, KEEP:] = (corr - high.astype(F32)).astype(BF16)

    cross = {}
    for i in range(2):
        left = hi[:, i * 256:(i + 1) * 256]
        for j in range(2):
            cross[i, j] = tdot(left, lo[:, j * 256:(j + 1) * 256])
    for i in range(2):
        left = hi[:, i * 256:(i + 1) * 256]
        for j in range(i, 2):
            full = tdot(left, hi[:, j * 256:(j + 1) * 256]) + cross[i, j] + cross[j, i].T
            for n, (s, t) in enumerate(PAIRS):
                if s // 2 == i and t // 2 == j:
                    block = full[s % 2 * 128:s % 2 * 128 + 128, t % 2 * 128:t % 2 * 128 + 128]
                    part[n * 32:(n + 1) * 32] = block.reshape(32, UNIT, 128)

    pl.semaphore_wait(barrier, PLANE + LINE - 1)

    def remote(src, dst, sems, device):
        return pltpu.make_async_remote_copy(
            src_ref=src, dst_ref=dst, send_sem=sems.at[0], recv_sem=sems.at[1],
            device_id=device, device_id_type=MESH,
        )

    mine, theirs = c * HALF, (1 - c) * HALF
    swap = remote(part.at[pl.ds(theirs, HALF)], peer, core_sems, other)
    swap.start()
    swap.wait_recv()
    peer[...] += part[pl.ds(mine, HALF)]

    def scatter(j, _):
        k = (me + j) % PLANE
        remote(
            peer.at[pl.ds(k * CHUNK, CHUNK)], held.at[pl.ds((j - 1) * CHUNK, CHUNK)], plane_sems, in_plane(k)
        ).start()
        return _

    lax.fori_loop(1, PLANE, scatter, 0)
    arrived = remote(held, held, plane_sems, other)
    arrived.wait_recv()
    total = peer[pl.ds(me * CHUNK, CHUNK)]
    for j in range(PLANE - 1):
        total += held[j * CHUNK:(j + 1) * CHUNK]
    own[...] = total
    line[pl.ds(q * CHUNK, CHUNK)] = total

    def exchange(j, _):
        remote(own, line.at[pl.ds(q * CHUNK, CHUNK)], line_sems, in_line((q + j) % LINE)).start()
        return _

    lax.fori_loop(1, LINE, exchange, 0)
    lines = line.at[pl.ds(0, (LINE - 1) * CHUNK)]
    remote(lines, lines, line_sems, other).wait_recv()
    total = line[0:CHUNK]
    for j in range(1, LINE):
        total += line[j * CHUNK:(j + 1) * CHUNK]
    done[...] = total
    total_ref[pl.ds(mine + me * CHUNK, CHUNK)] = total

    def chunk_of(k):
        return total_ref.at[pl.ds(mine + k * CHUNK, CHUNK)]

    def spread(j, _):
        k = (me + j) % PLANE
        pltpu.make_async_remote_copy(
            src_ref=done, dst_ref=chunk_of(me), send_sem=gather_sems.at[0], recv_sem=spread_sems.at[me],
            device_id=in_plane(k), device_id_type=MESH,
        ).start()
        return _

    lax.fori_loop(1, PLANE, spread, 0)
    remote(done, chunk_of(me), last_sems, other).start()

    def forward(j, _):
        k = (me + j) % PLANE
        pltpu.make_async_remote_copy(
            src_ref=done, dst_ref=chunk_of(k), send_sem=gather_sems.at[0], recv_sem=spread_sems.at[k],
            device_id=other, device_id_type=MESH,
        ).wait_recv()
        remote(chunk_of(k), chunk_of(k), last_sems, other).start()
        return _

    lax.fori_loop(1, PLANE, forward, 0)
    whole = total_ref.at[pl.ds(theirs, HALF)]
    remote(whole, whole, last_sems, other).wait_recv()

    swap.wait_send()
    arrived.wait_send()
    remote(lines, lines, line_sems, other).wait_send()
    remote(held, held, gather_sems, other).wait_send()
    remote(whole, whole, last_sems, other).wait_send()


def gram(trial, resid, energy, shift):
    vmem = pl.BlockSpec(memory_space=pltpu.VMEM)
    return pl.pallas_call(
        gram_kernel,
        out_shape=(
            jax.ShapeDtypeStruct((2 * HALF, UNIT, 128), F32),
            jax.ShapeDtypeStruct((ROWS, NEW), F32),
        ),
        in_specs=[vmem] * 4,
        out_specs=(vmem, vmem),
        scratch_shapes=[
            pltpu.VMEM((ROWS, KEEP + NEW), BF16),
            pltpu.VMEM((ROWS, KEEP + NEW), BF16),
            pltpu.VMEM((2 * HALF, UNIT, 128), F32),
            pltpu.VMEM((HALF, UNIT, 128), F32),
            pltpu.VMEM(((PLANE - 1) * CHUNK, UNIT, 128), F32),
            pltpu.VMEM((CHUNK, UNIT, 128), F32),
            pltpu.VMEM((LINE * CHUNK, UNIT, 128), F32),
            pltpu.VMEM((CHUNK, UNIT, 128), F32),
            pltpu.SemaphoreType.DMA((2,)),
            pltpu.SemaphoreType.DMA((2,)),
            pltpu.SemaphoreType.DMA((2,)),
            pltpu.SemaphoreType.DMA((2,)),
            pltpu.SemaphoreType.DMA((PLANE,)),
            pltpu.SemaphoreType.DMA((2,)),
        ],
        compiler_params=pltpu.CompilerParams(collective_id=0, has_side_effects=True),
        name="gram",
    )(trial, resid, energy.reshape(ROWS // 128, 128), shift.reshape(1, NEW))


def fdot(left, right):
    return jnp.dot(left, right, precision=lax.Precision.HIGHEST, preferred_element_type=F32)


def explicit(trial, resid, energy, shift, raw_first, raw_metric, count):
    corr = resid / (energy[:, None] - shift[None, :])
    def total(v):
        return lax.psum(v, AXES)
    work = corr
    for sweep in range(2):
        work = work - fdot(trial, total(fdot(trial.T, work)) / count)
    gram_two = total(fdot(work.T, work)) / count
    lower = jnp.linalg.cholesky(gram_two)
    return jax.scipy.linalg.solve_triangular(lower, work.T, lower=True).T


def per_device(trial, resid, energy, shift):
    count = ROWS * 512
    total, corr = gram(trial, resid, energy, shift)
    blocks = total.reshape(len(PAIRS), 128, 128) / count
    at = {pair: blocks[n] for n, pair in enumerate(PAIRS)}
    metric = jnp.concatenate(
        [jnp.concatenate([at[i, j] if i <= j else at[j, i].T for j in range(3)], 1) for i in range(3)], 0
    )
    first = jnp.concatenate([at[i, 3] for i in range(3)], 0)
    coef = 2 * first - fdot(metric, first)
    cross = fdot(coef.T, first)
    inner = fdot(coef.T, fdot(metric, coef))
    gram_one = at[3, 3] - cross - cross.T + inner
    terms = jnp.diagonal(at[3, 3]) + 2 * jnp.abs(jnp.diagonal(cross)) + jnp.diagonal(inner)
    steady = jnp.all(terms <= 16 * jnp.diagonal(gram_one))

    def fast():
        lower = jnp.linalg.cholesky(gram_one)
        inverse = jax.scipy.linalg.solve_triangular(lower, jnp.eye(NEW, dtype=F32), lower=True)
        return fdot(corr, inverse.T) - fdot(trial, fdot(coef, inverse.T))

    def slow():
        return explicit(trial, resid, energy, shift, None, None, count)

    return lax.cond(steady, fast, slow)


def solution(mesh):
    split = Mesh(mesh.devices.reshape(4, 2, 8, 8), AXES)
    in_specs = (P(AXES, None), P(AXES, None), P(AXES), P())
    return jax.shard_map(
        per_device, mesh=split, in_specs=in_specs, out_specs=P(AXES, None), check_vma=False
    )
```

```python
import jax
import jax.numpy as jnp
from jax import lax
from jax.experimental import pallas as pl
from jax.experimental.pallas import tpu as pltpu
from jax.sharding import Mesh
from jax.sharding import PartitionSpec as P

MESH = pl.DeviceIdType.MESH
AXES = ("x", "core", "y", "z")
ROWS, KEEP, NEW = 1536, 384, 128
UNIT = 4
PAIRS = [(i, j) for i in range(4) for j in range(i, 4)]
HALF = len(PAIRS) * 128 // UNIT // 2
PLANE, LINE = 32, 8
CHUNK = HALF // PLANE
F32, BF16 = jnp.float32, jnp.bfloat16


def tdot(a, b):
    return lax.dot_general(a, b, (((0,), (0,)), ((), ())), preferred_element_type=F32)


def gram_kernel(
    trial_ref, resid_ref, energy_ref, shift_ref, total_ref, high_ref, low_ref,
    hi, lo, part, peer, held, own, line, done,
    core_sems, plane_sems, line_sems, gather_sems, spread_sems, last_sems, keep_sems,
):
    x, c = lax.axis_index("x"), lax.axis_index("core")
    y, z = lax.axis_index("y"), lax.axis_index("z")
    p = (1 - c) * y + c * z
    q = (1 - c) * z + c * y
    me = x * 8 + p
    other = {"x": x, "core": 1 - c, "y": y, "z": z}

    def in_plane(k):
        a, b = k // 8, k % 8
        return {"x": a, "core": c, "y": (1 - c) * b + c * y, "z": (1 - c) * z + c * b}

    def in_line(b):
        return {"x": x, "core": c, "y": (1 - c) * y + c * b, "z": (1 - c) * b + c * z}

    barrier = pltpu.get_barrier_semaphore()

    def greet_plane(j, _):
        pl.semaphore_signal(barrier, inc=1, device_id=in_plane((me + j) % PLANE), device_id_type=MESH)
        return _

    def greet_line(j, _):
        pl.semaphore_signal(barrier, inc=1, device_id=in_line((q + j) % LINE), device_id_type=MESH)
        return _

    pl.semaphore_signal(barrier, inc=1, device_id=other, device_id_type=MESH)
    lax.fori_loop(1, PLANE, greet_plane, 0)
    lax.fori_loop(1, LINE, greet_line, 0)

    shift = shift_ref[...]
    for b in range(ROWS // 128):
        rows = pl.ds(b * 128, 128)
        gap = jnp.broadcast_to(energy_ref[pl.ds(b, 1), :], (128, 128)).T - shift
        corr = resid_ref[rows, :] / gap
        trial = trial_ref[rows, :]
        high = trial.astype(BF16)
        hi[rows, :KEEP] = high
        lo[rows, :KEEP] = (trial - high.astype(F32)).astype(BF16)
        high = corr.astype(BF16)
        hi[rows, KEEP:] = high
        lo[rows, KEEP:] = (corr - high.astype(F32)).astype(BF16)

    keep = [
        pltpu.make_async_copy(hi, high_ref, keep_sems.at[0]),
        pltpu.make_async_copy(lo, low_ref, keep_sems.at[1]),
    ]
    for copy in keep:
        copy.start()

    cross = {}
    for i in range(2):
        left = hi[:, i * 256:(i + 1) * 256]
        for j in range(2):
            cross[i, j] = tdot(left, lo[:, j * 256:(j + 1) * 256])
    for i in range(2):
        left = hi[:, i * 256:(i + 1) * 256]
        for j in range(i, 2):
            full = tdot(left, hi[:, j * 256:(j + 1) * 256]) + cross[i, j] + cross[j, i].T
            for n, (s, t) in enumerate(PAIRS):
                if s // 2 == i and t // 2 == j:
                    block = full[s % 2 * 128:s % 2 * 128 + 128, t % 2 * 128:t % 2 * 128 + 128]
                    part[n * 32:(n + 1) * 32] = block.reshape(32, UNIT, 128)

    pl.semaphore_wait(barrier, PLANE + LINE - 1)

    def remote(src, dst, sems, device):
        return pltpu.make_async_remote_copy(
            src_ref=src, dst_ref=dst, send_sem=sems.at[0], recv_sem=sems.at[1],
            device_id=device, device_id_type=MESH,
        )

    mine, theirs = c * HALF, (1 - c) * HALF
    swap = remote(part.at[pl.ds(theirs, HALF)], peer, core_sems, other)
    swap.start()
    swap.wait_recv()
    peer[...] += part[pl.ds(mine, HALF)]

    def scatter(j, _):
        k = (me + j) % PLANE
        remote(
            peer.at[pl.ds(k * CHUNK, CHUNK)], held.at[pl.ds((j - 1) * CHUNK, CHUNK)], plane_sems, in_plane(k)
        ).start()
        return _

    lax.fori_loop(1, PLANE, scatter, 0)
    arrived = remote(held, held, plane_sems, other)
    arrived.wait_recv()
    total = peer[pl.ds(me * CHUNK, CHUNK)]
    for j in range(PLANE - 1):
        total += held[j * CHUNK:(j + 1) * CHUNK]
    own[...] = total
    line[pl.ds(q * CHUNK, CHUNK)] = total

    def exchange(j, _):
        remote(own, line.at[pl.ds(q * CHUNK, CHUNK)], line_sems, in_line((q + j) % LINE)).start()
        return _

    lax.fori_loop(1, LINE, exchange, 0)
    lines = line.at[pl.ds(0, (LINE - 1) * CHUNK)]
    remote(lines, lines, line_sems, other).wait_recv()
    total = line[0:CHUNK]
    for j in range(1, LINE):
        total += line[j * CHUNK:(j + 1) * CHUNK]
    done[...] = total
    total_ref[pl.ds(mine + me * CHUNK, CHUNK)] = total

    def chunk_of(k):
        return total_ref.at[pl.ds(mine + k * CHUNK, CHUNK)]

    def spread(j, _):
        k = (me + j) % PLANE
        pltpu.make_async_remote_copy(
            src_ref=done, dst_ref=chunk_of(me), send_sem=gather_sems.at[0], recv_sem=spread_sems.at[me],
            device_id=in_plane(k), device_id_type=MESH,
        ).start()
        return _

    lax.fori_loop(1, PLANE, spread, 0)
    remote(done, chunk_of(me), last_sems, other).start()

    def forward(j, _):
        k = (me + j) % PLANE
        pltpu.make_async_remote_copy(
            src_ref=done, dst_ref=chunk_of(k), send_sem=gather_sems.at[0], recv_sem=spread_sems.at[k],
            device_id=other, device_id_type=MESH,
        ).wait_recv()
        remote(chunk_of(k), chunk_of(k), last_sems, other).start()
        return _

    lax.fori_loop(1, PLANE, forward, 0)
    whole = total_ref.at[pl.ds(theirs, HALF)]
    remote(whole, whole, last_sems, other).wait_recv()

    for copy in keep:
        copy.wait()
    swap.wait_send()
    arrived.wait_send()
    remote(lines, lines, line_sems, other).wait_send()
    remote(held, held, gather_sems, other).wait_send()
    remote(whole, whole, last_sems, other).wait_send()


def gram(trial, resid, energy, shift):
    vmem = pl.BlockSpec(memory_space=pltpu.VMEM)
    hbm = pl.BlockSpec(memory_space=pl.ANY)
    return pl.pallas_call(
        gram_kernel,
        out_shape=(
            jax.ShapeDtypeStruct((2 * HALF, UNIT, 128), F32),
            jax.ShapeDtypeStruct((ROWS, KEEP + NEW), BF16),
            jax.ShapeDtypeStruct((ROWS, KEEP + NEW), BF16),
        ),
        in_specs=[vmem] * 4,
        out_specs=(vmem, hbm, hbm),
        scratch_shapes=[
            pltpu.VMEM((ROWS, KEEP + NEW), BF16),
            pltpu.VMEM((ROWS, KEEP + NEW), BF16),
            pltpu.VMEM((2 * HALF, UNIT, 128), F32),
            pltpu.VMEM((HALF, UNIT, 128), F32),
            pltpu.VMEM(((PLANE - 1) * CHUNK, UNIT, 128), F32),
            pltpu.VMEM((CHUNK, UNIT, 128), F32),
            pltpu.VMEM((LINE * CHUNK, UNIT, 128), F32),
            pltpu.VMEM((CHUNK, UNIT, 128), F32),
            pltpu.SemaphoreType.DMA((2,)),
            pltpu.SemaphoreType.DMA((2,)),
            pltpu.SemaphoreType.DMA((2,)),
            pltpu.SemaphoreType.DMA((2,)),
            pltpu.SemaphoreType.DMA((PLANE,)),
            pltpu.SemaphoreType.DMA((2,)),
            pltpu.SemaphoreType.DMA((2,)),
        ],
        compiler_params=pltpu.CompilerParams(collective_id=0, has_side_effects=True),
        name="gram",
    )(trial, resid, energy.reshape(ROWS // 128, 128), shift.reshape(1, NEW))


SIDE = 32


def mul(left, right, dims):
    return lax.dot_general(
        left, right, ((dims[:1], dims[1:]), ((), ())), precision=lax.Precision.HIGHEST, preferred_element_type=F32
    )


def inverse_factor(square, lane, row):
    tiles = SIDE // 8
    sub = row[:8]
    panels = []
    rest = square
    for base in range(0, NEW, SIDE):
        here = (lane >= base) & (lane < base + SIDE)
        top = rest[:SIDE]
        cols = [
            [jnp.broadcast_to(top[t * 8:t * 8 + 8, base + j:base + j + 1], (8, 128)) if t >= j // 8 else None
             for t in range(tiles)]
            for j in range(SIDE)
        ]
        unit = jnp.where(lane[:SIDE] == row[:SIDE] + base, 1.0, 0.0)
        panel = jnp.where(here[:SIDE], unit, top)
        panel = [panel[t * 8:t * 8 + 8] for t in range(tiles)]
        for k in range(SIDE):
            tk, sk = k // 8, k % 8
            pivot = jnp.broadcast_to(cols[k][tk][sk:sk + 1], (8, 128))
            scale = lax.rsqrt(pivot)
            if k + 1 < SIDE:
                tn, sn = (k + 1) // 8, (k + 1) % 8
                line = jnp.broadcast_to(cols[k][tn][sn:sn + 1], (8, 128))
                ratio = scale * scale
                for t in range(tn, tiles):
                    cols[k + 1][t] = cols[k + 1][t] - (cols[k][t] * line) * ratio
            for t in range(tk, tiles):
                cols[k][t] = cols[k][t] * scale
            line = jnp.broadcast_to(panel[tk][sk:sk + 1], (8, 128)) * scale
            panel[tk] = jnp.where(
                sub == sk, line, panel[tk] - jnp.where(sub > sk, cols[k][tk], 0.0) * line
            )
            for t in range(tk + 1, tiles):
                panel[t] = panel[t] - cols[k][t] * line
            for j in range(k + 2, SIDE):
                line = jnp.broadcast_to(cols[k][j // 8][j % 8:j % 8 + 1], (8, 128))
                for t in range(j // 8, tiles):
                    cols[j][t] = cols[j][t] - cols[k][t] * line
        done = jnp.concatenate(panel, 0)
        panels.append(done)
        if base + SIDE < NEW:
            left = rest.shape[0] - SIDE
            below = jnp.where(here[:left], 0.0, rest[SIDE:])
            rest = below - mul(done, done, (0, 0))[base + SIDE:]
    whole = jnp.concatenate(panels, 0)
    return jnp.where(lane <= row, whole, 0.0)


def finish_kernel(count, total_ref, high_ref, low_ref, basis_ref, steady_ref, high, low, sems):
    fetch = [
        pltpu.make_async_copy(high_ref, high, sems.at[0]),
        pltpu.make_async_copy(low_ref, low, sems.at[1]),
    ]
    for copy in fetch:
        copy.start()
    at = {
        pair: total_ref[n * 32:(n + 1) * 32].reshape(128, 128) * (1.0 / count) for n, pair in enumerate(PAIRS)
    }
    metric = jnp.concatenate(
        [jnp.concatenate([at[i, j] if i <= j else at[j, i].T for j in range(3)], 1) for i in range(3)], 0
    )
    first = jnp.concatenate([at[i, 3] for i in range(3)], 0)
    second = mul(metric, first, (1, 0))
    third = mul(metric, second, (1, 0))
    coef = 2.0 * first - second
    image = 2.0 * second - third
    square = at[3, 3] + mul(coef, image - 2.0 * first, (0, 0))

    lane = lax.broadcasted_iota(jnp.int32, (NEW, NEW), 1)
    row = lax.broadcasted_iota(jnp.int32, (NEW, NEW), 0)
    def on_diagonal(v):
        return jnp.sum(jnp.where(lane == row, v, 0.0), axis=0, keepdims=True)
    terms = on_diagonal(at[3, 3]) + jnp.sum(jnp.abs(coef) * (2.0 * jnp.abs(first) + jnp.abs(image)), axis=0, keepdims=True)
    steady = jnp.where(terms <= 16.0 * on_diagonal(square), 1.0, 0.0)
    steady_ref[...] = jnp.broadcast_to(jnp.min(steady, axis=1, keepdims=True), (8, 128))

    inverse = inverse_factor(square, lane, row)
    tail = jnp.concatenate([-mul(coef, inverse, (1, 1)), inverse.T], 0)
    tail_high = tail.astype(BF16)
    tail_low = (tail - tail_high.astype(F32)).astype(BF16)
    both = jnp.concatenate([tail_high, tail_low], 1)
    for copy in fetch:
        copy.wait()

    def rows_of(b, _):
        rows = pl.ds(pl.multiple_of(b * 256, 256), 256)
        two = jnp.dot(high[rows, :], both, preferred_element_type=F32)
        one = jnp.dot(low[rows, :], tail_high, preferred_element_type=F32)
        basis_ref[rows, :] = two[:, :128] + (two[:, 128:] + one)
        return _

    lax.fori_loop(0, ROWS // 256, rows_of, 0)


def finish(total, high, low, count):
    vmem = pl.BlockSpec(memory_space=pltpu.VMEM)
    hbm = pl.BlockSpec(memory_space=pl.ANY)
    return pl.pallas_call(
        lambda *refs: finish_kernel(count, *refs),
        out_shape=(jax.ShapeDtypeStruct((ROWS, NEW), F32), jax.ShapeDtypeStruct((8, 128), F32)),
        in_specs=[vmem, hbm, hbm],
        out_specs=(vmem, vmem),
        scratch_shapes=[
            pltpu.VMEM((ROWS, KEEP + NEW), BF16),
            pltpu.VMEM((ROWS, KEEP + NEW), BF16),
            pltpu.SemaphoreType.DMA((2,)),
        ],
        name="finish",
    )(total, high, low)


def in_blocks(x, dim, size):
    before, after = (x.shape[:dim], x.shape[dim + 1 :])
    return jnp.moveaxis(x.reshape(*before, size, -1, *after), dim, 0)


def summed_on_arrival(x, axis, dim):
    parts = in_blocks(x, dim, lax.axis_size(axis))
    arrived = lax.all_to_all(parts, axis, split_axis=0, concat_axis=0, tiled=True)
    return arrived.sum(axis=0)


def sum_by_axis(x, axes, dim):
    far, near = axes
    own = summed_on_arrival(in_blocks(x, dim, lax.axis_size(far)), near, dim + 1)
    return jnp.sum(lax.all_to_all(own, far, 0, 0, tiled=True), axis=0)


def rows_for(lines, size):
    spare = -lines.shape[0] % size
    if not spare:
        return lines
    return jnp.concatenate([lines, jnp.zeros((spare, *lines.shape[1:]), lines.dtype)])


def sent_to_all(x, axis):
    copies = jnp.broadcast_to(x, (lax.axis_size(axis), *x.shape))
    return lax.all_to_all(copies, axis, split_axis=0, concat_axis=0, tiled=True)


def laid_out(parts, dim):
    parts = jnp.moveaxis(parts, 0, dim)
    dims = parts.shape
    return parts.reshape(*dims[:dim], dims[dim] * dims[dim + 1], *dims[dim + 2 :])


def whole_of(x, axes, dim):
    far, near = axes
    first = sent_to_all(x, far)
    parts = jnp.swapaxes(sent_to_all(first, near), 0, 1)
    return laid_out(parts.reshape(-1, *x.shape), dim)


def nested_sum(x, axes):
    own = sum_by_axis(rows_for(x, lax.axis_size(axes[0]) * lax.axis_size(axes[1])), axes, 0)
    whole = whole_of(own, axes, 0)
    return whole[: len(x)].reshape(x.shape)


def fdot(left, right):
    return jnp.dot(left, right, precision=lax.Precision.HIGHEST, preferred_element_type=F32)


def explicit(trial, resid, energy, shift, count):
    def total(v):
        return nested_sum(v.reshape(-1), (("x", "core"), ("y", "z"))).reshape(v.shape)

    work = resid / (energy[:, None] - shift[None, :])
    for sweep in range(2):
        work = work - fdot(trial, total(fdot(trial.T, work)) / count)
    lower = jnp.linalg.cholesky(total(fdot(work.T, work)) / count)
    return jax.scipy.linalg.solve_triangular(lower, work.T, lower=True).T


def per_device(trial, resid, energy, shift):
    count = ROWS * 512
    total, high, low = gram(trial, resid, energy, shift)
    basis, steady = finish(total, high, low, count)
    return lax.cond(
        steady[0, 0] > 0.5, lambda: basis, lambda: explicit(trial, resid, energy, shift, count)
    )


def solution(mesh):
    split = Mesh(mesh.devices.reshape(4, 2, 8, 8), AXES)
    in_specs = (P(AXES, None), P(AXES, None), P(AXES), P())
    return jax.shard_map(
        per_device, mesh=split, in_specs=in_specs, out_specs=P(AXES, None), check_vma=False
    )
```

```python
import jax
import jax.numpy as jnp
from jax import lax
from jax.experimental import pallas as pl
from jax.experimental.pallas import tpu as pltpu
from jax.sharding import Mesh
from jax.sharding import PartitionSpec as P

MESH = pl.DeviceIdType.MESH
AXES = ("x", "core", "y", "z")
ROWS, KEEP, NEW = 1536, 384, 128
STEP = 384
UNIT = 4
PAIRS = [(0, 0), (0, 1), (1, 1), (0, 2), (0, 3), (2, 2), (2, 3), (3, 3), (1, 2), (1, 3)]
HALF = len(PAIRS) * 128 // UNIT // 2
PLANE, LINE = 32, 8
CHUNK = HALF // PLANE
NEAR = [(i, j) for i in range(4) for j in range(8) if (i, j) != (0, 0)]
FAR = sorted(NEAR, key=lambda o: -min(o[0], 4 - o[0]) - min(o[1], 8 - o[1]))
F32, BF16 = jnp.float32, jnp.bfloat16


def tdot(a, b):
    return lax.dot_general(a, b, (((0,), (0,)), ((), ())), preferred_element_type=F32)


def gram_kernel(
    trial_ref, resid_ref, energy_ref, shift_ref, total_ref, high_ref, low_ref,
    trial, resid, energy, shift, hi, lo, part, peer, held, own, line, done,
    load_sems, core_sems, plane_sems, line_sems, gather_sems, spread_sems, last_sems, keep_sems,
):
    loads = [
        pltpu.make_async_copy(energy_ref, energy, load_sems.at[0]),
        pltpu.make_async_copy(shift_ref, shift, load_sems.at[1]),
    ]
    for b in range(ROWS // STEP):
        rows = pl.ds(b * STEP, STEP)
        loads.append(pltpu.make_async_copy(resid_ref.at[rows], resid.at[rows], load_sems.at[2 + 2 * b]))
        loads.append(pltpu.make_async_copy(trial_ref.at[rows], trial.at[rows], load_sems.at[3 + 2 * b]))
    for load in loads:
        load.start()

    x, c = lax.axis_index("x"), lax.axis_index("core")
    y, z = lax.axis_index("y"), lax.axis_index("z")
    p = (1 - c) * y + c * z
    q = (1 - c) * z + c * y
    me = x * 8 + p
    other = {"x": x, "core": 1 - c, "y": y, "z": z}
    xs = [(x + i) % 4 for i in range(4)]
    ps = [(p + j) % 8 for j in range(8)]
    qs = [(q + j) % 8 for j in range(8)]

    def in_plane(i, j):
        return {"x": xs[i], "core": c, "y": (1 - c) * ps[j] + c * y, "z": (1 - c) * z + c * ps[j]}

    def in_line(j):
        return {"x": x, "core": c, "y": (1 - c) * y + c * qs[j], "z": (1 - c) * qs[j] + c * z}

    barrier = pltpu.get_barrier_semaphore()
    for device in [other] + [in_plane(i, j) for i, j in FAR] + [in_line(j) for j in range(1, 8)]:
        pl.semaphore_signal(barrier, inc=1, device_id=device, device_id_type=MESH)

    for b in range(ROWS // STEP):
        for load in loads[2 * b + 2:2 * b + 4] + (loads[:2] if b == 0 else []):
            load.wait()
        for r in range(b * STEP, (b + 1) * STEP, 128):
            rows = pl.ds(r, 128)
            gap = jnp.broadcast_to(energy[pl.ds(r // 128, 1), :], (128, 128)).T - shift[...]
            for at, value in ((slice(0, KEEP), trial[rows, :]), (slice(KEEP, KEEP + NEW), resid[rows, :] / gap)):
                high = value.astype(BF16)
                hi[rows, at] = high
                lo[rows, at] = (value - high.astype(F32)).astype(BF16)

    keep = [
        pltpu.make_async_copy(hi, high_ref, keep_sems.at[0]),
        pltpu.make_async_copy(lo, low_ref, keep_sems.at[1]),
    ]
    for copy in keep:
        copy.start()

    def half(h):
        wide = pl.ds(pl.multiple_of(h * 256, 256), 256)
        thin = pl.ds(pl.multiple_of(h * 128, 128), 128)
        left = hi[:, wide]
        cross = tdot(left, lo[:, wide])
        full = tdot(left, left) + (cross + cross.T)
        left = hi[:, thin]
        side = tdot(left, hi[:, 256:]) + (tdot(left, lo[:, 256:]) + tdot(lo[:, thin], hi[:, 256:]))
        blocks = (full[:128, :128], full[:128, 128:], full[128:, 128:], side[:, :128], side[:, 128:])
        for n, block in enumerate(blocks):
            part[pl.ds(h * HALF + n * 32, 32)] = block.reshape(32, UNIT, 128)

    def remote(src, dst, sems, device):
        return pltpu.make_async_remote_copy(
            src_ref=src, dst_ref=dst, send_sem=sems.at[0], recv_sem=sems.at[1],
            device_id=device, device_id_type=MESH,
        )

    mine, theirs = c * HALF, (1 - c) * HALF
    half(1 - c)
    pl.semaphore_wait(barrier, PLANE + LINE - 1)
    swap = remote(part.at[pl.ds(theirs, HALF)], peer, core_sems, other)
    swap.start()
    half(c)
    swap.wait_recv()
    peer[...] += part[pl.ds(mine, HALF)]

    for n, (i, j) in enumerate(FAR):
        k = xs[i] * 8 + ps[j]
        remote(
            peer.at[pl.ds(k * CHUNK, CHUNK)], held.at[pl.ds(n * CHUNK, CHUNK)], plane_sems, in_plane(i, j)
        ).start()
    arrived = remote(held, held, plane_sems, other)
    arrived.wait_recv()
    total = peer[pl.ds(me * CHUNK, CHUNK)]
    for j in range(PLANE - 1):
        total += held[j * CHUNK:(j + 1) * CHUNK]
    own[...] = total
    line[pl.ds(q * CHUNK, CHUNK)] = total

    for j in (4, 3, 5, 2, 6, 1, 7):
        remote(own, line.at[pl.ds(q * CHUNK, CHUNK)], line_sems, in_line(j)).start()
    lines = line.at[pl.ds(0, (LINE - 1) * CHUNK)]
    remote(lines, lines, line_sems, other).wait_recv()
    total = line[0:CHUNK]
    for j in range(1, LINE):
        total += line[j * CHUNK:(j + 1) * CHUNK]
    done[...] = total
    total_ref[pl.ds(mine + me * CHUNK, CHUNK)] = total

    def chunk_of(k):
        return total_ref.at[pl.ds(mine + k * CHUNK, CHUNK)]

    def spread(n, k, device):
        return pltpu.make_async_remote_copy(
            src_ref=done, dst_ref=chunk_of(k), send_sem=gather_sems.at[0], recv_sem=spread_sems.at[n],
            device_id=device, device_id_type=MESH,
        )

    for n, (i, j) in enumerate(NEAR):
        spread(n, me, in_plane(i, j)).start()
    remote(done, chunk_of(me), last_sems, other).start()
    for n, (i, j) in enumerate(NEAR):
        k = xs[-i % 4] * 8 + ps[-j % 8]
        spread(n, k, other).wait_recv()
        remote(chunk_of(k), chunk_of(k), last_sems, other).start()
    whole = total_ref.at[pl.ds(theirs, HALF)]
    remote(whole, whole, last_sems, other).wait_recv()

    for copy in keep:
        copy.wait()
    swap.wait_send()
    arrived.wait_send()
    remote(lines, lines, line_sems, other).wait_send()
    remote(held, held, gather_sems, other).wait_send()
    remote(whole, whole, last_sems, other).wait_send()


def gram(trial, resid, energy, shift):
    vmem = pl.BlockSpec(memory_space=pltpu.VMEM)
    hbm = pl.BlockSpec(memory_space=pl.ANY)
    return pl.pallas_call(
        gram_kernel,
        out_shape=(
            jax.ShapeDtypeStruct((2 * HALF, UNIT, 128), F32),
            jax.ShapeDtypeStruct((ROWS, KEEP + NEW), BF16),
            jax.ShapeDtypeStruct((ROWS, KEEP + NEW), BF16),
        ),
        in_specs=[hbm] * 4,
        out_specs=(vmem, hbm, hbm),
        scratch_shapes=[
            pltpu.VMEM((ROWS, KEEP), F32),
            pltpu.VMEM((ROWS, NEW), F32),
            pltpu.VMEM((ROWS // 128, 128), F32),
            pltpu.VMEM((1, NEW), F32),
            pltpu.VMEM((ROWS, KEEP + NEW), BF16),
            pltpu.VMEM((ROWS, KEEP + NEW), BF16),
            pltpu.VMEM((2 * HALF, UNIT, 128), F32),
            pltpu.VMEM((HALF, UNIT, 128), F32),
            pltpu.VMEM(((PLANE - 1) * CHUNK, UNIT, 128), F32),
            pltpu.VMEM((CHUNK, UNIT, 128), F32),
            pltpu.VMEM((LINE * CHUNK, UNIT, 128), F32),
            pltpu.VMEM((CHUNK, UNIT, 128), F32),
            pltpu.SemaphoreType.DMA((2 + 2 * ROWS // STEP,)),
            pltpu.SemaphoreType.DMA((2,)),
            pltpu.SemaphoreType.DMA((2,)),
            pltpu.SemaphoreType.DMA((2,)),
            pltpu.SemaphoreType.DMA((2,)),
            pltpu.SemaphoreType.DMA((PLANE,)),
            pltpu.SemaphoreType.DMA((2,)),
            pltpu.SemaphoreType.DMA((2,)),
        ],
        compiler_params=pltpu.CompilerParams(collective_id=0, has_side_effects=True),
        name="gram",
    )(trial, resid, energy.reshape(ROWS // 128, 128), shift.reshape(1, NEW))


SIDE = 32


def mul(left, right, dims):
    return lax.dot_general(
        left, right, ((dims[:1], dims[1:]), ((), ())), precision=lax.Precision.HIGHEST, preferred_element_type=F32
    )


def inverse_factor(square, lane, row):
    tiles = SIDE // 8
    sub = row[:8]
    panels = []
    rest = square
    for base in range(0, NEW, SIDE):
        here = (lane >= base) & (lane < base + SIDE)
        top = rest[:SIDE]
        cols = [
            [jnp.broadcast_to(top[t * 8:t * 8 + 8, base + j:base + j + 1], (8, 128)) if t >= j // 8 else None
             for t in range(tiles)]
            for j in range(SIDE)
        ]
        unit = jnp.where(lane[:SIDE] == row[:SIDE] + base, 1.0, 0.0)
        panel = jnp.where(here[:SIDE], unit, top)
        panel = [panel[t * 8:t * 8 + 8] for t in range(tiles)]
        for k in range(SIDE):
            tk, sk = k // 8, k % 8
            pivot = jnp.broadcast_to(cols[k][tk][sk:sk + 1], (8, 128))
            scale = lax.rsqrt(pivot)
            if k + 1 < SIDE:
                tn, sn = (k + 1) // 8, (k + 1) % 8
                line = jnp.broadcast_to(cols[k][tn][sn:sn + 1], (8, 128))
                ratio = scale * scale
                for t in range(tn, tiles):
                    cols[k + 1][t] = cols[k + 1][t] - (cols[k][t] * line) * ratio
            for t in range(tk, tiles):
                cols[k][t] = cols[k][t] * scale
            line = jnp.broadcast_to(panel[tk][sk:sk + 1], (8, 128)) * scale
            panel[tk] = jnp.where(
                sub == sk, line, panel[tk] - jnp.where(sub > sk, cols[k][tk], 0.0) * line
            )
            for t in range(tk + 1, tiles):
                panel[t] = panel[t] - cols[k][t] * line
            for j in range(k + 2, SIDE):
                line = jnp.broadcast_to(cols[k][j // 8][j % 8:j % 8 + 1], (8, 128))
                for t in range(j // 8, tiles):
                    cols[j][t] = cols[j][t] - cols[k][t] * line
        done = jnp.concatenate(panel, 0)
        panels.append(done)
        if base + SIDE < NEW:
            left = rest.shape[0] - SIDE
            below = jnp.where(here[:left], 0.0, rest[SIDE:])
            rest = below - mul(done, done, (0, 0))[base + SIDE:]
    whole = jnp.concatenate(panels, 0)
    return jnp.where(lane <= row, whole, 0.0)


def finish_kernel(count, total_ref, high_ref, low_ref, basis_ref, steady_ref, high, low, sems):
    fetch = [
        pltpu.make_async_copy(high_ref, high, sems.at[0]),
        pltpu.make_async_copy(low_ref, low, sems.at[1]),
    ]
    for copy in fetch:
        copy.start()
    at = {
        pair: total_ref[n * 32:(n + 1) * 32].reshape(128, 128) * (1.0 / count) for n, pair in enumerate(PAIRS)
    }
    metric = jnp.concatenate(
        [jnp.concatenate([at[i, j] if i <= j else at[j, i].T for j in range(3)], 1) for i in range(3)], 0
    )
    first = jnp.concatenate([at[i, 3] for i in range(3)], 0)
    second = mul(metric, first, (1, 0))
    third = mul(metric, second, (1, 0))
    coef = 2.0 * first - second
    image = 2.0 * second - third
    square = at[3, 3] + mul(coef, image - 2.0 * first, (0, 0))

    lane = lax.broadcasted_iota(jnp.int32, (NEW, NEW), 1)
    row = lax.broadcasted_iota(jnp.int32, (NEW, NEW), 0)
    def on_diagonal(v):
        return jnp.sum(jnp.where(lane == row, v, 0.0), axis=0, keepdims=True)
    terms = on_diagonal(at[3, 3]) + jnp.sum(jnp.abs(coef) * (2.0 * jnp.abs(first) + jnp.abs(image)), axis=0, keepdims=True)
    steady = jnp.where(terms <= 16.0 * on_diagonal(square), 1.0, 0.0)
    steady_ref[0, 0] = jnp.min(steady)

    inverse = inverse_factor(square, lane, row)
    tail = jnp.concatenate([-mul(coef, inverse, (1, 1)), inverse.T], 0)
    tail_high = tail.astype(BF16)
    tail_low = (tail - tail_high.astype(F32)).astype(BF16)
    both = jnp.concatenate([tail_high, tail_low], 1)
    for copy in fetch:
        copy.wait()

    def rows_of(b, _):
        rows = pl.ds(pl.multiple_of(b * 256, 256), 256)
        two = jnp.dot(high[rows, :], both, preferred_element_type=F32)
        one = jnp.dot(low[rows, :], tail_high, preferred_element_type=F32)
        basis_ref[rows, :] = two[:, :128] + (two[:, 128:] + one)
        return _

    lax.fori_loop(0, ROWS // 256, rows_of, 0)


def finish(total, high, low, count):
    vmem = pl.BlockSpec(memory_space=pltpu.VMEM)
    hbm = pl.BlockSpec(memory_space=pl.ANY)
    return pl.pallas_call(
        lambda *refs: finish_kernel(count, *refs),
        out_shape=(jax.ShapeDtypeStruct((ROWS, NEW), F32), jax.ShapeDtypeStruct((1, 1), F32)),
        in_specs=[vmem, hbm, hbm],
        out_specs=(vmem, pl.BlockSpec(memory_space=pltpu.SMEM)),
        scratch_shapes=[
            pltpu.VMEM((ROWS, KEEP + NEW), BF16),
            pltpu.VMEM((ROWS, KEEP + NEW), BF16),
            pltpu.SemaphoreType.DMA((2,)),
        ],
        name="finish",
    )(total, high, low)


def in_blocks(x, dim, size):
    before, after = (x.shape[:dim], x.shape[dim + 1 :])
    return jnp.moveaxis(x.reshape(*before, size, -1, *after), dim, 0)


def summed_on_arrival(x, axis, dim):
    parts = in_blocks(x, dim, lax.axis_size(axis))
    arrived = lax.all_to_all(parts, axis, split_axis=0, concat_axis=0, tiled=True)
    return arrived.sum(axis=0)


def sum_by_axis(x, axes, dim):
    far, near = axes
    own = summed_on_arrival(in_blocks(x, dim, lax.axis_size(far)), near, dim + 1)
    return jnp.sum(lax.all_to_all(own, far, 0, 0, tiled=True), axis=0)


def rows_for(lines, size):
    spare = -lines.shape[0] % size
    if not spare:
        return lines
    return jnp.concatenate([lines, jnp.zeros((spare, *lines.shape[1:]), lines.dtype)])


def sent_to_all(x, axis):
    copies = jnp.broadcast_to(x, (lax.axis_size(axis), *x.shape))
    return lax.all_to_all(copies, axis, split_axis=0, concat_axis=0, tiled=True)


def laid_out(parts, dim):
    parts = jnp.moveaxis(parts, 0, dim)
    dims = parts.shape
    return parts.reshape(*dims[:dim], dims[dim] * dims[dim + 1], *dims[dim + 2 :])


def whole_of(x, axes, dim):
    far, near = axes
    first = sent_to_all(x, far)
    parts = jnp.swapaxes(sent_to_all(first, near), 0, 1)
    return laid_out(parts.reshape(-1, *x.shape), dim)


def nested_sum(x, axes):
    own = sum_by_axis(rows_for(x, lax.axis_size(axes[0]) * lax.axis_size(axes[1])), axes, 0)
    whole = whole_of(own, axes, 0)
    return whole[: len(x)].reshape(x.shape)


def fdot(left, right):
    return jnp.dot(left, right, precision=lax.Precision.HIGHEST, preferred_element_type=F32)


def explicit(trial, resid, energy, shift, count):
    def total(v):
        return nested_sum(v.reshape(-1), (("x", "core"), ("y", "z"))).reshape(v.shape)

    work = resid / (energy[:, None] - shift[None, :])
    for sweep in range(2):
        work = work - fdot(trial, total(fdot(trial.T, work)) / count)
    lower = jnp.linalg.cholesky(total(fdot(work.T, work)) / count)
    return jax.scipy.linalg.solve_triangular(lower, work.T, lower=True).T


def per_device(trial, resid, energy, shift):
    count = ROWS * 512
    total, high, low = gram(trial, resid, energy, shift)
    basis, steady = finish(total, high, low, count)
    return lax.cond(
        steady[0, 0] > 0.5, lambda: basis, lambda: explicit(trial, resid, energy, shift, count)
    )


def solution(mesh):
    split = Mesh(mesh.devices.reshape(4, 2, 8, 8), AXES)
    in_specs = (P(AXES, None), P(AXES, None), P(AXES), P())
    return jax.shard_map(
        per_device, mesh=split, in_specs=in_specs, out_specs=P(AXES, None), check_vma=False
    )
```

```python
import jax
import jax.numpy as jnp
from jax import lax
from jax.experimental import pallas as pl
from jax.experimental.pallas import tpu as pltpu
from jax.sharding import Mesh
from jax.sharding import PartitionSpec as P

MESH = pl.DeviceIdType.MESH
AXES = ("x", "core", "y", "z")
ROWS, KEEP, NEW = 1536, 384, 128
STEP = 384
VMEM_LIMIT = 24 * 2**20
UNIT = 4
PAIRS = [(0, 0), (0, 1), (1, 1), (0, 2), (0, 3), (2, 2), (2, 3), (3, 3), (1, 2), (1, 3)]
HALF = len(PAIRS) * 128 // UNIT // 2
PLANE, LINE = 32, 8
CHUNK = HALF // PLANE
NEAR = [(i, j) for i in range(4) for j in range(8) if (i, j) != (0, 0)]
FAR = sorted(NEAR, key=lambda o: -min(o[0], 4 - o[0]) - min(o[1], 8 - o[1]))
F32, BF16 = jnp.float32, jnp.bfloat16


def tdot(a, b):
    return lax.dot_general(a, b, (((0,), (0,)), ((), ())), preferred_element_type=F32)


def gram_kernel(
    trial_ref, resid_ref, energy_ref, shift_ref, total_ref, hi, lo,
    trial, resid, energy, shift, part, peer, held, own, line, done,
    load_sems, core_sems, plane_sems, line_sems, gather_sems, spread_sems, last_sems,
):
    loads = [
        pltpu.make_async_copy(energy_ref, energy, load_sems.at[0]),
        pltpu.make_async_copy(shift_ref, shift, load_sems.at[1]),
    ]
    for b in range(ROWS // STEP):
        rows = pl.ds(b * STEP, STEP)
        loads.append(pltpu.make_async_copy(resid_ref.at[rows], resid.at[rows], load_sems.at[2 + 2 * b]))
        loads.append(pltpu.make_async_copy(trial_ref.at[rows], trial.at[rows], load_sems.at[3 + 2 * b]))
    for load in loads:
        load.start()

    x, c = lax.axis_index("x"), lax.axis_index("core")
    y, z = lax.axis_index("y"), lax.axis_index("z")
    p = (1 - c) * y + c * z
    q = (1 - c) * z + c * y
    me = x * 8 + p
    other = {"x": x, "core": 1 - c, "y": y, "z": z}
    xs = [(x + i) % 4 for i in range(4)]
    ps = [(p + j) % 8 for j in range(8)]
    qs = [(q + j) % 8 for j in range(8)]

    def in_plane(i, j):
        return {"x": xs[i], "core": c, "y": (1 - c) * ps[j] + c * y, "z": (1 - c) * z + c * ps[j]}

    def in_line(j):
        return {"x": x, "core": c, "y": (1 - c) * y + c * qs[j], "z": (1 - c) * qs[j] + c * z}

    barrier = pltpu.get_barrier_semaphore()
    for device in [other] + [in_plane(i, j) for i, j in FAR] + [in_line(j) for j in range(1, 8)]:
        pl.semaphore_signal(barrier, inc=1, device_id=device, device_id_type=MESH)

    for b in range(ROWS // STEP):
        for load in loads[2 * b + 2:2 * b + 4] + (loads[:2] if b == 0 else []):
            load.wait()
        for r in range(b * STEP, (b + 1) * STEP, 128):
            rows = pl.ds(r, 128)
            gap = jnp.broadcast_to(energy[pl.ds(r // 128, 1), :], (128, 128)).T - shift[...]
            for at, value in ((slice(0, KEEP), trial[rows, :]), (slice(KEEP, KEEP + NEW), resid[rows, :] / gap)):
                high = value.astype(BF16)
                hi[rows, at] = high
                lo[rows, at] = (value - high.astype(F32)).astype(BF16)

    def half(h):
        wide = pl.ds(pl.multiple_of(h * 256, 256), 256)
        thin = pl.ds(pl.multiple_of(h * 128, 128), 128)
        left = hi[:, wide]
        cross = tdot(left, lo[:, wide])
        full = tdot(left, left) + (cross + cross.T)
        left = hi[:, thin]
        side = tdot(left, hi[:, 256:]) + (tdot(left, lo[:, 256:]) + tdot(lo[:, thin], hi[:, 256:]))
        blocks = (full[:128, :128], full[:128, 128:], full[128:, 128:], side[:, :128], side[:, 128:])
        for n, block in enumerate(blocks):
            part[pl.ds(h * HALF + n * 32, 32)] = block.reshape(32, UNIT, 128)

    def remote(src, dst, sems, device):
        return pltpu.make_async_remote_copy(
            src_ref=src, dst_ref=dst, send_sem=sems.at[0], recv_sem=sems.at[1],
            device_id=device, device_id_type=MESH,
        )

    mine, theirs = c * HALF, (1 - c) * HALF
    half(1 - c)
    pl.semaphore_wait(barrier, PLANE + LINE - 1)
    swap = remote(part.at[pl.ds(theirs, HALF)], peer, core_sems, other)
    swap.start()
    half(c)
    swap.wait_recv()
    peer[...] += part[pl.ds(mine, HALF)]

    for n, (i, j) in enumerate(FAR):
        k = xs[i] * 8 + ps[j]
        remote(
            peer.at[pl.ds(k * CHUNK, CHUNK)], held.at[pl.ds(n * CHUNK, CHUNK)], plane_sems, in_plane(i, j)
        ).start()
    arrived = remote(held, held, plane_sems, other)
    arrived.wait_recv()
    total = peer[pl.ds(me * CHUNK, CHUNK)]
    for j in range(PLANE - 1):
        total += held[j * CHUNK:(j + 1) * CHUNK]
    own[...] = total
    line[pl.ds(q * CHUNK, CHUNK)] = total

    for j in (4, 3, 5, 2, 6, 1, 7):
        remote(own, line.at[pl.ds(q * CHUNK, CHUNK)], line_sems, in_line(j)).start()
    lines = line.at[pl.ds(0, (LINE - 1) * CHUNK)]
    remote(lines, lines, line_sems, other).wait_recv()
    total = line[0:CHUNK]
    for j in range(1, LINE):
        total += line[j * CHUNK:(j + 1) * CHUNK]
    done[...] = total
    total_ref[pl.ds(mine + me * CHUNK, CHUNK)] = total

    def chunk_of(k):
        return total_ref.at[pl.ds(mine + k * CHUNK, CHUNK)]

    def spread(n, k, device):
        return pltpu.make_async_remote_copy(
            src_ref=done, dst_ref=chunk_of(k), send_sem=gather_sems.at[0], recv_sem=spread_sems.at[n],
            device_id=device, device_id_type=MESH,
        )

    for n, (i, j) in enumerate(NEAR):
        spread(n, me, in_plane(i, j)).start()
    remote(done, chunk_of(me), last_sems, other).start()
    for n, (i, j) in enumerate(NEAR):
        k = xs[-i % 4] * 8 + ps[-j % 8]
        spread(n, k, other).wait_recv()
        remote(chunk_of(k), chunk_of(k), last_sems, other).start()
    whole = total_ref.at[pl.ds(theirs, HALF)]
    remote(whole, whole, last_sems, other).wait_recv()

    swap.wait_send()
    arrived.wait_send()
    remote(lines, lines, line_sems, other).wait_send()
    remote(held, held, gather_sems, other).wait_send()
    remote(whole, whole, last_sems, other).wait_send()


def gram(trial, resid, energy, shift):
    vmem = pl.BlockSpec(memory_space=pltpu.VMEM)
    hbm = pl.BlockSpec(memory_space=pl.ANY)
    return pl.pallas_call(
        gram_kernel,
        out_shape=(
            pltpu.VMEM((2 * HALF, UNIT, 128), F32),
            pltpu.VMEM((ROWS, KEEP + NEW), BF16),
            pltpu.VMEM((ROWS, KEEP + NEW), BF16),
        ),
        in_specs=[hbm] * 4,
        out_specs=(vmem, vmem, vmem),
        scratch_shapes=[
            pltpu.VMEM((ROWS, KEEP), F32),
            pltpu.VMEM((ROWS, NEW), F32),
            pltpu.VMEM((ROWS // 128, 128), F32),
            pltpu.VMEM((1, NEW), F32),
            pltpu.VMEM((2 * HALF, UNIT, 128), F32),
            pltpu.VMEM((HALF, UNIT, 128), F32),
            pltpu.VMEM(((PLANE - 1) * CHUNK, UNIT, 128), F32),
            pltpu.VMEM((CHUNK, UNIT, 128), F32),
            pltpu.VMEM((LINE * CHUNK, UNIT, 128), F32),
            pltpu.VMEM((CHUNK, UNIT, 128), F32),
            pltpu.SemaphoreType.DMA((2 + 2 * ROWS // STEP,)),
            pltpu.SemaphoreType.DMA((2,)),
            pltpu.SemaphoreType.DMA((2,)),
            pltpu.SemaphoreType.DMA((2,)),
            pltpu.SemaphoreType.DMA((2,)),
            pltpu.SemaphoreType.DMA((PLANE,)),
            pltpu.SemaphoreType.DMA((2,)),
        ],
        compiler_params=pltpu.CompilerParams(
            collective_id=0, has_side_effects=True, vmem_limit_bytes=VMEM_LIMIT
        ),
        name="gram",
    )(trial, resid, energy.reshape(ROWS // 128, 128), shift.reshape(1, NEW))


SIDE = 32


def halves(value):
    high = value.astype(BF16)
    return high, (value - high.astype(F32)).astype(BF16)


def dot(left, right):
    return jnp.dot(left, right, preferred_element_type=F32)


def mul(left, right):
    wide = dot(left[0], jnp.concatenate(right, 1))
    return wide[:, :NEW] + (wide[:, NEW:] + dot(left[1], right[0]))


def square_of(v):
    a, rest = v.astype(BF16), v
    rest = rest - a.astype(F32)
    b = rest.astype(BF16)
    c = (rest - b.astype(F32)).astype(BF16)
    return tdot(jnp.concatenate([a, a, a, b, b, c], 0), jnp.concatenate([a, b, c, a, b, a], 0))


def inverse_factor(square, lane, row):
    tiles = SIDE // 8
    sub = row[:8]
    panels = []
    rest = square
    for base in range(0, NEW, SIDE):
        here = (lane >= base) & (lane < base + SIDE)
        top = rest[:SIDE]
        cols = [
            [jnp.broadcast_to(top[t * 8:t * 8 + 8, base + j:base + j + 1], (8, 128)) if t >= j // 8 else None
             for t in range(tiles)]
            for j in range(SIDE)
        ]
        unit = jnp.where(lane[:SIDE] == row[:SIDE] + base, 1.0, 0.0)
        panel = jnp.where(here[:SIDE], unit, top)
        panel = [panel[t * 8:t * 8 + 8] for t in range(tiles)]
        for k in range(SIDE):
            tk, sk = k // 8, k % 8
            pivot = jnp.broadcast_to(cols[k][tk][sk:sk + 1], (8, 128))
            scale = lax.rsqrt(pivot)
            if k + 1 < SIDE:
                tn, sn = (k + 1) // 8, (k + 1) % 8
                line = jnp.broadcast_to(cols[k][tn][sn:sn + 1], (8, 128))
                ratio = scale * scale
                for t in range(tn, tiles):
                    cols[k + 1][t] = cols[k + 1][t] - (cols[k][t] * line) * ratio
            for t in range(tk, tiles):
                cols[k][t] = cols[k][t] * scale
            line = jnp.broadcast_to(panel[tk][sk:sk + 1], (8, 128)) * scale
            panel[tk] = jnp.where(
                sub == sk, line, panel[tk] - jnp.where(sub > sk, cols[k][tk], 0.0) * line
            )
            for t in range(tk + 1, tiles):
                panel[t] = panel[t] - cols[k][t] * line
            for j in range(k + 2, SIDE):
                line = jnp.broadcast_to(cols[k][j // 8][j % 8:j % 8 + 1], (8, 128))
                for t in range(j // 8, tiles):
                    cols[j][t] = cols[j][t] - cols[k][t] * line
        done = jnp.concatenate(panel, 0)
        panels.append(done)
        if base + SIDE < NEW:
            left = rest.shape[0] - SIDE
            below = jnp.where(here[:left], 0.0, rest[SIDE:])
            rest = below - square_of(done)[base + SIDE:]
    whole = jnp.concatenate(panels, 0)
    return jnp.where(lane <= row, whole, 0.0)


def finish_kernel(count, total_ref, high, low, basis_ref, steady_ref, work, basis, sems):
    at = {
        pair: total_ref[n * 32:(n + 1) * 32].reshape(128, 128) * (1.0 / count) for n, pair in enumerate(PAIRS)
    }
    metric = halves(jnp.concatenate(
        [jnp.concatenate([at[i, j] if i <= j else at[j, i].T for j in range(3)], 1) for i in range(3)], 0
    ))
    first = jnp.concatenate([at[i, 3] for i in range(3)], 0)
    second = mul(metric, halves(first))
    third = mul(metric, halves(second))
    coef = 2.0 * first - second
    image = 2.0 * second - third
    pair = halves(coef)
    known = halves(image - 2.0 * first)
    wide = tdot(pair[0], jnp.concatenate(known, 1))
    square = at[3, 3] + (wide[:, :NEW] + (wide[:, NEW:] + tdot(pair[1], known[0])))

    lane = lax.broadcasted_iota(jnp.int32, (NEW, NEW), 1)
    row = lax.broadcasted_iota(jnp.int32, (NEW, NEW), 0)

    def on_diagonal(v):
        return jnp.sum(jnp.where(lane == row, v, 0.0), axis=0, keepdims=True)

    terms = on_diagonal(at[3, 3]) + jnp.sum(
        jnp.abs(coef) * (2.0 * jnp.abs(first) + jnp.abs(image)), axis=0, keepdims=True
    )
    both = jnp.concatenate(pair, 1)
    for r in range(0, ROWS, 256):
        rows = slice(r, r + 256)
        wide = dot(high[rows, :KEEP], both)
        inside = wide[:, :NEW] + (wide[:, NEW:] + dot(low[rows, :KEEP], pair[0]))
        block = (high[rows, KEEP:].astype(F32) - inside) + low[rows, KEEP:].astype(F32)
        work[rows, :NEW], work[rows, NEW:] = halves(block)

    inverse = inverse_factor(square, lane, row)
    steady = (terms <= 4.0 * on_diagonal(square)) & (on_diagonal(square) * on_diagonal(inverse) ** 2 <= 1000.0)
    steady_ref[0, 0] = jnp.min(jnp.where(steady, 1.0, 0.0))
    inverse = halves(inverse.T)
    stack = jnp.concatenate(
        [jnp.concatenate(inverse, 1), jnp.concatenate([inverse[0], jnp.zeros_like(inverse[0])], 1)], 0
    )
    stores = []
    for n in range(4):
        rows = pl.ds(n * (ROWS // 4), ROWS // 4)
        wide = dot(work[rows, :], stack)
        basis[rows, :] = wide[:, :NEW] + wide[:, NEW:]
        stores.append(pltpu.make_async_copy(basis.at[rows], basis_ref.at[rows], sems.at[n]))
        stores[-1].start()
    for store in stores:
        store.wait()


def finish(total, high, low, count):
    vmem = pl.BlockSpec(memory_space=pltpu.VMEM)
    return pl.pallas_call(
        lambda *refs: finish_kernel(count, *refs),
        out_shape=(jax.ShapeDtypeStruct((ROWS, NEW), F32), jax.ShapeDtypeStruct((1, 1), F32)),
        in_specs=[vmem] * 3,
        out_specs=(pl.BlockSpec(memory_space=pl.ANY), pl.BlockSpec(memory_space=pltpu.SMEM)),
        scratch_shapes=[
            pltpu.VMEM((ROWS, 2 * NEW), BF16),
            pltpu.VMEM((ROWS, NEW), F32),
            pltpu.SemaphoreType.DMA((4,)),
        ],
        compiler_params=pltpu.CompilerParams(vmem_limit_bytes=VMEM_LIMIT),
        name="finish",
    )(total, high, low)


def in_blocks(x, dim, size):
    before, after = (x.shape[:dim], x.shape[dim + 1 :])
    return jnp.moveaxis(x.reshape(*before, size, -1, *after), dim, 0)


def summed_on_arrival(x, axis, dim):
    parts = in_blocks(x, dim, lax.axis_size(axis))
    arrived = lax.all_to_all(parts, axis, split_axis=0, concat_axis=0, tiled=True)
    return arrived.sum(axis=0)


def sum_by_axis(x, axes, dim):
    far, near = axes
    own = summed_on_arrival(in_blocks(x, dim, lax.axis_size(far)), near, dim + 1)
    return jnp.sum(lax.all_to_all(own, far, 0, 0, tiled=True), axis=0)


def rows_for(lines, size):
    spare = -lines.shape[0] % size
    if not spare:
        return lines
    return jnp.concatenate([lines, jnp.zeros((spare, *lines.shape[1:]), lines.dtype)])


def sent_to_all(x, axis):
    copies = jnp.broadcast_to(x, (lax.axis_size(axis), *x.shape))
    return lax.all_to_all(copies, axis, split_axis=0, concat_axis=0, tiled=True)


def laid_out(parts, dim):
    parts = jnp.moveaxis(parts, 0, dim)
    dims = parts.shape
    return parts.reshape(*dims[:dim], dims[dim] * dims[dim + 1], *dims[dim + 2 :])


def whole_of(x, axes, dim):
    far, near = axes
    first = sent_to_all(x, far)
    parts = jnp.swapaxes(sent_to_all(first, near), 0, 1)
    return laid_out(parts.reshape(-1, *x.shape), dim)


def nested_sum(x, axes):
    own = sum_by_axis(rows_for(x, lax.axis_size(axes[0]) * lax.axis_size(axes[1])), axes, 0)
    whole = whole_of(own, axes, 0)
    return whole[: len(x)].reshape(x.shape)


def fdot(left, right):
    return jnp.dot(left, right, precision=lax.Precision.HIGHEST, preferred_element_type=F32)


def explicit(trial, resid, energy, shift, count):
    def total(v):
        return nested_sum(v.reshape(-1), (("x", "core"), ("y", "z"))).reshape(v.shape)

    work = resid / (energy[:, None] - shift[None, :])
    work = lax.fori_loop(0, 2, lambda _, w: w - fdot(trial, total(fdot(trial.T, w)) / count), work)
    lower = jnp.linalg.cholesky(total(fdot(work.T, work)) / count)
    return jax.scipy.linalg.solve_triangular(lower, work.T, lower=True).T


def per_device(trial, resid, energy, shift):
    count = ROWS * 512
    total, high, low = gram(trial, resid, energy, shift)
    basis, steady = finish(total, high, low, count)
    return lax.cond(
        steady[0, 0] > 0.5, lambda: basis, lambda: explicit(trial, resid, energy, shift, count)
    )


def solution(mesh):
    split = Mesh(mesh.devices.reshape(4, 2, 8, 8), AXES)
    in_specs = (P(AXES, None), P(AXES, None), P(AXES), P())
    return jax.shard_map(
        per_device, mesh=split, in_specs=in_specs, out_specs=P(AXES, None), check_vma=False
    )
```

```python
import jax
import jax.numpy as jnp
from jax import lax
from jax.experimental import pallas as pl
from jax.experimental.pallas import tpu as pltpu
from jax.sharding import Mesh
from jax.sharding import PartitionSpec as P

MESH = pl.DeviceIdType.MESH
AXES = ("x", "core", "y", "z")
ROWS, KEEP, NEW = 1536, 384, 128
STEP = 384
VMEM_LIMIT = 24 * 2**20
UNIT = 4
PAIRS = [(0, 0), (0, 1), (1, 1), (0, 2), (0, 3), (2, 2), (2, 3), (3, 3), (1, 2), (1, 3)]
HALF = len(PAIRS) * 128 // UNIT // 2
PLANE, LINE = 32, 8
PIECES = ((0, 2), (2, 3))
CHUNK = sum(size for _, size in PIECES)
NEAR = [(i, j) for i in range(4) for j in range(8) if (i, j) != (0, 0)]
ARRIVAL = sorted(NEAR, key=lambda o: min(o[0], 4 - o[0]) + min(o[1], 8 - o[1]))
FAR = ARRIVAL[::-1]
F32, BF16 = jnp.float32, jnp.bfloat16


def tdot(a, b):
    return lax.dot_general(a, b, (((0,), (0,)), ((), ())), preferred_element_type=F32)


def gram_kernel(
    trial_ref, resid_ref, energy_ref, shift_ref, total_ref, hi, lo,
    trial, resid, energy, shift, part, peer, held, own, line, done,
    load_sems, core_sems, plane_sems, line_sems, gather_sems, spread_sems, last_sems,
):
    x, c = lax.axis_index("x"), lax.axis_index("core")
    y, z = lax.axis_index("y"), lax.axis_index("z")
    p = (1 - c) * y + c * z
    q = (1 - c) * z + c * y
    me = x * 8 + p
    other = {"x": x, "core": 1 - c, "y": y, "z": z}
    xs = [(x + i) % 4 for i in range(4)]
    ps = [(p + j) % 8 for j in range(8)]
    qs = [(q + j) % 8 for j in range(8)]

    def in_plane(i, j):
        return {"x": xs[i], "core": c, "y": (1 - c) * ps[j] + c * y, "z": (1 - c) * z + c * ps[j]}

    def in_line(j):
        return {"x": x, "core": c, "y": (1 - c) * y + c * qs[j], "z": (1 - c) * qs[j] + c * z}

    barrier = pltpu.get_barrier_semaphore()
    for device in [other] + [in_plane(i, j) for i, j in FAR] + [in_line(j) for j in range(1, 8)]:
        pl.semaphore_signal(barrier, inc=1, device_id=device, device_id_type=MESH)

    loads = [
        pltpu.make_async_copy(energy_ref, energy, load_sems.at[0]),
        pltpu.make_async_copy(shift_ref, shift, load_sems.at[1]),
    ]
    for b in range(ROWS // STEP):
        rows = pl.ds(b * STEP, STEP)
        loads.append(pltpu.make_async_copy(resid_ref.at[rows], resid.at[rows], load_sems.at[2 + 2 * b]))
        loads.append(pltpu.make_async_copy(trial_ref.at[rows], trial.at[rows], load_sems.at[3 + 2 * b]))
    for load in loads:
        load.start()

    for b in range(ROWS // STEP):
        for load in loads[2 * b + 2:2 * b + 4] + (loads[:2] if b == 0 else []):
            load.wait()
        for r in range(b * STEP, (b + 1) * STEP, 128):
            rows = pl.ds(r, 128)
            gap = jnp.broadcast_to(energy[pl.ds(r // 128, 1), :], (128, 128)).T - shift[...]
            for at, value in ((slice(0, KEEP), trial[rows, :]), (slice(KEEP, KEEP + NEW), resid[rows, :] / gap)):
                high = value.astype(BF16)
                hi[rows, at] = high
                lo[rows, at] = (value - high.astype(F32)).astype(BF16)

    def half(h):
        wide = pl.ds(pl.multiple_of(h * 256, 256), 256)
        thin = pl.ds(pl.multiple_of(h * 128, 128), 128)
        left = hi[:, wide]
        cross = tdot(left, lo[:, wide])
        full = tdot(left, left) + (cross + cross.T)
        left = hi[:, thin]
        side = tdot(left, hi[:, 256:]) + (tdot(left, lo[:, 256:]) + tdot(lo[:, thin], hi[:, 256:]))
        blocks = (full[:128, :128], full[:128, 128:], full[128:, 128:], side[:, :128], side[:, 128:])
        for n, block in enumerate(blocks):
            part[pl.ds(h * HALF + n * 32, 32)] = block.reshape(32, UNIT, 128)

    def remote(src, dst, sems, n, device):
        return pltpu.make_async_remote_copy(
            src_ref=src, dst_ref=dst, send_sem=sems.at[2 * n], recv_sem=sems.at[2 * n + 1],
            device_id=device, device_id_type=MESH,
        )

    mine, theirs = c * HALF, (1 - c) * HALF
    started = []
    half(1 - c)
    pl.semaphore_wait(barrier, PLANE + LINE - 1)
    swaps = [
        remote(
            part.at[pl.ds(theirs + at * PLANE, size * PLANE)], peer.at[pl.ds(at * PLANE, size * PLANE)],
            core_sems, n, other,
        )
        for n, (at, size) in enumerate(PIECES)
    ]
    for swap in swaps:
        swap.start()
    half(c)
    for n, (at, size) in enumerate(PIECES):
        swaps[n].wait_recv()
        peer[at * PLANE:(at + size) * PLANE] += part[pl.ds(mine + at * PLANE, size * PLANE)]
        for m, (i, j) in enumerate(FAR):
            k = xs[i] * 8 + ps[j]
            remote(
                peer.at[pl.ds(at * PLANE + k * size, size)], held.at[pl.ds(at * (PLANE - 1) + m * size, size)],
                plane_sems, n, in_plane(i, j),
            ).start()

    for n, (at, size) in enumerate(PIECES):
        base = at * (PLANE - 1)
        pieces = held.at[pl.ds(base, (PLANE - 1) * size)]
        started.append(remote(pieces, pieces, plane_sems, n, other))
        started[-1].wait_recv()
        total = peer[pl.ds(at * PLANE + me * size, size)]
        for m in range(PLANE - 1):
            total += held[base + m * size:base + (m + 1) * size]
        own[at:at + size] = total
        spot = pl.ds(at * LINE + q * size, size)
        line[spot] = total
        for j in (4, 3, 5, 2, 6, 1, 7):
            remote(own.at[pl.ds(at, size)], line.at[spot], line_sems, n, in_line(j)).start()

    def chunk_of(n, k):
        at, size = PIECES[n]
        return total_ref.at[pl.ds(mine + at * PLANE + k * size, size)]

    def spread(n, m, k, device):
        return pltpu.make_async_remote_copy(
            src_ref=done.at[pl.ds(*PIECES[n])], dst_ref=chunk_of(n, k),
            send_sem=gather_sems.at[n], recv_sem=spread_sems.at[n * PLANE + m],
            device_id=device, device_id_type=MESH,
        )

    for n, (at, size) in enumerate(PIECES):
        lines = line.at[pl.ds(at * LINE, (LINE - 1) * size)]
        started.append(remote(lines, lines, line_sems, n, other))
        started[-1].wait_recv()
        total = line[at * LINE:at * LINE + size]
        for j in range(1, LINE):
            total += line[at * LINE + j * size:at * LINE + (j + 1) * size]
        done[at:at + size] = total
        total_ref[pl.ds(mine + at * PLANE + me * size, size)] = total
        for m, (i, j) in enumerate(NEAR):
            spread(n, m, me, in_plane(i, j)).start()
        remote(done.at[pl.ds(at, size)], chunk_of(n, me), last_sems, 0, other).start()

    for n in range(len(PIECES)):
        for i, j in ARRIVAL:
            k = xs[-i % 4] * 8 + ps[-j % 8]
            spread(n, NEAR.index((i, j)), k, other).wait_recv()
            remote(chunk_of(n, k), chunk_of(n, k), last_sems, 0, other).start()
    whole = total_ref.at[pl.ds(theirs, HALF)]
    last = remote(whole, whole, last_sems, 0, other)
    last.wait_recv()

    for copy in (*swaps, *started, last):
        copy.wait_send()
    for n, (at, size) in enumerate(PIECES):
        pieces = held.at[pl.ds(0, (PLANE - 1) * size)]
        pltpu.make_async_remote_copy(
            src_ref=pieces, dst_ref=pieces, send_sem=gather_sems.at[n], recv_sem=spread_sems.at[0],
            device_id=other, device_id_type=MESH,
        ).wait_send()


def gram(trial, resid, energy, shift):
    vmem = pl.BlockSpec(memory_space=pltpu.VMEM)
    hbm = pl.BlockSpec(memory_space=pl.ANY)
    return pl.pallas_call(
        gram_kernel,
        out_shape=(
            pltpu.VMEM((2 * HALF, UNIT, 128), F32),
            pltpu.VMEM((ROWS, KEEP + NEW), BF16),
            pltpu.VMEM((ROWS, KEEP + NEW), BF16),
        ),
        in_specs=[hbm] * 4,
        out_specs=(vmem, vmem, vmem),
        scratch_shapes=[
            pltpu.VMEM((ROWS, KEEP), F32),
            pltpu.VMEM((ROWS, NEW), F32),
            pltpu.VMEM((ROWS // 128, 128), F32),
            pltpu.VMEM((1, NEW), F32),
            pltpu.VMEM((2 * HALF, UNIT, 128), F32),
            pltpu.VMEM((HALF, UNIT, 128), F32),
            pltpu.VMEM(((PLANE - 1) * CHUNK, UNIT, 128), F32),
            pltpu.VMEM((CHUNK, UNIT, 128), F32),
            pltpu.VMEM((LINE * CHUNK, UNIT, 128), F32),
            pltpu.VMEM((CHUNK, UNIT, 128), F32),
            pltpu.SemaphoreType.DMA((2 + 2 * ROWS // STEP,)),
            pltpu.SemaphoreType.DMA((2 * len(PIECES),)),
            pltpu.SemaphoreType.DMA((2 * len(PIECES),)),
            pltpu.SemaphoreType.DMA((2 * len(PIECES),)),
            pltpu.SemaphoreType.DMA((len(PIECES),)),
            pltpu.SemaphoreType.DMA((PLANE * len(PIECES),)),
            pltpu.SemaphoreType.DMA((2,)),
        ],
        compiler_params=pltpu.CompilerParams(
            collective_id=0, has_side_effects=True, vmem_limit_bytes=VMEM_LIMIT
        ),
        name="gram",
    )(trial, resid, energy.reshape(ROWS // 128, 128), shift.reshape(1, NEW))


SIDE = 32


def halves(value):
    high = value.astype(BF16)
    return high, (value - high.astype(F32)).astype(BF16)


def dot(left, right):
    return jnp.dot(left, right, preferred_element_type=F32)


def mul(left, right):
    wide = dot(left[0], jnp.concatenate(right, 1))
    return wide[:, :NEW] + (wide[:, NEW:] + dot(left[1], right[0]))


def square_of(v):
    a, rest = v.astype(BF16), v
    rest = rest - a.astype(F32)
    b = rest.astype(BF16)
    c = (rest - b.astype(F32)).astype(BF16)
    return tdot(jnp.concatenate([a, a, a, b, b, c], 0), jnp.concatenate([a, b, c, a, b, a], 0))


def inverse_factor(square, lane, row):
    tiles = SIDE // 8
    sub = row[:8]
    panels = []
    rest = square
    for base in range(0, NEW, SIDE):
        here = (lane >= base) & (lane < base + SIDE)
        top = rest[:SIDE]
        cols = [
            [jnp.broadcast_to(top[t * 8:t * 8 + 8, base + j:base + j + 1], (8, 128)) if t >= j // 8 else None
             for t in range(tiles)]
            for j in range(SIDE)
        ]
        unit = jnp.where(lane[:SIDE] == row[:SIDE] + base, 1.0, 0.0)
        panel = jnp.where(here[:SIDE], unit, top)
        panel = [panel[t * 8:t * 8 + 8] for t in range(tiles)]
        for k in range(SIDE):
            tk, sk = k // 8, k % 8
            pivot = jnp.broadcast_to(cols[k][tk][sk:sk + 1], (8, 128))
            scale = lax.rsqrt(pivot)
            if k + 1 < SIDE:
                tn, sn = (k + 1) // 8, (k + 1) % 8
                line = jnp.broadcast_to(cols[k][tn][sn:sn + 1], (8, 128))
                ratio = scale * scale
                for t in range(tn, tiles):
                    cols[k + 1][t] = cols[k + 1][t] - (cols[k][t] * line) * ratio
            for t in range(tk, tiles):
                cols[k][t] = cols[k][t] * scale
            line = jnp.broadcast_to(panel[tk][sk:sk + 1], (8, 128)) * scale
            panel[tk] = jnp.where(
                sub == sk, line, panel[tk] - jnp.where(sub > sk, cols[k][tk], 0.0) * line
            )
            for t in range(tk + 1, tiles):
                panel[t] = panel[t] - cols[k][t] * line
            for j in range(k + 2, SIDE):
                line = jnp.broadcast_to(cols[k][j // 8][j % 8:j % 8 + 1], (8, 128))
                for t in range(j // 8, tiles):
                    cols[j][t] = cols[j][t] - cols[k][t] * line
        done = jnp.concatenate(panel, 0)
        panels.append(done)
        if base + SIDE < NEW:
            left = rest.shape[0] - SIDE
            below = jnp.where(here[:left], 0.0, rest[SIDE:])
            rest = below - square_of(done)[base + SIDE:]
    whole = jnp.concatenate(panels, 0)
    return jnp.where(lane <= row, whole, 0.0)


def finish_kernel(count, total_ref, high, low, basis_ref, steady_ref, work, basis, sems):
    at = {
        pair: total_ref[n * 32:(n + 1) * 32].reshape(128, 128) * (1.0 / count) for n, pair in enumerate(PAIRS)
    }
    metric = halves(jnp.concatenate(
        [jnp.concatenate([at[i, j] if i <= j else at[j, i].T for j in range(3)], 1) for i in range(3)], 0
    ))
    first = jnp.concatenate([at[i, 3] for i in range(3)], 0)
    second = mul(metric, halves(first))
    third = mul(metric, halves(second))
    coef = 2.0 * first - second
    image = 2.0 * second - third
    pair = halves(coef)
    known = halves(image - 2.0 * first)
    wide = tdot(pair[0], jnp.concatenate(known, 1))
    square = at[3, 3] + (wide[:, :NEW] + (wide[:, NEW:] + tdot(pair[1], known[0])))

    lane = lax.broadcasted_iota(jnp.int32, (NEW, NEW), 1)
    row = lax.broadcasted_iota(jnp.int32, (NEW, NEW), 0)

    def on_diagonal(v):
        return jnp.sum(jnp.where(lane == row, v, 0.0), axis=0, keepdims=True)

    terms = on_diagonal(at[3, 3]) + jnp.sum(
        jnp.abs(coef) * (2.0 * jnp.abs(first) + jnp.abs(image)), axis=0, keepdims=True
    )
    both = jnp.concatenate(pair, 1)
    for r in range(0, ROWS, 256):
        rows = slice(r, r + 256)
        wide = dot(high[rows, :KEEP], both)
        inside = wide[:, :NEW] + (wide[:, NEW:] + dot(low[rows, :KEEP], pair[0]))
        block = (high[rows, KEEP:].astype(F32) - inside) + low[rows, KEEP:].astype(F32)
        work[rows, :NEW], work[rows, NEW:] = halves(block)

    inverse = inverse_factor(square, lane, row)
    steady = (terms <= 4.0 * on_diagonal(square)) & (on_diagonal(square) * on_diagonal(inverse) ** 2 <= 1000.0)
    steady_ref[0, 0] = jnp.min(jnp.where(steady, 1.0, 0.0))
    inverse = halves(inverse.T)
    stack = jnp.concatenate(
        [jnp.concatenate(inverse, 1), jnp.concatenate([inverse[0], jnp.zeros_like(inverse[0])], 1)], 0
    )
    stores = []
    for n in range(4):
        rows = pl.ds(n * (ROWS // 4), ROWS // 4)
        wide = dot(work[rows, :], stack)
        basis[rows, :] = wide[:, :NEW] + wide[:, NEW:]
        stores.append(pltpu.make_async_copy(basis.at[rows], basis_ref.at[rows], sems.at[n]))
        stores[-1].start()
    for store in stores:
        store.wait()


def finish(total, high, low, count):
    vmem = pl.BlockSpec(memory_space=pltpu.VMEM)
    return pl.pallas_call(
        lambda *refs: finish_kernel(count, *refs),
        out_shape=(jax.ShapeDtypeStruct((ROWS, NEW), F32), pltpu.SMEM((1, 1), F32)),
        in_specs=[vmem] * 3,
        out_specs=(pl.BlockSpec(memory_space=pl.ANY), pl.BlockSpec(memory_space=pltpu.SMEM)),
        scratch_shapes=[
            pltpu.VMEM((ROWS, 2 * NEW), BF16),
            pltpu.VMEM((ROWS, NEW), F32),
            pltpu.SemaphoreType.DMA((4,)),
        ],
        compiler_params=pltpu.CompilerParams(vmem_limit_bytes=VMEM_LIMIT),
        name="finish",
    )(total, high, low)


def in_blocks(x, dim, size):
    before, after = (x.shape[:dim], x.shape[dim + 1 :])
    return jnp.moveaxis(x.reshape(*before, size, -1, *after), dim, 0)


def summed_on_arrival(x, axis, dim):
    parts = in_blocks(x, dim, lax.axis_size(axis))
    arrived = lax.all_to_all(parts, axis, split_axis=0, concat_axis=0, tiled=True)
    return arrived.sum(axis=0)


def sum_by_axis(x, axes, dim):
    far, near = axes
    own = summed_on_arrival(in_blocks(x, dim, lax.axis_size(far)), near, dim + 1)
    return jnp.sum(lax.all_to_all(own, far, 0, 0, tiled=True), axis=0)


def rows_for(lines, size):
    spare = -lines.shape[0] % size
    if not spare:
        return lines
    return jnp.concatenate([lines, jnp.zeros((spare, *lines.shape[1:]), lines.dtype)])


def sent_to_all(x, axis):
    copies = jnp.broadcast_to(x, (lax.axis_size(axis), *x.shape))
    return lax.all_to_all(copies, axis, split_axis=0, concat_axis=0, tiled=True)


def laid_out(parts, dim):
    parts = jnp.moveaxis(parts, 0, dim)
    dims = parts.shape
    return parts.reshape(*dims[:dim], dims[dim] * dims[dim + 1], *dims[dim + 2 :])


def whole_of(x, axes, dim):
    far, near = axes
    first = sent_to_all(x, far)
    parts = jnp.swapaxes(sent_to_all(first, near), 0, 1)
    return laid_out(parts.reshape(-1, *x.shape), dim)


def nested_sum(x, axes):
    own = sum_by_axis(rows_for(x, lax.axis_size(axes[0]) * lax.axis_size(axes[1])), axes, 0)
    whole = whole_of(own, axes, 0)
    return whole[: len(x)].reshape(x.shape)


def fdot(left, right):
    return jnp.dot(left, right, precision=lax.Precision.HIGHEST, preferred_element_type=F32)


def explicit(trial, resid, energy, shift, count):
    def total(v):
        return nested_sum(v.reshape(-1), (("x", "core"), ("y", "z"))).reshape(v.shape)

    work = resid / (energy[:, None] - shift[None, :])
    work = lax.fori_loop(0, 2, lambda _, w: w - fdot(trial, total(fdot(trial.T, w)) / count), work)
    lower = jnp.linalg.cholesky(total(fdot(work.T, work)) / count)
    return jax.scipy.linalg.solve_triangular(lower, work.T, lower=True).T


def per_device(trial, resid, energy, shift):
    count = ROWS * 512
    total, high, low = gram(trial, resid, energy, shift)
    basis, steady = finish(total, high, low, count)
    return lax.cond(
        steady[0, 0] > 0.5, lambda: basis, lambda: explicit(trial, resid, energy, shift, count)
    )


def solution(mesh):
    split = Mesh(mesh.devices.reshape(4, 2, 8, 8), AXES)
    in_specs = (P(AXES, None), P(AXES, None), P(AXES), P())
    return jax.shard_map(
        per_device, mesh=split, in_specs=in_specs, out_specs=P(AXES, None), check_vma=False
    )
```

```python
import jax
import jax.numpy as jnp
from jax import lax
from jax.experimental import pallas as pl
from jax.experimental.pallas import tpu as pltpu
from jax.sharding import Mesh
from jax.sharding import PartitionSpec as P

MESH = pl.DeviceIdType.MESH
AXES = ("x", "core", "y", "z")
ROWS, KEEP, NEW = 1536, 384, 128
STEP = 384
VMEM_LIMIT = 24 * 2**20
UNIT = 4
PAIRS = [(0, 0), (0, 1), (1, 1), (0, 2), (0, 3), (2, 2), (2, 3), (3, 3), (1, 2), (1, 3)]
HALF = len(PAIRS) * 128 // UNIT // 2
PLANE, LINE = 32, 8
PIECES = ((0, 2), (2, 3))
CHUNK = sum(size for _, size in PIECES)
NEAR = [(i, j) for i in range(4) for j in range(8) if (i, j) != (0, 0)]
ARRIVAL = sorted(NEAR, key=lambda o: min(o[0], 4 - o[0]) + min(o[1], 8 - o[1]))
FAR = ARRIVAL[::-1]
F32, BF16 = jnp.float32, jnp.bfloat16


def tdot(a, b):
    return lax.dot_general(a, b, (((0,), (0,)), ((), ())), preferred_element_type=F32)


def gram_kernel(
    trial_ref, resid_ref, energy_ref, shift_ref, total_ref, hi, lo,
    trial, resid, energy, shift, part, peer, held, own, line, done,
    load_sems, core_sems, plane_sems, line_sems, gather_sems, spread_sems, last_sems,
):
    x, c = lax.axis_index("x"), lax.axis_index("core")
    y, z = lax.axis_index("y"), lax.axis_index("z")
    p = (1 - c) * y + c * z
    q = (1 - c) * z + c * y
    me = x * 8 + p
    other = {"x": x, "core": 1 - c, "y": y, "z": z}
    xs = [(x + i) % 4 for i in range(4)]
    ps = [(p + j) % 8 for j in range(8)]
    qs = [(q + j) % 8 for j in range(8)]

    def in_plane(i, j):
        return {"x": xs[i], "core": c, "y": (1 - c) * ps[j] + c * y, "z": (1 - c) * z + c * ps[j]}

    def in_line(j):
        return {"x": x, "core": c, "y": (1 - c) * y + c * qs[j], "z": (1 - c) * qs[j] + c * z}

    barrier = pltpu.get_barrier_semaphore()
    for device in [other] + [in_plane(i, j) for i, j in FAR] + [in_line(j) for j in range(1, 8)]:
        pl.semaphore_signal(barrier, inc=1, device_id=device, device_id_type=MESH)

    loads = [
        pltpu.make_async_copy(energy_ref, energy, load_sems.at[0]),
        pltpu.make_async_copy(shift_ref, shift, load_sems.at[1]),
    ]
    for b in range(ROWS // STEP):
        rows = pl.ds(b * STEP, STEP)
        loads.append(pltpu.make_async_copy(resid_ref.at[rows], resid.at[rows], load_sems.at[2 + 2 * b]))
        loads.append(pltpu.make_async_copy(trial_ref.at[rows], trial.at[rows], load_sems.at[3 + 2 * b]))
    for load in loads:
        load.start()

    for b in range(ROWS // STEP):
        for load in loads[2 * b + 2:2 * b + 4] + (loads[:2] if b == 0 else []):
            load.wait()
        for r in range(b * STEP, (b + 1) * STEP, 128):
            rows = pl.ds(r, 128)
            gap = jnp.broadcast_to(energy[pl.ds(r // 128, 1), :], (128, 128)).T - shift[...]
            for at, value in ((slice(0, KEEP), trial[rows, :]), (slice(KEEP, KEEP + NEW), resid[rows, :] / gap)):
                high = value.astype(BF16)
                hi[rows, at] = high
                lo[rows, at] = (value - high.astype(F32)).astype(BF16)

    def half(h):
        wide = pl.ds(pl.multiple_of(h * 256, 256), 256)
        thin = pl.ds(pl.multiple_of(h * 128, 128), 128)
        left = hi[:, wide]
        cross = tdot(left, lo[:, wide])
        full = tdot(left, left) + (cross + cross.T)
        left = hi[:, thin]
        side = tdot(left, hi[:, 256:]) + (tdot(left, lo[:, 256:]) + tdot(lo[:, thin], hi[:, 256:]))
        blocks = (full[:128, :128], full[:128, 128:], full[128:, 128:], side[:, :128], side[:, 128:])
        for n, block in enumerate(blocks):
            part[pl.ds(h * HALF + n * 32, 32)] = block.reshape(32, UNIT, 128)

    def remote(src, dst, sems, n, device):
        return pltpu.make_async_remote_copy(
            src_ref=src, dst_ref=dst, send_sem=sems.at[2 * n], recv_sem=sems.at[2 * n + 1],
            device_id=device, device_id_type=MESH,
        )

    mine, theirs = c * HALF, (1 - c) * HALF
    started = []
    half(1 - c)
    pl.semaphore_wait(barrier, PLANE + LINE - 1)
    swaps = [
        remote(
            part.at[pl.ds(theirs + at * PLANE, size * PLANE)], peer.at[pl.ds(at * PLANE, size * PLANE)],
            core_sems, n, other,
        )
        for n, (at, size) in enumerate(PIECES)
    ]
    for swap in swaps:
        swap.start()
    half(c)
    for n, (at, size) in enumerate(PIECES):
        swaps[n].wait_recv()
        peer[at * PLANE:(at + size) * PLANE] += part[pl.ds(mine + at * PLANE, size * PLANE)]
        for m, (i, j) in enumerate(FAR):
            k = xs[i] * 8 + ps[j]
            remote(
                peer.at[pl.ds(at * PLANE + k * size, size)], held.at[pl.ds(at * (PLANE - 1) + m * size, size)],
                plane_sems, n, in_plane(i, j),
            ).start()

    for n, (at, size) in enumerate(PIECES):
        base = at * (PLANE - 1)
        pieces = held.at[pl.ds(base, (PLANE - 1) * size)]
        started.append(remote(pieces, pieces, plane_sems, n, other))
        started[-1].wait_recv()
        total = peer[pl.ds(at * PLANE + me * size, size)]
        for m in range(PLANE - 1):
            total += held[base + m * size:base + (m + 1) * size]
        own[at:at + size] = total
        spot = pl.ds(at * LINE + q * size, size)
        line[spot] = total
        for j in (4, 3, 5, 2, 6, 1, 7):
            remote(own.at[pl.ds(at, size)], line.at[spot], line_sems, n, in_line(j)).start()

    def chunk_of(n, k):
        at, size = PIECES[n]
        return total_ref.at[pl.ds(mine + at * PLANE + k * size, size)]

    def spread(n, m, k, device):
        return pltpu.make_async_remote_copy(
            src_ref=done.at[pl.ds(*PIECES[n])], dst_ref=chunk_of(n, k),
            send_sem=gather_sems.at[n], recv_sem=spread_sems.at[n * PLANE + m],
            device_id=device, device_id_type=MESH,
        )

    for n, (at, size) in enumerate(PIECES):
        lines = line.at[pl.ds(at * LINE, (LINE - 1) * size)]
        started.append(remote(lines, lines, line_sems, n, other))
        started[-1].wait_recv()
        total = line[at * LINE:at * LINE + size]
        for j in range(1, LINE):
            total += line[at * LINE + j * size:at * LINE + (j + 1) * size]
        done[at:at + size] = total
        total_ref[pl.ds(mine + at * PLANE + me * size, size)] = total
        for m, (i, j) in enumerate(NEAR):
            spread(n, m, me, in_plane(i, j)).start()
        remote(done.at[pl.ds(at, size)], chunk_of(n, me), last_sems, 0, other).start()

    for n in range(len(PIECES)):
        for i, j in ARRIVAL:
            k = xs[-i % 4] * 8 + ps[-j % 8]
            spread(n, NEAR.index((i, j)), k, other).wait_recv()
            remote(chunk_of(n, k), chunk_of(n, k), last_sems, 0, other).start()
    whole = total_ref.at[pl.ds(theirs, HALF)]
    last = remote(whole, whole, last_sems, 0, other)
    last.wait_recv()

    for copy in (*swaps, *started, last):
        copy.wait_send()
    for n, (at, size) in enumerate(PIECES):
        pieces = held.at[pl.ds(0, (PLANE - 1) * size)]
        pltpu.make_async_remote_copy(
            src_ref=pieces, dst_ref=pieces, send_sem=gather_sems.at[n], recv_sem=spread_sems.at[0],
            device_id=other, device_id_type=MESH,
        ).wait_send()


def gram(trial, resid, energy, shift):
    vmem = pl.BlockSpec(memory_space=pltpu.VMEM)
    hbm = pl.BlockSpec(memory_space=pl.ANY)
    return pl.pallas_call(
        gram_kernel,
        out_shape=(
            pltpu.VMEM((2 * HALF, UNIT, 128), F32),
            pltpu.VMEM((ROWS, KEEP + NEW), BF16),
            pltpu.VMEM((ROWS, KEEP + NEW), BF16),
        ),
        in_specs=[hbm] * 4,
        out_specs=(vmem, vmem, vmem),
        scratch_shapes=[
            pltpu.VMEM((ROWS, KEEP), F32),
            pltpu.VMEM((ROWS, NEW), F32),
            pltpu.VMEM((ROWS // 128, 128), F32),
            pltpu.VMEM((1, NEW), F32),
            pltpu.VMEM((2 * HALF, UNIT, 128), F32),
            pltpu.VMEM((HALF, UNIT, 128), F32),
            pltpu.VMEM(((PLANE - 1) * CHUNK, UNIT, 128), F32),
            pltpu.VMEM((CHUNK, UNIT, 128), F32),
            pltpu.VMEM((LINE * CHUNK, UNIT, 128), F32),
            pltpu.VMEM((CHUNK, UNIT, 128), F32),
            pltpu.SemaphoreType.DMA((2 + 2 * ROWS // STEP,)),
            pltpu.SemaphoreType.DMA((2 * len(PIECES),)),
            pltpu.SemaphoreType.DMA((2 * len(PIECES),)),
            pltpu.SemaphoreType.DMA((2 * len(PIECES),)),
            pltpu.SemaphoreType.DMA((len(PIECES),)),
            pltpu.SemaphoreType.DMA((PLANE * len(PIECES),)),
            pltpu.SemaphoreType.DMA((2,)),
        ],
        compiler_params=pltpu.CompilerParams(
            collective_id=0, has_side_effects=True, vmem_limit_bytes=VMEM_LIMIT
        ),
        name="gram",
    )(trial, resid, energy.reshape(ROWS // 128, 128), shift.reshape(1, NEW))


SIDE = 16


def halves(value):
    high = value.astype(BF16)
    return high, (value - high.astype(F32)).astype(BF16)


def dot(left, right):
    return jnp.dot(left, right, preferred_element_type=F32)


def mul(left, right):
    wide = dot(left[0], jnp.concatenate(right, 1))
    return wide[:, :NEW] + (wide[:, NEW:] + dot(left[1], right[0]))


def square_of(v):
    a, rest = v.astype(BF16), v
    rest = rest - a.astype(F32)
    b = rest.astype(BF16)
    c = (rest - b.astype(F32)).astype(BF16)
    return tdot(jnp.concatenate([a, a, a, b, b, c], 0), jnp.concatenate([a, b, c, a, b, a], 0))


def inverse_factor(square, lane, row):
    lane, sub = lane[:8], row[:8]
    count, own = NEW // 8, SIDE // 8
    tiles = [square[t * 8:t * 8 + 8] for t in range(count)]
    for first in range(0, count, own):
        base, window = first * 8, range(min(2 * own, count - first))
        here = (lane >= base) & (lane < base + SIDE)
        cols = [
            [jnp.broadcast_to(tiles[first + t][:, base + j:base + j + 1], (8, 128)) if t >= j // 8 else None
             for t in window]
            for j in range(SIDE)
        ]
        panel = [
            jnp.where(here, jnp.where(lane == sub + base + 8 * t, 1.0, 0.0) if t < own else 0.0, tiles[first + t])
            for t in window
        ]
        for k in range(SIDE):
            tk, sk = k // 8, k % 8
            pivot = jnp.broadcast_to(cols[k][tk][sk:sk + 1], (8, 128))
            scale = lax.rsqrt(pivot)
            if k + 1 < SIDE:
                tn, sn = (k + 1) // 8, (k + 1) % 8
                line = jnp.broadcast_to(cols[k][tn][sn:sn + 1], (8, 128))
                ratio = scale * scale
                for t in window[tn:]:
                    cols[k + 1][t] = cols[k + 1][t] - (cols[k][t] * line) * ratio
            for t in window[tk:]:
                cols[k][t] = cols[k][t] * scale
            line = jnp.broadcast_to(panel[tk][sk:sk + 1], (8, 128)) * scale
            panel[tk] = jnp.where(
                sub == sk, line, panel[tk] - jnp.where(sub > sk, cols[k][tk], 0.0) * line
            )
            for t in window[tk + 1:]:
                panel[t] = panel[t] - cols[k][t] * line
            for j in range(k + 2, SIDE):
                line = jnp.broadcast_to(cols[k][j // 8][j % 8:j % 8 + 1], (8, 128))
                for t in window[j // 8:]:
                    cols[j][t] = cols[j][t] - cols[k][t] * line
        tiles[first:first + len(window)] = panel
        if first + 2 * own < count:
            update = square_of(jnp.concatenate(panel[:own], 0))
            for t in range(first + 2 * own, count):
                tiles[t] = jnp.where(here, 0.0, tiles[t]) - update[t * 8:t * 8 + 8]
    return jnp.where(lane[:1] <= row[:, :1], jnp.concatenate(tiles, 0), 0.0)


def finish_kernel(count, total_ref, high, low, basis_ref, steady_ref, work, basis, sems):
    at = {
        pair: total_ref[n * 32:(n + 1) * 32].reshape(128, 128) * (1.0 / count) for n, pair in enumerate(PAIRS)
    }
    metric = halves(jnp.concatenate(
        [jnp.concatenate([at[i, j] if i <= j else at[j, i].T for j in range(3)], 1) for i in range(3)], 0
    ))
    first = jnp.concatenate([at[i, 3] for i in range(3)], 0)
    second = mul(metric, halves(first))
    third = mul(metric, halves(second))
    coef = 2.0 * first - second
    image = 2.0 * second - third
    pair = halves(coef)
    known = halves(image - 2.0 * first)
    wide = tdot(pair[0], jnp.concatenate(known, 1))
    square = at[3, 3] + (wide[:, :NEW] + (wide[:, NEW:] + tdot(pair[1], known[0])))

    lane = lax.broadcasted_iota(jnp.int32, (NEW, NEW), 1)
    row = lax.broadcasted_iota(jnp.int32, (NEW, NEW), 0)

    def on_diagonal(v):
        return jnp.sum(jnp.where(lane == row, v, 0.0), axis=0, keepdims=True)

    terms = on_diagonal(at[3, 3]) + jnp.sum(
        jnp.abs(coef) * (2.0 * jnp.abs(first) + jnp.abs(image)), axis=0, keepdims=True
    )
    inverse = inverse_factor(square, lane, row)

    both = jnp.concatenate(pair, 1)
    for r in range(0, ROWS, 256):
        rows = slice(r, r + 256)
        wide = dot(high[rows, :KEEP], both)
        inside = wide[:, :NEW] + (wide[:, NEW:] + dot(low[rows, :KEEP], pair[0]))
        block = (high[rows, KEEP:].astype(F32) - inside) + low[rows, KEEP:].astype(F32)
        work[rows, :NEW], work[rows, NEW:] = halves(block)

    steady = (terms <= 4.0 * on_diagonal(square)) & (on_diagonal(square) * on_diagonal(inverse) ** 2 <= 1000.0)
    steady_ref[0, 0] = jnp.min(jnp.where(steady, 1.0, 0.0))
    inverse = halves(inverse.T)
    stack = jnp.concatenate(
        [jnp.concatenate(inverse, 1), jnp.concatenate([inverse[0], jnp.zeros_like(inverse[0])], 1)], 0
    )
    stores = []
    for n in range(4):
        rows = pl.ds(n * (ROWS // 4), ROWS // 4)
        wide = dot(work[rows, :], stack)
        basis[rows, :] = wide[:, :NEW] + wide[:, NEW:]
        stores.append(pltpu.make_async_copy(basis.at[rows], basis_ref.at[rows], sems.at[n]))
        stores[-1].start()
    for store in stores:
        store.wait()


def finish(total, high, low, count):
    vmem = pl.BlockSpec(memory_space=pltpu.VMEM)
    return pl.pallas_call(
        lambda *refs: finish_kernel(count, *refs),
        out_shape=(jax.ShapeDtypeStruct((ROWS, NEW), F32), pltpu.SMEM((1, 1), F32)),
        in_specs=[vmem] * 3,
        out_specs=(pl.BlockSpec(memory_space=pl.ANY), pl.BlockSpec(memory_space=pltpu.SMEM)),
        scratch_shapes=[
            pltpu.VMEM((ROWS, 2 * NEW), BF16),
            pltpu.VMEM((ROWS, NEW), F32),
            pltpu.SemaphoreType.DMA((4,)),
        ],
        compiler_params=pltpu.CompilerParams(vmem_limit_bytes=VMEM_LIMIT),
        name="finish",
    )(total, high, low)


def in_blocks(x, dim, size):
    before, after = (x.shape[:dim], x.shape[dim + 1 :])
    return jnp.moveaxis(x.reshape(*before, size, -1, *after), dim, 0)


def summed_on_arrival(x, axis, dim):
    parts = in_blocks(x, dim, lax.axis_size(axis))
    arrived = lax.all_to_all(parts, axis, split_axis=0, concat_axis=0, tiled=True)
    return arrived.sum(axis=0)


def sum_by_axis(x, axes, dim):
    far, near = axes
    own = summed_on_arrival(in_blocks(x, dim, lax.axis_size(far)), near, dim + 1)
    return jnp.sum(lax.all_to_all(own, far, 0, 0, tiled=True), axis=0)


def rows_for(lines, size):
    spare = -lines.shape[0] % size
    if not spare:
        return lines
    return jnp.concatenate([lines, jnp.zeros((spare, *lines.shape[1:]), lines.dtype)])


def sent_to_all(x, axis):
    copies = jnp.broadcast_to(x, (lax.axis_size(axis), *x.shape))
    return lax.all_to_all(copies, axis, split_axis=0, concat_axis=0, tiled=True)


def laid_out(parts, dim):
    parts = jnp.moveaxis(parts, 0, dim)
    dims = parts.shape
    return parts.reshape(*dims[:dim], dims[dim] * dims[dim + 1], *dims[dim + 2 :])


def whole_of(x, axes, dim):
    far, near = axes
    first = sent_to_all(x, far)
    parts = jnp.swapaxes(sent_to_all(first, near), 0, 1)
    return laid_out(parts.reshape(-1, *x.shape), dim)


def nested_sum(x, axes):
    own = sum_by_axis(rows_for(x, lax.axis_size(axes[0]) * lax.axis_size(axes[1])), axes, 0)
    whole = whole_of(own, axes, 0)
    return whole[: len(x)].reshape(x.shape)


def fdot(left, right):
    return jnp.dot(left, right, precision=lax.Precision.HIGHEST, preferred_element_type=F32)


def explicit(trial, resid, energy, shift, count):
    def total(v):
        return nested_sum(v.reshape(-1), (("x", "core"), ("y", "z"))).reshape(v.shape)

    work = resid / (energy[:, None] - shift[None, :])
    work = lax.fori_loop(0, 2, lambda _, w: w - fdot(trial, total(fdot(trial.T, w)) / count), work)
    lower = jnp.linalg.cholesky(total(fdot(work.T, work)) / count)
    return jax.scipy.linalg.solve_triangular(lower, work.T, lower=True).T


def per_device(trial, resid, energy, shift):
    count = ROWS * 512
    total, high, low = gram(trial, resid, energy, shift)
    basis, steady = finish(total, high, low, count)
    return lax.cond(
        steady[0, 0] > 0.5, lambda: basis, lambda: explicit(trial, resid, energy, shift, count)
    )


def solution(mesh):
    split = Mesh(mesh.devices.reshape(4, 2, 8, 8), AXES)
    in_specs = (P(AXES, None), P(AXES, None), P(AXES), P())
    return jax.shard_map(
        per_device, mesh=split, in_specs=in_specs, out_specs=P(AXES, None), check_vma=False
    )
```

```python
import jax
import jax.numpy as jnp
from jax import lax
from jax.experimental import pallas as pl
from jax.experimental.pallas import tpu as pltpu
from jax.sharding import Mesh
from jax.sharding import PartitionSpec as P

MESH = pl.DeviceIdType.MESH
AXES = ("x", "core", "y", "z")
ROWS, KEEP, NEW = 1536, 384, 128
STEP = 384
VMEM_LIMIT = 24 * 2**20
UNIT = 4
MAIN = 4 * 128 // UNIT
HALF = MAIN + 1
PLANE, LINE = 32, 8
PIECES = ((0, 2), (2, 2))
CHUNK = MAIN // PLANE
NEAR = [(i, j) for i in range(4) for j in range(8) if (i, j) != (0, 0)]
ARRIVAL = sorted(NEAR, key=lambda o: min(o[0], 4 - o[0]) + min(o[1], 8 - o[1]))
FAR = ARRIVAL[::-1]
F32, BF16 = jnp.float32, jnp.bfloat16


def tdot(a, b):
    return lax.dot_general(a, b, (((0,), (0,)), ((), ())), preferred_element_type=F32)


def gram_kernel(
    trial_ref, resid_ref, energy_ref, shift_ref, total_ref, hi, lo,
    trial, resid, energy, shift, part, peer, held, own, line, done,
    load_sems, core_sems, plane_sems, line_sems, gather_sems, spread_sems, last_sems,
    held_extra, own_extra, line_extra, done_extra, extra_sems,
):
    x, c = lax.axis_index("x"), lax.axis_index("core")
    y, z = lax.axis_index("y"), lax.axis_index("z")
    p = (1 - c) * y + c * z
    q = (1 - c) * z + c * y
    me = x * 8 + p
    other = {"x": x, "core": 1 - c, "y": y, "z": z}
    xs = [(x + i) % 4 for i in range(4)]
    ps = [(p + j) % 8 for j in range(8)]
    qs = [(q + j) % 8 for j in range(8)]

    def in_plane(i, j):
        return {"x": xs[i], "core": c, "y": (1 - c) * ps[j] + c * y, "z": (1 - c) * z + c * ps[j]}

    def in_line(j):
        return {"x": x, "core": c, "y": (1 - c) * y + c * qs[j], "z": (1 - c) * qs[j] + c * z}

    barrier = pltpu.get_barrier_semaphore()
    for device in [other] + [in_plane(i, j) for i, j in FAR] + [in_line(j) for j in range(1, 8)]:
        pl.semaphore_signal(barrier, inc=1, device_id=device, device_id_type=MESH)

    loads = [
        pltpu.make_async_copy(energy_ref, energy, load_sems.at[0]),
        pltpu.make_async_copy(shift_ref, shift, load_sems.at[1]),
    ]
    for b in range(ROWS // STEP):
        rows = pl.ds(b * STEP, STEP)
        loads.append(pltpu.make_async_copy(resid_ref.at[rows], resid.at[rows], load_sems.at[2 + 2 * b]))
        loads.append(pltpu.make_async_copy(trial_ref.at[rows], trial.at[rows], load_sems.at[3 + 2 * b]))
    for load in loads:
        load.start()

    for b in range(ROWS // STEP):
        for load in loads[2 * b + 2:2 * b + 4] + (loads[:2] if b == 0 else []):
            load.wait()
        for r in range(b * STEP, (b + 1) * STEP, 128):
            rows = pl.ds(r, 128)
            gap = jnp.broadcast_to(energy[pl.ds(r // 128, 1), :], (128, 128)).T - shift[...]
            for at, value in ((slice(0, KEEP), trial[rows, :]), (slice(KEEP, KEEP + NEW), resid[rows, :] / gap)):
                high = value.astype(BF16)
                hi[rows, at] = high
                lo[rows, at] = (value - high.astype(F32)).astype(BF16)

    def half(h):
        wide = pl.ds(pl.multiple_of(h * 256, 256), 256)
        thin = pl.ds(pl.multiple_of(h * 128, 128), 128)
        left = hi[:, wide]
        cross = tdot(left, lo[:, wide])
        full = tdot(left, left) + (cross + cross.T)
        left = hi[:, thin]
        side = tdot(left, hi[:, 256:]) + (tdot(left, lo[:, 256:]) + tdot(lo[:, thin], hi[:, 256:]))
        lane = lax.broadcasted_iota(jnp.int32, (128, 128), 1)
        row = lax.broadcasted_iota(jnp.int32, (128, 128), 0)
        packed = jnp.where(lane >= row, full[:128, :128], full[128:, 128:])
        diagonal = jnp.sum(jnp.where(lane == row, full[128:, 128:], 0.0), axis=0, keepdims=True)
        part[pl.ds(h * HALF + MAIN, 1)] = jnp.broadcast_to(diagonal, (UNIT, 128)).reshape(1, UNIT, 128)
        blocks = (packed, full[:128, 128:], side[:, :128], side[:, 128:])
        for n, block in enumerate(blocks):
            part[pl.ds(h * HALF + n * 32, 32)] = block.reshape(32, UNIT, 128)

    def remote(src, dst, sems, n, device):
        return pltpu.make_async_remote_copy(
            src_ref=src, dst_ref=dst, send_sem=sems.at[2 * n], recv_sem=sems.at[2 * n + 1],
            device_id=device, device_id_type=MESH,
        )

    mine, theirs = c * HALF, (1 - c) * HALF
    started = []
    half(1 - c)
    pl.semaphore_wait(barrier, PLANE + LINE - 1)
    swaps = [
        remote(
            part.at[pl.ds(theirs + at * PLANE, size * PLANE + n)], peer.at[pl.ds(at * PLANE, size * PLANE + n)],
            core_sems, n, other,
        )
        for n, (at, size) in enumerate(PIECES)
    ]
    for swap in swaps:
        swap.start()
    half(c)
    for n, (at, size) in enumerate(PIECES):
        swaps[n].wait_recv()
        peer[at * PLANE:(at + size) * PLANE + n] += part[pl.ds(mine + at * PLANE, size * PLANE + n)]
        for m, (i, j) in enumerate(FAR):
            k = xs[i] * 8 + ps[j]
            remote(
                peer.at[pl.ds(at * PLANE + k * size, size)], held.at[pl.ds(at * (PLANE - 1) + m * size, size)],
                plane_sems, n, in_plane(i, j),
            ).start()

    spot_extra = total_ref.at[pl.ds(mine + MAIN, 1)]
    to_first = remote(
        peer.at[pl.ds(MAIN, 1)], held_extra.at[pl.ds((me + PLANE - 1) % PLANE, 1)], extra_sems, 0,
        {"x": 0, "core": c, "y": c * y, "z": (1 - c) * z},
    )

    @pl.when(me != 0)
    def _():
        to_first.start()

    for n, (at, size) in enumerate(PIECES):
        base = at * (PLANE - 1)
        pieces = held.at[pl.ds(base, (PLANE - 1) * size)]
        started.append(remote(pieces, pieces, plane_sems, n, other))
        started[-1].wait_recv()
        total = peer[pl.ds(at * PLANE + me * size, size)]
        for m in range(PLANE - 1):
            total += held[base + m * size:base + (m + 1) * size]
        own[at:at + size] = total
        spot = pl.ds(at * LINE + q * size, size)
        line[spot] = total
        for j in (4, 3, 5, 2, 6, 1, 7):
            remote(own.at[pl.ds(at, size)], line.at[spot], line_sems, n, in_line(j)).start()

    all_extra = held_extra.at[pl.ds(0, PLANE - 1)]
    lines_extra = line_extra.at[pl.ds(0, LINE - 1)]

    @pl.when(me == 0)
    def _():
        remote(all_extra, all_extra, extra_sems, 0, other).wait_recv()
        total = peer[MAIN:MAIN + 1]
        for m in range(PLANE - 1):
            total += held_extra[m:m + 1]
        own_extra[...] = total
        line_extra[pl.ds(q, 1)] = total
        for j in range(1, LINE):
            remote(own_extra, line_extra.at[pl.ds(q, 1)], extra_sems, 1, in_line(j)).start()

    def chunk_of(n, k):
        at, size = PIECES[n]
        return total_ref.at[pl.ds(mine + at * PLANE + k * size, size)]

    def spread(n, m, k, device):
        return pltpu.make_async_remote_copy(
            src_ref=done.at[pl.ds(*PIECES[n])], dst_ref=chunk_of(n, k),
            send_sem=gather_sems.at[n], recv_sem=spread_sems.at[n * PLANE + m],
            device_id=device, device_id_type=MESH,
        )

    for n, (at, size) in enumerate(PIECES):
        lines = line.at[pl.ds(at * LINE, (LINE - 1) * size)]
        started.append(remote(lines, lines, line_sems, n, other))
        started[-1].wait_recv()
        total = line[at * LINE:at * LINE + size]
        for j in range(1, LINE):
            total += line[at * LINE + j * size:at * LINE + (j + 1) * size]
        done[at:at + size] = total
        total_ref[pl.ds(mine + at * PLANE + me * size, size)] = total
        for m, (i, j) in enumerate(NEAR):
            spread(n, m, me, in_plane(i, j)).start()
        remote(done.at[pl.ds(at, size)], chunk_of(n, me), last_sems, 0, other).start()

    @pl.when(me == 0)
    def _():
        remote(lines_extra, lines_extra, extra_sems, 1, other).wait_recv()
        total = line_extra[0:1]
        for j in range(1, LINE):
            total += line_extra[j:j + 1]
        done_extra[...] = total
        total_ref[pl.ds(mine + MAIN, 1)] = total
        for i, j in NEAR:
            remote(done_extra, spot_extra, extra_sems, 2, in_plane(i, j)).start()
        remote(done_extra, spot_extra, last_sems, 0, other).start()

    for n in range(len(PIECES)):
        for i, j in ARRIVAL:
            k = xs[-i % 4] * 8 + ps[-j % 8]
            spread(n, NEAR.index((i, j)), k, other).wait_recv()
            remote(chunk_of(n, k), chunk_of(n, k), last_sems, 0, other).start()

    @pl.when(me != 0)
    def _():
        remote(done_extra, spot_extra, extra_sems, 2, other).wait_recv()
        remote(spot_extra, spot_extra, last_sems, 0, other).start()

    whole = total_ref.at[pl.ds(theirs, HALF)]
    last = remote(whole, whole, last_sems, 0, other)
    last.wait_recv()

    for copy in (*swaps, *started, last):
        copy.wait_send()
    @pl.when(me != 0)
    def _():
        to_first.wait_send()

    @pl.when(me == 0)
    def _():
        remote(lines_extra, lines_extra, extra_sems, 1, other).wait_send()
        remote(all_extra, all_extra, extra_sems, 2, other).wait_send()

    for n, (at, size) in enumerate(PIECES):
        pieces = held.at[pl.ds(0, (PLANE - 1) * size)]
        pltpu.make_async_remote_copy(
            src_ref=pieces, dst_ref=pieces, send_sem=gather_sems.at[n], recv_sem=spread_sems.at[0],
            device_id=other, device_id_type=MESH,
        ).wait_send()


def gram(trial, resid, energy, shift):
    vmem = pl.BlockSpec(memory_space=pltpu.VMEM)
    hbm = pl.BlockSpec(memory_space=pl.ANY)
    return pl.pallas_call(
        gram_kernel,
        out_shape=(
            pltpu.VMEM((2 * HALF, UNIT, 128), F32),
            pltpu.VMEM((ROWS, KEEP + NEW), BF16),
            pltpu.VMEM((ROWS, KEEP + NEW), BF16),
        ),
        in_specs=[hbm] * 4,
        out_specs=(vmem, vmem, vmem),
        scratch_shapes=[
            pltpu.VMEM((ROWS, KEEP), F32),
            pltpu.VMEM((ROWS, NEW), F32),
            pltpu.VMEM((ROWS // 128, 128), F32),
            pltpu.VMEM((1, NEW), F32),
            pltpu.VMEM((2 * HALF, UNIT, 128), F32),
            pltpu.VMEM((HALF, UNIT, 128), F32),
            pltpu.VMEM(((PLANE - 1) * CHUNK, UNIT, 128), F32),
            pltpu.VMEM((CHUNK, UNIT, 128), F32),
            pltpu.VMEM((LINE * CHUNK, UNIT, 128), F32),
            pltpu.VMEM((CHUNK, UNIT, 128), F32),
            pltpu.SemaphoreType.DMA((2 + 2 * ROWS // STEP,)),
            pltpu.SemaphoreType.DMA((2 * len(PIECES),)),
            pltpu.SemaphoreType.DMA((2 * len(PIECES),)),
            pltpu.SemaphoreType.DMA((2 * len(PIECES),)),
            pltpu.SemaphoreType.DMA((len(PIECES),)),
            pltpu.SemaphoreType.DMA((PLANE * len(PIECES),)),
            pltpu.SemaphoreType.DMA((2,)),
            pltpu.VMEM((PLANE, UNIT, 128), F32),
            pltpu.VMEM((1, UNIT, 128), F32),
            pltpu.VMEM((LINE, UNIT, 128), F32),
            pltpu.VMEM((1, UNIT, 128), F32),
            pltpu.SemaphoreType.DMA((6,)),
        ],
        compiler_params=pltpu.CompilerParams(
            collective_id=0, has_side_effects=True, vmem_limit_bytes=VMEM_LIMIT
        ),
        name="gram",
    )(trial, resid, energy.reshape(ROWS // 128, 128), shift.reshape(1, NEW))


SIDE = 16


def halves(value):
    high = value.astype(BF16)
    return high, (value - high.astype(F32)).astype(BF16)


def dot(left, right):
    return jnp.dot(left, right, preferred_element_type=F32)


def mul(left, right):
    wide = dot(left[0], jnp.concatenate(right, 1))
    return wide[:, :NEW] + (wide[:, NEW:] + dot(left[1], right[0]))


def square_of(v):
    a, rest = v.astype(BF16), v
    rest = rest - a.astype(F32)
    b = rest.astype(BF16)
    c = (rest - b.astype(F32)).astype(BF16)
    return tdot(jnp.concatenate([a, a, a, b, b, c], 0), jnp.concatenate([a, b, c, a, b, a], 0))


def inverse_factor(square, lane, row):
    lane, sub = lane[:8], row[:8]
    count, own = NEW // 8, SIDE // 8
    tiles = [square[t * 8:t * 8 + 8] for t in range(count)]
    for first in range(0, count, own):
        base, window = first * 8, range(min(2 * own, count - first))
        here = (lane >= base) & (lane < base + SIDE)
        cols = [
            [jnp.broadcast_to(tiles[first + t][:, base + j:base + j + 1], (8, 128)) if t >= j // 8 else None
             for t in window]
            for j in range(SIDE)
        ]
        panel = [
            jnp.where(here, jnp.where(lane == sub + base + 8 * t, 1.0, 0.0) if t < own else 0.0, tiles[first + t])
            for t in window
        ]
        for k in range(SIDE):
            tk, sk = k // 8, k % 8
            pivot = jnp.broadcast_to(cols[k][tk][sk:sk + 1], (8, 128))
            scale = lax.rsqrt(pivot)
            if k + 1 < SIDE:
                tn, sn = (k + 1) // 8, (k + 1) % 8
                line = jnp.broadcast_to(cols[k][tn][sn:sn + 1], (8, 128))
                ratio = scale * scale
                for t in window[tn:]:
                    cols[k + 1][t] = cols[k + 1][t] - (cols[k][t] * line) * ratio
            for t in window[tk:]:
                cols[k][t] = cols[k][t] * scale
            line = jnp.broadcast_to(panel[tk][sk:sk + 1], (8, 128)) * scale
            panel[tk] = jnp.where(
                sub == sk, line, panel[tk] - jnp.where(sub > sk, cols[k][tk], 0.0) * line
            )
            for t in window[tk + 1:]:
                panel[t] = panel[t] - cols[k][t] * line
            for j in range(k + 2, SIDE):
                line = jnp.broadcast_to(cols[k][j // 8][j % 8:j % 8 + 1], (8, 128))
                for t in window[j // 8:]:
                    cols[j][t] = cols[j][t] - cols[k][t] * line
        tiles[first:first + len(window)] = panel
        if first + 2 * own < count:
            update = square_of(jnp.concatenate(panel[:own], 0))
            for t in range(first + 2 * own, count):
                tiles[t] = jnp.where(here, 0.0, tiles[t]) - update[t * 8:t * 8 + 8]
    return jnp.where(lane[:1] <= row[:, :1], jnp.concatenate(tiles, 0), 0.0)


def finish_kernel(count, total_ref, high, low, basis_ref, steady_ref, work, basis, sems):
    lane = lax.broadcasted_iota(jnp.int32, (NEW, NEW), 1)
    row = lax.broadcasted_iota(jnp.int32, (NEW, NEW), 0)
    at = {}
    for h in range(2):
        packed, *others = [
            total_ref[h * HALF + n * 32:h * HALF + n * 32 + 32].reshape(128, 128) * (1.0 / count) for n in range(4)
        ]
        diagonal = total_ref[h * HALF + MAIN, 0:1, :] * (1.0 / count)
        turned = packed.T
        at[2 * h, 2 * h] = jnp.where(lane >= row, packed, turned)
        at[2 * h + 1, 2 * h + 1] = jnp.where(lane < row, packed, jnp.where(lane > row, turned, diagonal))
        at[2 * h, 2 * h + 1], at[h, 2], at[h, 3] = others
    metric = halves(jnp.concatenate(
        [jnp.concatenate([at[i, j] if i <= j else at[j, i].T for j in range(3)], 1) for i in range(3)], 0
    ))
    first = jnp.concatenate([at[i, 3] for i in range(3)], 0)
    second = mul(metric, halves(first))
    third = mul(metric, halves(second))
    coef = 2.0 * first - second
    image = 2.0 * second - third
    pair = halves(coef)
    known = halves(image - 2.0 * first)
    wide = tdot(pair[0], jnp.concatenate(known, 1))
    square = at[3, 3] + (wide[:, :NEW] + (wide[:, NEW:] + tdot(pair[1], known[0])))

    def on_diagonal(v):
        return jnp.sum(jnp.where(lane == row, v, 0.0), axis=0, keepdims=True)

    terms = on_diagonal(at[3, 3]) + jnp.sum(
        jnp.abs(coef) * (2.0 * jnp.abs(first) + jnp.abs(image)), axis=0, keepdims=True
    )
    inverse = inverse_factor(square, lane, row)

    both = jnp.concatenate(pair, 1)
    for r in range(0, ROWS, 256):
        rows = slice(r, r + 256)
        wide = dot(high[rows, :KEEP], both)
        inside = wide[:, :NEW] + (wide[:, NEW:] + dot(low[rows, :KEEP], pair[0]))
        block = (high[rows, KEEP:].astype(F32) - inside) + low[rows, KEEP:].astype(F32)
        work[rows, :NEW], work[rows, NEW:] = halves(block)

    steady = (terms <= 4.0 * on_diagonal(square)) & (on_diagonal(square) * on_diagonal(inverse) ** 2 <= 1000.0)
    steady_ref[0, 0] = jnp.min(jnp.where(steady, 1.0, 0.0))
    inverse = halves(inverse.T)
    stack = jnp.concatenate(
        [jnp.concatenate(inverse, 1), jnp.concatenate([inverse[0], jnp.zeros_like(inverse[0])], 1)], 0
    )
    stores = []
    for n in range(4):
        rows = pl.ds(n * (ROWS // 4), ROWS // 4)
        wide = dot(work[rows, :], stack)
        basis[rows, :] = wide[:, :NEW] + wide[:, NEW:]
        stores.append(pltpu.make_async_copy(basis.at[rows], basis_ref.at[rows], sems.at[n]))
        stores[-1].start()
    for store in stores:
        store.wait()


def finish(total, high, low, count):
    vmem = pl.BlockSpec(memory_space=pltpu.VMEM)
    return pl.pallas_call(
        lambda *refs: finish_kernel(count, *refs),
        out_shape=(jax.ShapeDtypeStruct((ROWS, NEW), F32), pltpu.SMEM((1, 1), F32)),
        in_specs=[vmem] * 3,
        out_specs=(pl.BlockSpec(memory_space=pl.ANY), pl.BlockSpec(memory_space=pltpu.SMEM)),
        scratch_shapes=[
            pltpu.VMEM((ROWS, 2 * NEW), BF16),
            pltpu.VMEM((ROWS, NEW), F32),
            pltpu.SemaphoreType.DMA((4,)),
        ],
        compiler_params=pltpu.CompilerParams(vmem_limit_bytes=VMEM_LIMIT),
        name="finish",
    )(total, high, low)


def in_blocks(x, dim, size):
    before, after = (x.shape[:dim], x.shape[dim + 1 :])
    return jnp.moveaxis(x.reshape(*before, size, -1, *after), dim, 0)


def summed_on_arrival(x, axis, dim):
    parts = in_blocks(x, dim, lax.axis_size(axis))
    arrived = lax.all_to_all(parts, axis, split_axis=0, concat_axis=0, tiled=True)
    return arrived.sum(axis=0)


def sum_by_axis(x, axes, dim):
    far, near = axes
    own = summed_on_arrival(in_blocks(x, dim, lax.axis_size(far)), near, dim + 1)
    return jnp.sum(lax.all_to_all(own, far, 0, 0, tiled=True), axis=0)


def rows_for(lines, size):
    spare = -lines.shape[0] % size
    if not spare:
        return lines
    return jnp.concatenate([lines, jnp.zeros((spare, *lines.shape[1:]), lines.dtype)])


def sent_to_all(x, axis):
    copies = jnp.broadcast_to(x, (lax.axis_size(axis), *x.shape))
    return lax.all_to_all(copies, axis, split_axis=0, concat_axis=0, tiled=True)


def laid_out(parts, dim):
    parts = jnp.moveaxis(parts, 0, dim)
    dims = parts.shape
    return parts.reshape(*dims[:dim], dims[dim] * dims[dim + 1], *dims[dim + 2 :])


def whole_of(x, axes, dim):
    far, near = axes
    first = sent_to_all(x, far)
    parts = jnp.swapaxes(sent_to_all(first, near), 0, 1)
    return laid_out(parts.reshape(-1, *x.shape), dim)


def nested_sum(x, axes):
    own = sum_by_axis(rows_for(x, lax.axis_size(axes[0]) * lax.axis_size(axes[1])), axes, 0)
    whole = whole_of(own, axes, 0)
    return whole[: len(x)].reshape(x.shape)


def fdot(left, right):
    return jnp.dot(left, right, precision=lax.Precision.HIGHEST, preferred_element_type=F32)


def explicit(trial, resid, energy, shift, count):
    def total(v):
        return nested_sum(v.reshape(-1), (("x", "core"), ("y", "z"))).reshape(v.shape)

    work = resid / (energy[:, None] - shift[None, :])
    work = lax.fori_loop(0, 2, lambda _, w: w - fdot(trial, total(fdot(trial.T, w)) / count), work)
    lower = jnp.linalg.cholesky(total(fdot(work.T, work)) / count)
    return jax.scipy.linalg.solve_triangular(lower, work.T, lower=True).T


def per_device(trial, resid, energy, shift):
    count = ROWS * 512
    total, high, low = gram(trial, resid, energy, shift)
    basis, steady = finish(total, high, low, count)
    return lax.cond(
        steady[0, 0] > 0.5, lambda: basis, lambda: explicit(trial, resid, energy, shift, count)
    )


def solution(mesh):
    split = Mesh(mesh.devices.reshape(4, 2, 8, 8), AXES)
    in_specs = (P(AXES, None), P(AXES, None), P(AXES), P())
    return jax.shard_map(
        per_device, mesh=split, in_specs=in_specs, out_specs=P(AXES, None), check_vma=False
    )
```

```python
import jax
import jax.numpy as jnp
from jax import lax
from jax.experimental import pallas as pl
from jax.experimental.pallas import tpu as pltpu
from jax.sharding import Mesh
from jax.sharding import PartitionSpec as P

MESH = pl.DeviceIdType.MESH
AXES = ("x", "core", "y", "z")
ROWS, KEEP, NEW = 1536, 384, 128
STEP = 384
VMEM_LIMIT = 24 * 2**20
UNIT = 8
BLOCK = 128 // UNIT
MAIN = 4 * BLOCK
HALF = MAIN + 1
PLANE, LINE = 32, 8
PIECES = ((0, 1), (1, 1))
CHUNK = MAIN // PLANE
NEAR = [(i, j) for i in range(4) for j in range(8) if (i, j) != (0, 0)]
ARRIVAL = sorted(NEAR, key=lambda o: min(o[0], 4 - o[0]) + min(o[1], 8 - o[1]))
FAR = ARRIVAL[::-1]
F32, BF16 = jnp.float32, jnp.bfloat16


def tdot(a, b):
    return lax.dot_general(a, b, (((0,), (0,)), ((), ())), preferred_element_type=F32)


def gram_kernel(
    trial_ref, resid_ref, energy_ref, shift_ref, total_ref, hi, lo,
    trial, resid, energy, shift, part, peer, held, own, line, done,
    load_sems, core_sems, plane_sems, line_sems, gather_sems, spread_sems, last_sems,
    held_extra, own_extra, line_extra, done_extra, extra_sems,
):
    x, c = lax.axis_index("x"), lax.axis_index("core")
    y, z = lax.axis_index("y"), lax.axis_index("z")
    p = (1 - c) * y + c * z
    q = (1 - c) * z + c * y
    me = x * 8 + p
    other = {"x": x, "core": 1 - c, "y": y, "z": z}
    xs = [(x + i) % 4 for i in range(4)]
    ps = [(p + j) % 8 for j in range(8)]
    qs = [(q + j) % 8 for j in range(8)]

    def in_plane(i, j):
        return {"x": xs[i], "core": c, "y": (1 - c) * ps[j] + c * y, "z": (1 - c) * z + c * ps[j]}

    def in_line(j):
        return {"x": x, "core": c, "y": (1 - c) * y + c * qs[j], "z": (1 - c) * qs[j] + c * z}

    barrier = pltpu.get_barrier_semaphore()
    for device in [other] + [in_plane(i, j) for i, j in FAR] + [in_line(j) for j in range(1, 8)]:
        pl.semaphore_signal(barrier, inc=1, device_id=device, device_id_type=MESH)

    loads = [
        pltpu.make_async_copy(energy_ref, energy, load_sems.at[0]),
        pltpu.make_async_copy(shift_ref, shift, load_sems.at[1]),
    ]
    for b in range(ROWS // STEP):
        rows = pl.ds(b * STEP, STEP)
        loads.append(pltpu.make_async_copy(resid_ref.at[rows], resid.at[rows], load_sems.at[2 + 2 * b]))
        loads.append(pltpu.make_async_copy(trial_ref.at[rows], trial.at[rows], load_sems.at[3 + 2 * b]))
    for load in loads:
        load.start()

    for b in range(ROWS // STEP):
        for load in loads[2 * b + 2:2 * b + 4] + (loads[:2] if b == 0 else []):
            load.wait()
        for r in range(b * STEP, (b + 1) * STEP, 128):
            rows = pl.ds(r, 128)
            gap = jnp.broadcast_to(energy[pl.ds(r // 128, 1), :], (128, 128)).T - shift[...]
            for at, value in ((slice(0, KEEP), trial[rows, :]), (slice(KEEP, KEEP + NEW), resid[rows, :] / gap)):
                high = value.astype(BF16)
                hi[rows, at] = high
                lo[rows, at] = (value - high.astype(F32)).astype(BF16)

    def half(h):
        wide = pl.ds(pl.multiple_of(h * 256, 256), 256)
        thin = pl.ds(pl.multiple_of(h * 128, 128), 128)
        left = hi[:, wide]
        cross = tdot(left, lo[:, wide])
        full = tdot(left, left) + (cross + cross.T)
        left = hi[:, thin]
        side = tdot(left, hi[:, 256:]) + (tdot(left, lo[:, 256:]) + tdot(lo[:, thin], hi[:, 256:]))
        lane = lax.broadcasted_iota(jnp.int32, (128, 128), 1)
        row = lax.broadcasted_iota(jnp.int32, (128, 128), 0)
        packed = jnp.where(lane >= row, full[:128, :128], full[128:, 128:])
        diagonal = jnp.sum(jnp.where(lane == row, full[128:, 128:], 0.0), axis=0, keepdims=True)
        part[pl.ds(h * HALF + MAIN, 1)] = jnp.broadcast_to(diagonal, (UNIT, 128)).reshape(1, UNIT, 128)
        blocks = (packed, full[:128, 128:], side[:, :128], side[:, 128:])
        for n, block in enumerate(blocks):
            part[pl.ds(h * HALF + n * BLOCK, BLOCK)] = block.reshape(BLOCK, UNIT, 128)

    def remote(src, dst, sems, n, device):
        return pltpu.make_async_remote_copy(
            src_ref=src, dst_ref=dst, send_sem=sems.at[2 * n], recv_sem=sems.at[2 * n + 1],
            device_id=device, device_id_type=MESH,
        )

    mine, theirs = c * HALF, (1 - c) * HALF
    started = []
    half(1 - c)
    pl.semaphore_wait(barrier, PLANE + LINE - 1)
    swaps = [
        remote(
            part.at[pl.ds(theirs + at * PLANE, size * PLANE + n)], peer.at[pl.ds(at * PLANE, size * PLANE + n)],
            core_sems, n, other,
        )
        for n, (at, size) in enumerate(PIECES)
    ]
    for swap in swaps:
        swap.start()
    half(c)
    for n, (at, size) in enumerate(PIECES):
        swaps[n].wait_recv()
        peer[at * PLANE:(at + size) * PLANE + n] += part[pl.ds(mine + at * PLANE, size * PLANE + n)]
        for m, (i, j) in enumerate(FAR):
            k = xs[i] * 8 + ps[j]
            remote(
                peer.at[pl.ds(at * PLANE + k * size, size)], held.at[pl.ds(at * (PLANE - 1) + m * size, size)],
                plane_sems, n, in_plane(i, j),
            ).start()

    spot_extra = total_ref.at[pl.ds(mine + MAIN, 1)]
    to_first = remote(
        peer.at[pl.ds(MAIN, 1)], held_extra.at[pl.ds((me + PLANE - 1) % PLANE, 1)], extra_sems, 0,
        {"x": 0, "core": c, "y": c * y, "z": (1 - c) * z},
    )

    @pl.when(me != 0)
    def _():
        to_first.start()

    for n, (at, size) in enumerate(PIECES):
        base = at * (PLANE - 1)
        pieces = held.at[pl.ds(base, (PLANE - 1) * size)]
        started.append(remote(pieces, pieces, plane_sems, n, other))
        started[-1].wait_recv()
        total = peer[pl.ds(at * PLANE + me * size, size)]
        for m in range(PLANE - 1):
            total += held[base + m * size:base + (m + 1) * size]
        own[at:at + size] = total
        spot = pl.ds(at * LINE + q * size, size)
        line[spot] = total
        for j in (4, 3, 5, 2, 6, 1, 7):
            remote(own.at[pl.ds(at, size)], line.at[spot], line_sems, n, in_line(j)).start()

    all_extra = held_extra.at[pl.ds(0, PLANE - 1)]
    lines_extra = line_extra.at[pl.ds(0, LINE - 1)]

    @pl.when(me == 0)
    def _():
        remote(all_extra, all_extra, extra_sems, 0, other).wait_recv()
        total = peer[MAIN:MAIN + 1]
        for m in range(PLANE - 1):
            total += held_extra[m:m + 1]
        own_extra[...] = total
        line_extra[pl.ds(q, 1)] = total
        for j in range(1, LINE):
            remote(own_extra, line_extra.at[pl.ds(q, 1)], extra_sems, 1, in_line(j)).start()

    def chunk_of(n, k):
        at, size = PIECES[n]
        return total_ref.at[pl.ds(mine + at * PLANE + k * size, size)]

    def spread(n, m, k, device):
        return pltpu.make_async_remote_copy(
            src_ref=done.at[pl.ds(*PIECES[n])], dst_ref=chunk_of(n, k),
            send_sem=gather_sems.at[n], recv_sem=spread_sems.at[n * PLANE + m],
            device_id=device, device_id_type=MESH,
        )

    for n, (at, size) in enumerate(PIECES):
        lines = line.at[pl.ds(at * LINE, (LINE - 1) * size)]
        started.append(remote(lines, lines, line_sems, n, other))
        started[-1].wait_recv()
        total = line[at * LINE:at * LINE + size]
        for j in range(1, LINE):
            total += line[at * LINE + j * size:at * LINE + (j + 1) * size]
        done[at:at + size] = total
        total_ref[pl.ds(mine + at * PLANE + me * size, size)] = total
        for m, (i, j) in enumerate(NEAR):
            spread(n, m, me, in_plane(i, j)).start()
        remote(done.at[pl.ds(at, size)], chunk_of(n, me), last_sems, 0, other).start()

    @pl.when(me == 0)
    def _():
        remote(lines_extra, lines_extra, extra_sems, 1, other).wait_recv()
        total = line_extra[0:1]
        for j in range(1, LINE):
            total += line_extra[j:j + 1]
        done_extra[...] = total
        total_ref[pl.ds(mine + MAIN, 1)] = total
        for i, j in NEAR:
            remote(done_extra, spot_extra, extra_sems, 2, in_plane(i, j)).start()
        remote(done_extra, spot_extra, last_sems, 0, other).start()

    for n in range(len(PIECES)):
        for i, j in ARRIVAL:
            k = xs[-i % 4] * 8 + ps[-j % 8]
            spread(n, NEAR.index((i, j)), k, other).wait_recv()
            remote(chunk_of(n, k), chunk_of(n, k), last_sems, 0, other).start()

    @pl.when(me != 0)
    def _():
        remote(done_extra, spot_extra, extra_sems, 2, other).wait_recv()
        remote(spot_extra, spot_extra, last_sems, 0, other).start()

    whole = total_ref.at[pl.ds(theirs, HALF)]
    last = remote(whole, whole, last_sems, 0, other)
    last.wait_recv()

    for copy in (*swaps, *started, last):
        copy.wait_send()
    @pl.when(me != 0)
    def _():
        to_first.wait_send()

    @pl.when(me == 0)
    def _():
        remote(lines_extra, lines_extra, extra_sems, 1, other).wait_send()
        remote(all_extra, all_extra, extra_sems, 2, other).wait_send()

    for n, (at, size) in enumerate(PIECES):
        pieces = held.at[pl.ds(0, (PLANE - 1) * size)]
        pltpu.make_async_remote_copy(
            src_ref=pieces, dst_ref=pieces, send_sem=gather_sems.at[n], recv_sem=spread_sems.at[0],
            device_id=other, device_id_type=MESH,
        ).wait_send()


def gram(trial, resid, energy, shift):
    vmem = pl.BlockSpec(memory_space=pltpu.VMEM)
    hbm = pl.BlockSpec(memory_space=pl.ANY)
    return pl.pallas_call(
        gram_kernel,
        out_shape=(
            pltpu.VMEM((2 * HALF, UNIT, 128), F32),
            pltpu.VMEM((ROWS, KEEP + NEW), BF16),
            pltpu.VMEM((ROWS, KEEP + NEW), BF16),
        ),
        in_specs=[hbm] * 4,
        out_specs=(vmem, vmem, vmem),
        scratch_shapes=[
            pltpu.VMEM((ROWS, KEEP), F32),
            pltpu.VMEM((ROWS, NEW), F32),
            pltpu.VMEM((ROWS // 128, 128), F32),
            pltpu.VMEM((1, NEW), F32),
            pltpu.VMEM((2 * HALF, UNIT, 128), F32),
            pltpu.VMEM((HALF, UNIT, 128), F32),
            pltpu.VMEM(((PLANE - 1) * CHUNK, UNIT, 128), F32),
            pltpu.VMEM((CHUNK, UNIT, 128), F32),
            pltpu.VMEM((LINE * CHUNK, UNIT, 128), F32),
            pltpu.VMEM((CHUNK, UNIT, 128), F32),
            pltpu.SemaphoreType.DMA((2 + 2 * ROWS // STEP,)),
            pltpu.SemaphoreType.DMA((2 * len(PIECES),)),
            pltpu.SemaphoreType.DMA((2 * len(PIECES),)),
            pltpu.SemaphoreType.DMA((2 * len(PIECES),)),
            pltpu.SemaphoreType.DMA((len(PIECES),)),
            pltpu.SemaphoreType.DMA((PLANE * len(PIECES),)),
            pltpu.SemaphoreType.DMA((2,)),
            pltpu.VMEM((PLANE, UNIT, 128), F32),
            pltpu.VMEM((1, UNIT, 128), F32),
            pltpu.VMEM((LINE, UNIT, 128), F32),
            pltpu.VMEM((1, UNIT, 128), F32),
            pltpu.SemaphoreType.DMA((6,)),
        ],
        compiler_params=pltpu.CompilerParams(
            collective_id=0, has_side_effects=True, vmem_limit_bytes=VMEM_LIMIT
        ),
        name="gram",
    )(trial, resid, energy.reshape(ROWS // 128, 128), shift.reshape(1, NEW))


SIDE = 16


def halves(value):
    high = value.astype(BF16)
    return high, (value - high.astype(F32)).astype(BF16)


def dot(left, right):
    return jnp.dot(left, right, preferred_element_type=F32)


def mul(left, right):
    wide = dot(left[0], jnp.concatenate(right, 1))
    return wide[:, :NEW] + (wide[:, NEW:] + dot(left[1], right[0]))


def square_of(v):
    a, rest = v.astype(BF16), v
    rest = rest - a.astype(F32)
    b = rest.astype(BF16)
    c = (rest - b.astype(F32)).astype(BF16)
    return tdot(jnp.concatenate([a, a, a, b, b, c], 0), jnp.concatenate([a, b, c, a, b, a], 0))


def inverse_factor(square, lane, row):
    lane, sub = lane[:8], row[:8]
    count, own = NEW // 8, SIDE // 8
    tiles = [square[t * 8:t * 8 + 8] for t in range(count)]
    for first in range(0, count, own):
        base, window = first * 8, range(min(2 * own, count - first))
        here = (lane >= base) & (lane < base + SIDE)
        cols = [
            [jnp.broadcast_to(tiles[first + t][:, base + j:base + j + 1], (8, 128)) if t >= j // 8 else None
             for t in window]
            for j in range(SIDE)
        ]
        panel = [
            jnp.where(here, jnp.where(lane == sub + base + 8 * t, 1.0, 0.0) if t < own else 0.0, tiles[first + t])
            for t in window
        ]
        for k in range(SIDE):
            tk, sk = k // 8, k % 8
            pivot = jnp.broadcast_to(cols[k][tk][sk:sk + 1], (8, 128))
            scale = lax.rsqrt(pivot)
            if k + 1 < SIDE:
                tn, sn = (k + 1) // 8, (k + 1) % 8
                line = jnp.broadcast_to(cols[k][tn][sn:sn + 1], (8, 128))
                ratio = scale * scale
                for t in window[tn:]:
                    cols[k + 1][t] = cols[k + 1][t] - (cols[k][t] * line) * ratio
            for t in window[tk:]:
                cols[k][t] = cols[k][t] * scale
            line = jnp.broadcast_to(panel[tk][sk:sk + 1], (8, 128)) * scale
            panel[tk] = jnp.where(
                sub == sk, line, panel[tk] - jnp.where(sub > sk, cols[k][tk], 0.0) * line
            )
            for t in window[tk + 1:]:
                panel[t] = panel[t] - cols[k][t] * line
            for j in range(k + 2, SIDE):
                line = jnp.broadcast_to(cols[k][j // 8][j % 8:j % 8 + 1], (8, 128))
                for t in window[j // 8:]:
                    cols[j][t] = cols[j][t] - cols[k][t] * line
        tiles[first:first + len(window)] = panel
        if first + 2 * own < count:
            update = square_of(jnp.concatenate(panel[:own], 0))
            for t in range(first + 2 * own, count):
                tiles[t] = jnp.where(here, 0.0, tiles[t]) - update[t * 8:t * 8 + 8]
    return jnp.where(lane[:1] <= row[:, :1], jnp.concatenate(tiles, 0), 0.0)


def finish_kernel(count, total_ref, high, low, basis_ref, steady_ref, work, basis, sems):
    lane = lax.broadcasted_iota(jnp.int32, (NEW, NEW), 1)
    row = lax.broadcasted_iota(jnp.int32, (NEW, NEW), 0)
    at = {}
    for h in range(2):
        packed, *others = [
            total_ref[h * HALF + n * BLOCK:h * HALF + (n + 1) * BLOCK].reshape(128, 128) * (1.0 / count)
            for n in range(4)
        ]
        diagonal = total_ref[h * HALF + MAIN, 0:1, :] * (1.0 / count)
        turned = packed.T
        at[2 * h, 2 * h] = jnp.where(lane >= row, packed, turned)
        at[2 * h + 1, 2 * h + 1] = jnp.where(lane < row, packed, jnp.where(lane > row, turned, diagonal))
        at[2 * h, 2 * h + 1], at[h, 2], at[h, 3] = others
    metric = halves(jnp.concatenate(
        [jnp.concatenate([at[i, j] if i <= j else at[j, i].T for j in range(3)], 1) for i in range(3)], 0
    ))
    first = jnp.concatenate([at[i, 3] for i in range(3)], 0)
    second = mul(metric, halves(first))
    third = mul(metric, halves(second))
    coef = 2.0 * first - second
    image = 2.0 * second - third
    pair = halves(coef)
    known = halves(image - 2.0 * first)
    wide = tdot(pair[0], jnp.concatenate(known, 1))
    square = at[3, 3] + (wide[:, :NEW] + (wide[:, NEW:] + tdot(pair[1], known[0])))

    def on_diagonal(v):
        return jnp.sum(jnp.where(lane == row, v, 0.0), axis=0, keepdims=True)

    terms = on_diagonal(at[3, 3]) + jnp.sum(
        jnp.abs(coef) * (2.0 * jnp.abs(first) + jnp.abs(image)), axis=0, keepdims=True
    )
    inverse = inverse_factor(square, lane, row)

    both = jnp.concatenate(pair, 1)
    for r in range(0, ROWS, 256):
        rows = slice(r, r + 256)
        wide = dot(high[rows, :KEEP], both)
        inside = wide[:, :NEW] + (wide[:, NEW:] + dot(low[rows, :KEEP], pair[0]))
        block = (high[rows, KEEP:].astype(F32) - inside) + low[rows, KEEP:].astype(F32)
        work[rows, :NEW], work[rows, NEW:] = halves(block)

    steady = (terms <= 4.0 * on_diagonal(square)) & (on_diagonal(square) * on_diagonal(inverse) ** 2 <= 1000.0)
    steady_ref[0, 0] = jnp.min(jnp.where(steady, 1.0, 0.0))
    inverse = halves(inverse.T)
    stack = jnp.concatenate(
        [jnp.concatenate(inverse, 1), jnp.concatenate([inverse[0], jnp.zeros_like(inverse[0])], 1)], 0
    )
    stores = []
    for n in range(4):
        rows = pl.ds(n * (ROWS // 4), ROWS // 4)
        wide = dot(work[rows, :], stack)
        basis[rows, :] = wide[:, :NEW] + wide[:, NEW:]
        stores.append(pltpu.make_async_copy(basis.at[rows], basis_ref.at[rows], sems.at[n]))
        stores[-1].start()
    for store in stores:
        store.wait()


def finish(total, high, low, count):
    vmem = pl.BlockSpec(memory_space=pltpu.VMEM)
    return pl.pallas_call(
        lambda *refs: finish_kernel(count, *refs),
        out_shape=(jax.ShapeDtypeStruct((ROWS, NEW), F32), pltpu.SMEM((1, 1), F32)),
        in_specs=[vmem] * 3,
        out_specs=(pl.BlockSpec(memory_space=pl.ANY), pl.BlockSpec(memory_space=pltpu.SMEM)),
        scratch_shapes=[
            pltpu.VMEM((ROWS, 2 * NEW), BF16),
            pltpu.VMEM((ROWS, NEW), F32),
            pltpu.SemaphoreType.DMA((4,)),
        ],
        compiler_params=pltpu.CompilerParams(vmem_limit_bytes=VMEM_LIMIT),
        name="finish",
    )(total, high, low)


def in_blocks(x, dim, size):
    before, after = (x.shape[:dim], x.shape[dim + 1 :])
    return jnp.moveaxis(x.reshape(*before, size, -1, *after), dim, 0)


def summed_on_arrival(x, axis, dim):
    parts = in_blocks(x, dim, lax.axis_size(axis))
    arrived = lax.all_to_all(parts, axis, split_axis=0, concat_axis=0, tiled=True)
    return arrived.sum(axis=0)


def sum_by_axis(x, axes, dim):
    far, near = axes
    own = summed_on_arrival(in_blocks(x, dim, lax.axis_size(far)), near, dim + 1)
    return jnp.sum(lax.all_to_all(own, far, 0, 0, tiled=True), axis=0)


def rows_for(lines, size):
    spare = -lines.shape[0] % size
    if not spare:
        return lines
    return jnp.concatenate([lines, jnp.zeros((spare, *lines.shape[1:]), lines.dtype)])


def sent_to_all(x, axis):
    copies = jnp.broadcast_to(x, (lax.axis_size(axis), *x.shape))
    return lax.all_to_all(copies, axis, split_axis=0, concat_axis=0, tiled=True)


def laid_out(parts, dim):
    parts = jnp.moveaxis(parts, 0, dim)
    dims = parts.shape
    return parts.reshape(*dims[:dim], dims[dim] * dims[dim + 1], *dims[dim + 2 :])


def whole_of(x, axes, dim):
    far, near = axes
    first = sent_to_all(x, far)
    parts = jnp.swapaxes(sent_to_all(first, near), 0, 1)
    return laid_out(parts.reshape(-1, *x.shape), dim)


def nested_sum(x, axes):
    own = sum_by_axis(rows_for(x, lax.axis_size(axes[0]) * lax.axis_size(axes[1])), axes, 0)
    whole = whole_of(own, axes, 0)
    return whole[: len(x)].reshape(x.shape)


def fdot(left, right):
    return jnp.dot(left, right, precision=lax.Precision.HIGHEST, preferred_element_type=F32)


def explicit(trial, resid, energy, shift, count):
    def total(v):
        return nested_sum(v.reshape(-1), (("x", "core"), ("y", "z"))).reshape(v.shape)

    work = resid / (energy[:, None] - shift[None, :])
    work = lax.fori_loop(0, 2, lambda _, w: w - fdot(trial, total(fdot(trial.T, w)) / count), work)
    lower = jnp.linalg.cholesky(total(fdot(work.T, work)) / count)
    return jax.scipy.linalg.solve_triangular(lower, work.T, lower=True).T


def per_device(trial, resid, energy, shift):
    count = ROWS * 512
    total, high, low = gram(trial, resid, energy, shift)
    basis, steady = finish(total, high, low, count)
    return lax.cond(
        steady[0, 0] > 0.5, lambda: basis, lambda: explicit(trial, resid, energy, shift, count)
    )


def solution(mesh):
    split = Mesh(mesh.devices.reshape(4, 2, 8, 8), AXES)
    in_specs = (P(AXES, None), P(AXES, None), P(AXES), P())
    return jax.shard_map(
        per_device, mesh=split, in_specs=in_specs, out_specs=P(AXES, None), check_vma=False
    )
```

```python
import jax
import jax.numpy as jnp
from jax import lax
from jax.experimental import pallas as pl
from jax.experimental.pallas import tpu as pltpu
from jax.sharding import Mesh
from jax.sharding import PartitionSpec as P

MESH = pl.DeviceIdType.MESH
AXES = ("x", "core", "y", "z")
ROWS, KEEP, NEW = 1536, 384, 128
STEP = 384
VMEM_LIMIT = 24 * 2**20
UNIT = 8
BLOCK = 128 // UNIT
MAIN = 4 * BLOCK
HALF = MAIN + 1
PLANE, LINE = 32, 8
PIECES = ((0, 1), (1, 1))
CHUNK = MAIN // PLANE
NEAR = [(i, j) for i in range(4) for j in range(8) if (i, j) != (0, 0)]
ARRIVAL = sorted(NEAR, key=lambda o: min(o[0], 4 - o[0]) + min(o[1], 8 - o[1]))
FAR = ARRIVAL[::-1]
F32, BF16 = jnp.float32, jnp.bfloat16


def tdot(a, b):
    return lax.dot_general(a, b, (((0,), (0,)), ((), ())), preferred_element_type=F32)


def gram_kernel(
    trial_ref, resid_ref, energy_ref, shift_ref, total_ref, hi, lo,
    trial, resid, energy, shift, part, peer, held, own, line, done,
    load_sems, core_sems, plane_sems, line_sems, gather_sems, spread_sems, last_sems,
    held_extra, own_extra, line_extra, done_extra, extra_sems,
):
    x, c = lax.axis_index("x"), lax.axis_index("core")
    y, z = lax.axis_index("y"), lax.axis_index("z")
    p = (1 - c) * y + c * z
    q = (1 - c) * z + c * y
    me = x * 8 + p
    other = {"x": x, "core": 1 - c, "y": y, "z": z}
    xs = [(x + i) % 4 for i in range(4)]
    ps = [(p + j) % 8 for j in range(8)]
    qs = [(q + j) % 8 for j in range(8)]

    def in_plane(i, j):
        return {"x": xs[i], "core": c, "y": (1 - c) * ps[j] + c * y, "z": (1 - c) * z + c * ps[j]}

    def in_line(j):
        return {"x": x, "core": c, "y": (1 - c) * y + c * qs[j], "z": (1 - c) * qs[j] + c * z}

    barrier = pltpu.get_barrier_semaphore()
    for device in [other] + [in_plane(i, j) for i, j in FAR] + [in_line(j) for j in range(1, 8)]:
        pl.semaphore_signal(barrier, inc=1, device_id=device, device_id_type=MESH)

    loads = [
        pltpu.make_async_copy(energy_ref, energy, load_sems.at[0]),
        pltpu.make_async_copy(shift_ref, shift, load_sems.at[1]),
    ]
    for b in range(ROWS // STEP):
        rows = pl.ds(b * STEP, STEP)
        loads.append(pltpu.make_async_copy(resid_ref.at[rows], resid.at[rows], load_sems.at[2 + 2 * b]))
        loads.append(pltpu.make_async_copy(trial_ref.at[rows], trial.at[rows], load_sems.at[3 + 2 * b]))
    for load in loads:
        load.start()

    for b in range(ROWS // STEP):
        for load in loads[2 * b + 2:2 * b + 4] + (loads[:2] if b == 0 else []):
            load.wait()
        for r in range(b * STEP, (b + 1) * STEP, 128):
            rows = pl.ds(r, 128)
            gap = jnp.broadcast_to(energy[pl.ds(r // 128, 1), :], (128, 128)).T - shift[...]
            for at, value in ((slice(0, KEEP), trial[rows, :]), (slice(KEEP, KEEP + NEW), resid[rows, :] / gap)):
                high = value.astype(BF16)
                hi[rows, at] = high
                lo[rows, at] = (value - high.astype(F32)).astype(BF16)

    def half(h):
        wide = pl.ds(pl.multiple_of(h * 256, 256), 256)
        thin = pl.ds(pl.multiple_of(h * 128, 128), 128)
        left = hi[:, wide]
        cross = tdot(left, lo[:, wide])
        full = tdot(left, left) + (cross + cross.T)
        left = hi[:, thin]
        side = tdot(left, hi[:, 256:]) + (tdot(left, lo[:, 256:]) + tdot(lo[:, thin], hi[:, 256:]))
        lane = lax.broadcasted_iota(jnp.int32, (128, 128), 1)
        row = lax.broadcasted_iota(jnp.int32, (128, 128), 0)
        packed = jnp.where(lane >= row, full[:128, :128], full[128:, 128:])
        diagonal = jnp.sum(jnp.where(lane == row, full[128:, 128:], 0.0), axis=0, keepdims=True)
        part[pl.ds(h * HALF + MAIN, 1)] = jnp.broadcast_to(diagonal, (UNIT, 128)).reshape(1, UNIT, 128)
        blocks = (packed, full[:128, 128:], side[:, :128], side[:, 128:])
        for n, block in enumerate(blocks):
            part[pl.ds(h * HALF + n * BLOCK, BLOCK)] = block.reshape(BLOCK, UNIT, 128)

    def remote(src, dst, sems, n, device):
        return pltpu.make_async_remote_copy(
            src_ref=src, dst_ref=dst, send_sem=sems.at[2 * n], recv_sem=sems.at[2 * n + 1],
            device_id=device, device_id_type=MESH,
        )

    mine, theirs = c * HALF, (1 - c) * HALF
    started = []
    half(1 - c)
    half(c)
    pl.semaphore_wait(barrier, PLANE + LINE - 1)
    swaps = [
        remote(
            part.at[pl.ds(theirs + at * PLANE, size * PLANE + n)], peer.at[pl.ds(at * PLANE, size * PLANE + n)],
            core_sems, n, other,
        )
        for n, (at, size) in enumerate(PIECES)
    ]
    for swap in swaps:
        swap.start()
    for n, (at, size) in enumerate(PIECES):
        swaps[n].wait_recv()
        peer[at * PLANE:(at + size) * PLANE + n] += part[pl.ds(mine + at * PLANE, size * PLANE + n)]
        for m, (i, j) in enumerate(FAR):
            k = xs[i] * 8 + ps[j]
            remote(
                peer.at[pl.ds(at * PLANE + k * size, size)], held.at[pl.ds(at * (PLANE - 1) + m * size, size)],
                plane_sems, n, in_plane(i, j),
            ).start()

    spot_extra = total_ref.at[pl.ds(mine + MAIN, 1)]
    to_first = remote(
        peer.at[pl.ds(MAIN, 1)], held_extra.at[pl.ds((me + PLANE - 1) % PLANE, 1)], extra_sems, 0,
        {"x": 0, "core": c, "y": c * y, "z": (1 - c) * z},
    )

    @pl.when(me != 0)
    def _():
        to_first.start()

    for n, (at, size) in enumerate(PIECES):
        base = at * (PLANE - 1)
        pieces = held.at[pl.ds(base, (PLANE - 1) * size)]
        started.append(remote(pieces, pieces, plane_sems, n, other))
        started[-1].wait_recv()
        total = peer[pl.ds(at * PLANE + me * size, size)]
        for m in range(PLANE - 1):
            total += held[base + m * size:base + (m + 1) * size]
        own[at:at + size] = total
        spot = pl.ds(at * LINE + q * size, size)
        line[spot] = total
        for j in (4, 3, 5, 2, 6, 1, 7):
            remote(own.at[pl.ds(at, size)], line.at[spot], line_sems, n, in_line(j)).start()

    all_extra = held_extra.at[pl.ds(0, PLANE - 1)]
    lines_extra = line_extra.at[pl.ds(0, LINE - 1)]

    @pl.when(me == 0)
    def _():
        remote(all_extra, all_extra, extra_sems, 0, other).wait_recv()
        total = peer[MAIN:MAIN + 1]
        for m in range(PLANE - 1):
            total += held_extra[m:m + 1]
        own_extra[...] = total
        line_extra[pl.ds(q, 1)] = total
        for j in range(1, LINE):
            remote(own_extra, line_extra.at[pl.ds(q, 1)], extra_sems, 1, in_line(j)).start()

    def chunk_of(n, k):
        at, size = PIECES[n]
        return total_ref.at[pl.ds(mine + at * PLANE + k * size, size)]

    def spread(n, m, k, device):
        return pltpu.make_async_remote_copy(
            src_ref=done.at[pl.ds(*PIECES[n])], dst_ref=chunk_of(n, k),
            send_sem=gather_sems.at[n], recv_sem=spread_sems.at[n * PLANE + m],
            device_id=device, device_id_type=MESH,
        )

    for n, (at, size) in enumerate(PIECES):
        lines = line.at[pl.ds(at * LINE, (LINE - 1) * size)]
        started.append(remote(lines, lines, line_sems, n, other))
        started[-1].wait_recv()
        total = line[at * LINE:at * LINE + size]
        for j in range(1, LINE):
            total += line[at * LINE + j * size:at * LINE + (j + 1) * size]
        done[at:at + size] = total
        total_ref[pl.ds(mine + at * PLANE + me * size, size)] = total
        for m, (i, j) in enumerate(NEAR):
            spread(n, m, me, in_plane(i, j)).start()
        remote(done.at[pl.ds(at, size)], chunk_of(n, me), last_sems, 0, other).start()

    @pl.when(me == 0)
    def _():
        remote(lines_extra, lines_extra, extra_sems, 1, other).wait_recv()
        total = line_extra[0:1]
        for j in range(1, LINE):
            total += line_extra[j:j + 1]
        done_extra[...] = total
        total_ref[pl.ds(mine + MAIN, 1)] = total
        for i, j in NEAR:
            remote(done_extra, spot_extra, extra_sems, 2, in_plane(i, j)).start()
        remote(done_extra, spot_extra, last_sems, 0, other).start()

    for n in range(len(PIECES)):
        for i, j in ARRIVAL:
            k = xs[-i % 4] * 8 + ps[-j % 8]
            spread(n, NEAR.index((i, j)), k, other).wait_recv()
            remote(chunk_of(n, k), chunk_of(n, k), last_sems, 0, other).start()

    @pl.when(me != 0)
    def _():
        remote(done_extra, spot_extra, extra_sems, 2, other).wait_recv()
        remote(spot_extra, spot_extra, last_sems, 0, other).start()

    whole = total_ref.at[pl.ds(theirs, HALF)]
    last = remote(whole, whole, last_sems, 0, other)
    last.wait_recv()

    for copy in (*swaps, *started, last):
        copy.wait_send()
    @pl.when(me != 0)
    def _():
        to_first.wait_send()

    @pl.when(me == 0)
    def _():
        remote(lines_extra, lines_extra, extra_sems, 1, other).wait_send()
        remote(all_extra, all_extra, extra_sems, 2, other).wait_send()

    for n, (at, size) in enumerate(PIECES):
        pieces = held.at[pl.ds(0, (PLANE - 1) * size)]
        pltpu.make_async_remote_copy(
            src_ref=pieces, dst_ref=pieces, send_sem=gather_sems.at[n], recv_sem=spread_sems.at[0],
            device_id=other, device_id_type=MESH,
        ).wait_send()


def gram(trial, resid, energy, shift):
    vmem = pl.BlockSpec(memory_space=pltpu.VMEM)
    hbm = pl.BlockSpec(memory_space=pl.ANY)
    return pl.pallas_call(
        gram_kernel,
        out_shape=(
            pltpu.VMEM((2 * HALF, UNIT, 128), F32),
            pltpu.VMEM((ROWS, KEEP + NEW), BF16),
            pltpu.VMEM((ROWS, KEEP + NEW), BF16),
        ),
        in_specs=[hbm] * 4,
        out_specs=(vmem, vmem, vmem),
        scratch_shapes=[
            pltpu.VMEM((ROWS, KEEP), F32),
            pltpu.VMEM((ROWS, NEW), F32),
            pltpu.VMEM((ROWS // 128, 128), F32),
            pltpu.VMEM((1, NEW), F32),
            pltpu.VMEM((2 * HALF, UNIT, 128), F32),
            pltpu.VMEM((HALF, UNIT, 128), F32),
            pltpu.VMEM(((PLANE - 1) * CHUNK, UNIT, 128), F32),
            pltpu.VMEM((CHUNK, UNIT, 128), F32),
            pltpu.VMEM((LINE * CHUNK, UNIT, 128), F32),
            pltpu.VMEM((CHUNK, UNIT, 128), F32),
            pltpu.SemaphoreType.DMA((2 + 2 * ROWS // STEP,)),
            pltpu.SemaphoreType.DMA((2 * len(PIECES),)),
            pltpu.SemaphoreType.DMA((2 * len(PIECES),)),
            pltpu.SemaphoreType.DMA((2 * len(PIECES),)),
            pltpu.SemaphoreType.DMA((len(PIECES),)),
            pltpu.SemaphoreType.DMA((PLANE * len(PIECES),)),
            pltpu.SemaphoreType.DMA((2,)),
            pltpu.VMEM((PLANE, UNIT, 128), F32),
            pltpu.VMEM((1, UNIT, 128), F32),
            pltpu.VMEM((LINE, UNIT, 128), F32),
            pltpu.VMEM((1, UNIT, 128), F32),
            pltpu.SemaphoreType.DMA((6,)),
        ],
        compiler_params=pltpu.CompilerParams(
            collective_id=0, has_side_effects=True, vmem_limit_bytes=VMEM_LIMIT
        ),
        name="gram",
    )(trial, resid, energy.reshape(ROWS // 128, 128), shift.reshape(1, NEW))


SIDE = 16


def halves(value):
    high = value.astype(BF16)
    return high, (value - high.astype(F32)).astype(BF16)


def dot(left, right):
    return jnp.dot(left, right, preferred_element_type=F32)


def mul(left, right):
    wide = dot(left[0], jnp.concatenate(right, 1))
    return wide[:, :NEW] + (wide[:, NEW:] + dot(left[1], right[0]))


def square_of(v):
    a, rest = v.astype(BF16), v
    rest = rest - a.astype(F32)
    b = rest.astype(BF16)
    c = (rest - b.astype(F32)).astype(BF16)
    return tdot(jnp.concatenate([a, a, a, b, b, c], 0), jnp.concatenate([a, b, c, a, b, a], 0))


def inverse_factor(square, lane, row):
    lane, sub = lane[:8], row[:8]
    count, own = NEW // 8, SIDE // 8
    tiles = [square[t * 8:t * 8 + 8] for t in range(count)]
    for first in range(0, count, own):
        base, window = first * 8, range(min(2 * own, count - first))
        here = (lane >= base) & (lane < base + SIDE)
        cols = [
            [jnp.broadcast_to(tiles[first + t][:, base + j:base + j + 1], (8, 128)) if t >= j // 8 else None
             for t in window]
            for j in range(SIDE)
        ]
        panel = [
            jnp.where(here, jnp.where(lane == sub + base + 8 * t, 1.0, 0.0) if t < own else 0.0, tiles[first + t])
            for t in window
        ]
        for k in range(SIDE):
            tk, sk = k // 8, k % 8
            pivot = jnp.broadcast_to(cols[k][tk][sk:sk + 1], (8, 128))
            scale = lax.rsqrt(pivot)
            if k + 1 < SIDE:
                tn, sn = (k + 1) // 8, (k + 1) % 8
                line = jnp.broadcast_to(cols[k][tn][sn:sn + 1], (8, 128))
                ratio = scale * scale
                for t in window[tn:]:
                    cols[k + 1][t] = cols[k + 1][t] - (cols[k][t] * line) * ratio
            for t in window[tk:]:
                cols[k][t] = cols[k][t] * scale
            line = jnp.broadcast_to(panel[tk][sk:sk + 1], (8, 128)) * scale
            panel[tk] = jnp.where(
                sub == sk, line, panel[tk] - jnp.where(sub > sk, cols[k][tk], 0.0) * line
            )
            for t in window[tk + 1:]:
                panel[t] = panel[t] - cols[k][t] * line
            for j in range(k + 2, SIDE):
                line = jnp.broadcast_to(cols[k][j // 8][j % 8:j % 8 + 1], (8, 128))
                for t in window[j // 8:]:
                    cols[j][t] = cols[j][t] - cols[k][t] * line
        tiles[first:first + len(window)] = panel
        if first + 2 * own < count:
            update = square_of(jnp.concatenate(panel[:own], 0))
            for t in range(first + 2 * own, count):
                tiles[t] = jnp.where(here, 0.0, tiles[t]) - update[t * 8:t * 8 + 8]
    return jnp.where(lane[:1] <= row[:, :1], jnp.concatenate(tiles, 0), 0.0)


def finish_kernel(count, total_ref, high, low, basis_ref, steady_ref, work, basis, sems):
    lane = lax.broadcasted_iota(jnp.int32, (NEW, NEW), 1)
    row = lax.broadcasted_iota(jnp.int32, (NEW, NEW), 0)
    at = {}
    for h in range(2):
        packed, *others = [
            total_ref[h * HALF + n * BLOCK:h * HALF + (n + 1) * BLOCK].reshape(128, 128) * (1.0 / count)
            for n in range(4)
        ]
        diagonal = total_ref[h * HALF + MAIN, 0:1, :] * (1.0 / count)
        turned = packed.T
        at[2 * h, 2 * h] = jnp.where(lane >= row, packed, turned)
        at[2 * h + 1, 2 * h + 1] = jnp.where(lane < row, packed, jnp.where(lane > row, turned, diagonal))
        at[2 * h, 2 * h + 1], at[h, 2], at[h, 3] = others
    metric = halves(jnp.concatenate(
        [jnp.concatenate([at[i, j] if i <= j else at[j, i].T for j in range(3)], 1) for i in range(3)], 0
    ))
    first = jnp.concatenate([at[i, 3] for i in range(3)], 0)
    second = mul(metric, halves(first))
    third = mul(metric, halves(second))
    coef = 2.0 * first - second
    image = 2.0 * second - third
    pair = halves(coef)
    known = halves(image - 2.0 * first)
    wide = tdot(pair[0], jnp.concatenate(known, 1))
    square = at[3, 3] + (wide[:, :NEW] + (wide[:, NEW:] + tdot(pair[1], known[0])))

    def on_diagonal(v):
        return jnp.sum(jnp.where(lane == row, v, 0.0), axis=0, keepdims=True)

    terms = on_diagonal(at[3, 3]) + jnp.sum(
        jnp.abs(coef) * (2.0 * jnp.abs(first) + jnp.abs(image)), axis=0, keepdims=True
    )
    inverse = inverse_factor(square, lane, row)

    both = jnp.concatenate(pair, 1)
    for r in range(0, ROWS, 256):
        rows = slice(r, r + 256)
        wide = dot(high[rows, :KEEP], both)
        inside = wide[:, :NEW] + (wide[:, NEW:] + dot(low[rows, :KEEP], pair[0]))
        block = (high[rows, KEEP:].astype(F32) - inside) + low[rows, KEEP:].astype(F32)
        work[rows, :NEW], work[rows, NEW:] = halves(block)

    steady = (terms <= 4.0 * on_diagonal(square)) & (on_diagonal(square) * on_diagonal(inverse) ** 2 <= 1000.0)
    steady_ref[0, 0] = jnp.min(jnp.where(steady, 1.0, 0.0))
    inverse = halves(inverse.T)
    stack = jnp.concatenate(
        [jnp.concatenate(inverse, 1), jnp.concatenate([inverse[0], jnp.zeros_like(inverse[0])], 1)], 0
    )
    stores = []
    for n in range(4):
        rows = pl.ds(n * (ROWS // 4), ROWS // 4)
        wide = dot(work[rows, :], stack)
        basis[rows, :] = wide[:, :NEW] + wide[:, NEW:]
        stores.append(pltpu.make_async_copy(basis.at[rows], basis_ref.at[rows], sems.at[n]))
        stores[-1].start()
    for store in stores:
        store.wait()


def finish(total, high, low, count):
    vmem = pl.BlockSpec(memory_space=pltpu.VMEM)
    return pl.pallas_call(
        lambda *refs: finish_kernel(count, *refs),
        out_shape=(jax.ShapeDtypeStruct((ROWS, NEW), F32), pltpu.SMEM((1, 1), F32)),
        in_specs=[vmem] * 3,
        out_specs=(pl.BlockSpec(memory_space=pl.ANY), pl.BlockSpec(memory_space=pltpu.SMEM)),
        scratch_shapes=[
            pltpu.VMEM((ROWS, 2 * NEW), BF16),
            pltpu.VMEM((ROWS, NEW), F32),
            pltpu.SemaphoreType.DMA((4,)),
        ],
        compiler_params=pltpu.CompilerParams(vmem_limit_bytes=VMEM_LIMIT),
        name="finish",
    )(total, high, low)


def in_blocks(x, dim, size):
    before, after = (x.shape[:dim], x.shape[dim + 1 :])
    return jnp.moveaxis(x.reshape(*before, size, -1, *after), dim, 0)


def summed_on_arrival(x, axis, dim):
    parts = in_blocks(x, dim, lax.axis_size(axis))
    arrived = lax.all_to_all(parts, axis, split_axis=0, concat_axis=0, tiled=True)
    return arrived.sum(axis=0)


def sum_by_axis(x, axes, dim):
    far, near = axes
    own = summed_on_arrival(in_blocks(x, dim, lax.axis_size(far)), near, dim + 1)
    return jnp.sum(lax.all_to_all(own, far, 0, 0, tiled=True), axis=0)


def rows_for(lines, size):
    spare = -lines.shape[0] % size
    if not spare:
        return lines
    return jnp.concatenate([lines, jnp.zeros((spare, *lines.shape[1:]), lines.dtype)])


def sent_to_all(x, axis):
    copies = jnp.broadcast_to(x, (lax.axis_size(axis), *x.shape))
    return lax.all_to_all(copies, axis, split_axis=0, concat_axis=0, tiled=True)


def laid_out(parts, dim):
    parts = jnp.moveaxis(parts, 0, dim)
    dims = parts.shape
    return parts.reshape(*dims[:dim], dims[dim] * dims[dim + 1], *dims[dim + 2 :])


def whole_of(x, axes, dim):
    far, near = axes
    first = sent_to_all(x, far)
    parts = jnp.swapaxes(sent_to_all(first, near), 0, 1)
    return laid_out(parts.reshape(-1, *x.shape), dim)


def nested_sum(x, axes):
    own = sum_by_axis(rows_for(x, lax.axis_size(axes[0]) * lax.axis_size(axes[1])), axes, 0)
    whole = whole_of(own, axes, 0)
    return whole[: len(x)].reshape(x.shape)


def fdot(left, right):
    return jnp.dot(left, right, precision=lax.Precision.HIGHEST, preferred_element_type=F32)


def explicit(trial, resid, energy, shift, count):
    def total(v):
        return nested_sum(v.reshape(-1), (("x", "core"), ("y", "z"))).reshape(v.shape)

    work = resid / (energy[:, None] - shift[None, :])
    work = lax.fori_loop(0, 2, lambda _, w: w - fdot(trial, total(fdot(trial.T, w)) / count), work)
    lower = jnp.linalg.cholesky(total(fdot(work.T, work)) / count)
    return jax.scipy.linalg.solve_triangular(lower, work.T, lower=True).T


def per_device(trial, resid, energy, shift):
    count = ROWS * 512
    total, high, low = gram(trial, resid, energy, shift)
    basis, steady = finish(total, high, low, count)
    return lax.cond(
        steady[0, 0] > 0.5, lambda: basis, lambda: explicit(trial, resid, energy, shift, count)
    )


def solution(mesh):
    split = Mesh(mesh.devices.reshape(4, 2, 8, 8), AXES)
    in_specs = (P(AXES, None), P(AXES, None), P(AXES), P())
    return jax.shard_map(
        per_device, mesh=split, in_specs=in_specs, out_specs=P(AXES, None), check_vma=False
    )
```

```python
import jax
import jax.numpy as jnp
from jax import lax
from jax.experimental import pallas as pl
from jax.experimental.pallas import tpu as pltpu
from jax.sharding import Mesh
from jax.sharding import PartitionSpec as P

MESH = pl.DeviceIdType.MESH
AXES = ("x", "core", "y", "z")
ROWS, KEEP, NEW = 1536, 384, 128
STEP = 384
VMEM_LIMIT = 24 * 2**20
UNIT = 8
BLOCK = 128 // UNIT
MAIN = 4 * BLOCK
HALF = MAIN + 1
PLANE, LINE = 32, 8
PIECES = ((0, 2),)
CHUNK = MAIN // PLANE
NEAR = [(i, j) for i in range(4) for j in range(8) if (i, j) != (0, 0)]
ARRIVAL = sorted(NEAR, key=lambda o: min(o[0], 4 - o[0]) + min(o[1], 8 - o[1]))
FAR = ARRIVAL[::-1]
F32, BF16 = jnp.float32, jnp.bfloat16


def tdot(a, b):
    return lax.dot_general(a, b, (((0,), (0,)), ((), ())), preferred_element_type=F32)


def gram_kernel(
    trial_ref, resid_ref, energy_ref, shift_ref, total_ref, hi, lo,
    trial, resid, energy, shift, part, peer, held, own, line, done,
    load_sems, core_sems, plane_sems, line_sems, gather_sems, spread_sems, last_sems,
    held_extra, own_extra, line_extra, done_extra, extra_sems,
):
    x, c = lax.axis_index("x"), lax.axis_index("core")
    y, z = lax.axis_index("y"), lax.axis_index("z")
    p = (1 - c) * y + c * z
    q = (1 - c) * z + c * y
    me = x * 8 + p
    other = {"x": x, "core": 1 - c, "y": y, "z": z}
    xs = [(x + i) % 4 for i in range(4)]
    ps = [(p + j) % 8 for j in range(8)]
    qs = [(q + j) % 8 for j in range(8)]

    def in_plane(i, j):
        return {"x": xs[i], "core": c, "y": (1 - c) * ps[j] + c * y, "z": (1 - c) * z + c * ps[j]}

    def in_line(j):
        return {"x": x, "core": c, "y": (1 - c) * y + c * qs[j], "z": (1 - c) * qs[j] + c * z}

    barrier = pltpu.get_barrier_semaphore()
    for device in [other] + [in_plane(i, j) for i, j in FAR] + [in_line(j) for j in range(1, 8)]:
        pl.semaphore_signal(barrier, inc=1, device_id=device, device_id_type=MESH)

    loads = [
        pltpu.make_async_copy(energy_ref, energy, load_sems.at[0]),
        pltpu.make_async_copy(shift_ref, shift, load_sems.at[1]),
    ]
    for b in range(ROWS // STEP):
        rows = pl.ds(b * STEP, STEP)
        loads.append(pltpu.make_async_copy(resid_ref.at[rows], resid.at[rows], load_sems.at[2 + 2 * b]))
        loads.append(pltpu.make_async_copy(trial_ref.at[rows], trial.at[rows], load_sems.at[3 + 2 * b]))
    for load in loads:
        load.start()

    for b in range(ROWS // STEP):
        for load in loads[2 * b + 2:2 * b + 4] + (loads[:2] if b == 0 else []):
            load.wait()
        for r in range(b * STEP, (b + 1) * STEP, 128):
            rows = pl.ds(r, 128)
            gap = jnp.broadcast_to(energy[pl.ds(r // 128, 1), :], (128, 128)).T - shift[...]
            for at, value in ((slice(0, KEEP), trial[rows, :]), (slice(KEEP, KEEP + NEW), resid[rows, :] / gap)):
                high = value.astype(BF16)
                hi[rows, at] = high
                lo[rows, at] = (value - high.astype(F32)).astype(BF16)

    def half(h):
        wide = pl.ds(pl.multiple_of(h * 256, 256), 256)
        thin = pl.ds(pl.multiple_of(h * 128, 128), 128)
        left = hi[:, wide]
        cross = tdot(left, lo[:, wide])
        full = tdot(left, left) + (cross + cross.T)
        left = hi[:, thin]
        side = tdot(left, hi[:, 256:]) + (tdot(left, lo[:, 256:]) + tdot(lo[:, thin], hi[:, 256:]))
        lane = lax.broadcasted_iota(jnp.int32, (128, 128), 1)
        row = lax.broadcasted_iota(jnp.int32, (128, 128), 0)
        packed = jnp.where(lane >= row, full[:128, :128], full[128:, 128:])
        diagonal = jnp.sum(jnp.where(lane == row, full[128:, 128:], 0.0), axis=0, keepdims=True)
        part[pl.ds(h * HALF + MAIN, 1)] = jnp.broadcast_to(diagonal, (UNIT, 128)).reshape(1, UNIT, 128)
        blocks = (packed, full[:128, 128:], side[:, :128], side[:, 128:])
        for n, block in enumerate(blocks):
            part[pl.ds(h * HALF + n * BLOCK, BLOCK)] = block.reshape(BLOCK, UNIT, 128)

    def remote(src, dst, sems, n, device):
        return pltpu.make_async_remote_copy(
            src_ref=src, dst_ref=dst, send_sem=sems.at[2 * n], recv_sem=sems.at[2 * n + 1],
            device_id=device, device_id_type=MESH,
        )

    mine, theirs = c * HALF, (1 - c) * HALF
    started = []
    half(1 - c)
    half(c)
    pl.semaphore_wait(barrier, PLANE + LINE - 1)
    swaps = [
        remote(
            part.at[pl.ds(theirs + at * PLANE, size * PLANE + (n == len(PIECES) - 1))], peer.at[pl.ds(at * PLANE, size * PLANE + (n == len(PIECES) - 1))],
            core_sems, n, other,
        )
        for n, (at, size) in enumerate(PIECES)
    ]
    for swap in swaps:
        swap.start()
    for n, (at, size) in enumerate(PIECES):
        swaps[n].wait_recv()
        peer[at * PLANE:(at + size) * PLANE + (n == len(PIECES) - 1)] += part[pl.ds(mine + at * PLANE, size * PLANE + (n == len(PIECES) - 1))]
        for m, (i, j) in enumerate(FAR):
            k = xs[i] * 8 + ps[j]
            remote(
                peer.at[pl.ds(at * PLANE + k * size, size)], held.at[pl.ds(at * (PLANE - 1) + m * size, size)],
                plane_sems, n, in_plane(i, j),
            ).start()

    spot_extra = total_ref.at[pl.ds(mine + MAIN, 1)]
    to_first = remote(
        peer.at[pl.ds(MAIN, 1)], held_extra.at[pl.ds((me + PLANE - 1) % PLANE, 1)], extra_sems, 0,
        {"x": 0, "core": c, "y": c * y, "z": (1 - c) * z},
    )

    @pl.when(me != 0)
    def _():
        to_first.start()

    for n, (at, size) in enumerate(PIECES):
        base = at * (PLANE - 1)
        pieces = held.at[pl.ds(base, (PLANE - 1) * size)]
        started.append(remote(pieces, pieces, plane_sems, n, other))
        started[-1].wait_recv()
        total = peer[pl.ds(at * PLANE + me * size, size)]
        for m in range(PLANE - 1):
            total += held[base + m * size:base + (m + 1) * size]
        own[at:at + size] = total
        spot = pl.ds(at * LINE + q * size, size)
        line[spot] = total
        for j in (4, 3, 5, 2, 6, 1, 7):
            remote(own.at[pl.ds(at, size)], line.at[spot], line_sems, n, in_line(j)).start()

    all_extra = held_extra.at[pl.ds(0, PLANE - 1)]
    lines_extra = line_extra.at[pl.ds(0, LINE - 1)]

    @pl.when(me == 0)
    def _():
        remote(all_extra, all_extra, extra_sems, 0, other).wait_recv()
        total = peer[MAIN:MAIN + 1]
        for m in range(PLANE - 1):
            total += held_extra[m:m + 1]
        own_extra[...] = total
        line_extra[pl.ds(q, 1)] = total
        for j in range(1, LINE):
            remote(own_extra, line_extra.at[pl.ds(q, 1)], extra_sems, 1, in_line(j)).start()

    def chunk_of(n, k):
        at, size = PIECES[n]
        return total_ref.at[pl.ds(mine + at * PLANE + k * size, size)]

    def spread(n, m, k, device):
        return pltpu.make_async_remote_copy(
            src_ref=done.at[pl.ds(*PIECES[n])], dst_ref=chunk_of(n, k),
            send_sem=gather_sems.at[n], recv_sem=spread_sems.at[n * PLANE + m],
            device_id=device, device_id_type=MESH,
        )

    for n, (at, size) in enumerate(PIECES):
        lines = line.at[pl.ds(at * LINE, (LINE - 1) * size)]
        started.append(remote(lines, lines, line_sems, n, other))
        started[-1].wait_recv()
        total = line[at * LINE:at * LINE + size]
        for j in range(1, LINE):
            total += line[at * LINE + j * size:at * LINE + (j + 1) * size]
        done[at:at + size] = total
        total_ref[pl.ds(mine + at * PLANE + me * size, size)] = total
        for m, (i, j) in enumerate(NEAR):
            spread(n, m, me, in_plane(i, j)).start()
        remote(done.at[pl.ds(at, size)], chunk_of(n, me), last_sems, 0, other).start()

    @pl.when(me == 0)
    def _():
        remote(lines_extra, lines_extra, extra_sems, 1, other).wait_recv()
        total = line_extra[0:1]
        for j in range(1, LINE):
            total += line_extra[j:j + 1]
        done_extra[...] = total
        total_ref[pl.ds(mine + MAIN, 1)] = total
        for i, j in NEAR:
            remote(done_extra, spot_extra, extra_sems, 2, in_plane(i, j)).start()
        remote(done_extra, spot_extra, last_sems, 0, other).start()

    for n in range(len(PIECES)):
        for i, j in ARRIVAL:
            k = xs[-i % 4] * 8 + ps[-j % 8]
            spread(n, NEAR.index((i, j)), k, other).wait_recv()
            remote(chunk_of(n, k), chunk_of(n, k), last_sems, 0, other).start()

    @pl.when(me != 0)
    def _():
        remote(done_extra, spot_extra, extra_sems, 2, other).wait_recv()
        remote(spot_extra, spot_extra, last_sems, 0, other).start()

    whole = total_ref.at[pl.ds(theirs, HALF)]
    last = remote(whole, whole, last_sems, 0, other)
    last.wait_recv()

    for copy in (*swaps, *started, last):
        copy.wait_send()
    @pl.when(me != 0)
    def _():
        to_first.wait_send()

    @pl.when(me == 0)
    def _():
        remote(lines_extra, lines_extra, extra_sems, 1, other).wait_send()
        remote(all_extra, all_extra, extra_sems, 2, other).wait_send()

    for n, (at, size) in enumerate(PIECES):
        pieces = held.at[pl.ds(0, (PLANE - 1) * size)]
        pltpu.make_async_remote_copy(
            src_ref=pieces, dst_ref=pieces, send_sem=gather_sems.at[n], recv_sem=spread_sems.at[0],
            device_id=other, device_id_type=MESH,
        ).wait_send()


def gram(trial, resid, energy, shift):
    vmem = pl.BlockSpec(memory_space=pltpu.VMEM)
    hbm = pl.BlockSpec(memory_space=pl.ANY)
    return pl.pallas_call(
        gram_kernel,
        out_shape=(
            pltpu.VMEM((2 * HALF, UNIT, 128), F32),
            pltpu.VMEM((ROWS, KEEP + NEW), BF16),
            pltpu.VMEM((ROWS, KEEP + NEW), BF16),
        ),
        in_specs=[hbm] * 4,
        out_specs=(vmem, vmem, vmem),
        scratch_shapes=[
            pltpu.VMEM((ROWS, KEEP), F32),
            pltpu.VMEM((ROWS, NEW), F32),
            pltpu.VMEM((ROWS // 128, 128), F32),
            pltpu.VMEM((1, NEW), F32),
            pltpu.VMEM((2 * HALF, UNIT, 128), F32),
            pltpu.VMEM((HALF, UNIT, 128), F32),
            pltpu.VMEM(((PLANE - 1) * CHUNK, UNIT, 128), F32),
            pltpu.VMEM((CHUNK, UNIT, 128), F32),
            pltpu.VMEM((LINE * CHUNK, UNIT, 128), F32),
            pltpu.VMEM((CHUNK, UNIT, 128), F32),
            pltpu.SemaphoreType.DMA((2 + 2 * ROWS // STEP,)),
            pltpu.SemaphoreType.DMA((2 * len(PIECES),)),
            pltpu.SemaphoreType.DMA((2 * len(PIECES),)),
            pltpu.SemaphoreType.DMA((2 * len(PIECES),)),
            pltpu.SemaphoreType.DMA((len(PIECES),)),
            pltpu.SemaphoreType.DMA((PLANE * len(PIECES),)),
            pltpu.SemaphoreType.DMA((2,)),
            pltpu.VMEM((PLANE, UNIT, 128), F32),
            pltpu.VMEM((1, UNIT, 128), F32),
            pltpu.VMEM((LINE, UNIT, 128), F32),
            pltpu.VMEM((1, UNIT, 128), F32),
            pltpu.SemaphoreType.DMA((6,)),
        ],
        compiler_params=pltpu.CompilerParams(
            collective_id=0, has_side_effects=True, vmem_limit_bytes=VMEM_LIMIT
        ),
        name="gram",
    )(trial, resid, energy.reshape(ROWS // 128, 128), shift.reshape(1, NEW))


SIDE = 16


def halves(value):
    high = value.astype(BF16)
    return high, (value - high.astype(F32)).astype(BF16)


def dot(left, right):
    return jnp.dot(left, right, preferred_element_type=F32)


def mul(left, right):
    wide = dot(left[0], jnp.concatenate(right, 1))
    return wide[:, :NEW] + (wide[:, NEW:] + dot(left[1], right[0]))


def square_of(v):
    a, rest = v.astype(BF16), v
    rest = rest - a.astype(F32)
    b = rest.astype(BF16)
    c = (rest - b.astype(F32)).astype(BF16)
    return tdot(jnp.concatenate([a, a, a, b, b, c], 0), jnp.concatenate([a, b, c, a, b, a], 0))


def inverse_factor(square, lane, row):
    lane, sub = lane[:8], row[:8]
    count, own = NEW // 8, SIDE // 8
    tiles = [square[t * 8:t * 8 + 8] for t in range(count)]
    for first in range(0, count, own):
        base, window = first * 8, range(min(2 * own, count - first))
        here = (lane >= base) & (lane < base + SIDE)
        cols = [
            [jnp.broadcast_to(tiles[first + t][:, base + j:base + j + 1], (8, 128)) if t >= j // 8 else None
             for t in window]
            for j in range(SIDE)
        ]
        panel = [
            jnp.where(here, jnp.where(lane == sub + base + 8 * t, 1.0, 0.0) if t < own else 0.0, tiles[first + t])
            for t in window
        ]
        for k in range(SIDE):
            tk, sk = k // 8, k % 8
            pivot = jnp.broadcast_to(cols[k][tk][sk:sk + 1], (8, 128))
            scale = lax.rsqrt(pivot)
            if k + 1 < SIDE:
                tn, sn = (k + 1) // 8, (k + 1) % 8
                line = jnp.broadcast_to(cols[k][tn][sn:sn + 1], (8, 128))
                ratio = scale * scale
                for t in window[tn:]:
                    cols[k + 1][t] = cols[k + 1][t] - (cols[k][t] * line) * ratio
            for t in window[tk:]:
                cols[k][t] = cols[k][t] * scale
            line = jnp.broadcast_to(panel[tk][sk:sk + 1], (8, 128)) * scale
            panel[tk] = jnp.where(
                sub == sk, line, panel[tk] - jnp.where(sub > sk, cols[k][tk], 0.0) * line
            )
            for t in window[tk + 1:]:
                panel[t] = panel[t] - cols[k][t] * line
            for j in range(k + 2, SIDE):
                line = jnp.broadcast_to(cols[k][j // 8][j % 8:j % 8 + 1], (8, 128))
                for t in window[j // 8:]:
                    cols[j][t] = cols[j][t] - cols[k][t] * line
        tiles[first:first + len(window)] = panel
        if first + 2 * own < count:
            update = square_of(jnp.concatenate(panel[:own], 0))
            for t in range(first + 2 * own, count):
                tiles[t] = jnp.where(here, 0.0, tiles[t]) - update[t * 8:t * 8 + 8]
    return jnp.where(lane[:1] <= row[:, :1], jnp.concatenate(tiles, 0), 0.0)


def finish_kernel(count, total_ref, high, low, basis_ref, steady_ref, work, basis, sems):
    lane = lax.broadcasted_iota(jnp.int32, (NEW, NEW), 1)
    row = lax.broadcasted_iota(jnp.int32, (NEW, NEW), 0)
    at = {}
    for h in range(2):
        packed, *others = [
            total_ref[h * HALF + n * BLOCK:h * HALF + (n + 1) * BLOCK].reshape(128, 128) * (1.0 / count)
            for n in range(4)
        ]
        diagonal = total_ref[h * HALF + MAIN, 0:1, :] * (1.0 / count)
        turned = packed.T
        at[2 * h, 2 * h] = jnp.where(lane >= row, packed, turned)
        at[2 * h + 1, 2 * h + 1] = jnp.where(lane < row, packed, jnp.where(lane > row, turned, diagonal))
        at[2 * h, 2 * h + 1], at[h, 2], at[h, 3] = others
    metric = halves(jnp.concatenate(
        [jnp.concatenate([at[i, j] if i <= j else at[j, i].T for j in range(3)], 1) for i in range(3)], 0
    ))
    first = jnp.concatenate([at[i, 3] for i in range(3)], 0)
    second = mul(metric, halves(first))
    third = mul(metric, halves(second))
    coef = 2.0 * first - second
    image = 2.0 * second - third
    pair = halves(coef)
    known = halves(image - 2.0 * first)
    wide = tdot(pair[0], jnp.concatenate(known, 1))
    square = at[3, 3] + (wide[:, :NEW] + (wide[:, NEW:] + tdot(pair[1], known[0])))

    def on_diagonal(v):
        return jnp.sum(jnp.where(lane == row, v, 0.0), axis=0, keepdims=True)

    terms = on_diagonal(at[3, 3]) + jnp.sum(
        jnp.abs(coef) * (2.0 * jnp.abs(first) + jnp.abs(image)), axis=0, keepdims=True
    )
    inverse = inverse_factor(square, lane, row)

    both = jnp.concatenate(pair, 1)
    for r in range(0, ROWS, 256):
        rows = slice(r, r + 256)
        wide = dot(high[rows, :KEEP], both)
        inside = wide[:, :NEW] + (wide[:, NEW:] + dot(low[rows, :KEEP], pair[0]))
        block = (high[rows, KEEP:].astype(F32) - inside) + low[rows, KEEP:].astype(F32)
        work[rows, :NEW], work[rows, NEW:] = halves(block)

    steady = (terms <= 4.0 * on_diagonal(square)) & (on_diagonal(square) * on_diagonal(inverse) ** 2 <= 1000.0)
    steady_ref[0, 0] = jnp.min(jnp.where(steady, 1.0, 0.0))
    inverse = halves(inverse.T)
    stack = jnp.concatenate(
        [jnp.concatenate(inverse, 1), jnp.concatenate([inverse[0], jnp.zeros_like(inverse[0])], 1)], 0
    )
    stores = []
    for n in range(4):
        rows = pl.ds(n * (ROWS // 4), ROWS // 4)
        wide = dot(work[rows, :], stack)
        basis[rows, :] = wide[:, :NEW] + wide[:, NEW:]
        stores.append(pltpu.make_async_copy(basis.at[rows], basis_ref.at[rows], sems.at[n]))
        stores[-1].start()
    for store in stores:
        store.wait()


def finish(total, high, low, count):
    vmem = pl.BlockSpec(memory_space=pltpu.VMEM)
    return pl.pallas_call(
        lambda *refs: finish_kernel(count, *refs),
        out_shape=(jax.ShapeDtypeStruct((ROWS, NEW), F32), pltpu.SMEM((1, 1), F32)),
        in_specs=[vmem] * 3,
        out_specs=(pl.BlockSpec(memory_space=pl.ANY), pl.BlockSpec(memory_space=pltpu.SMEM)),
        scratch_shapes=[
            pltpu.VMEM((ROWS, 2 * NEW), BF16),
            pltpu.VMEM((ROWS, NEW), F32),
            pltpu.SemaphoreType.DMA((4,)),
        ],
        compiler_params=pltpu.CompilerParams(vmem_limit_bytes=VMEM_LIMIT),
        name="finish",
    )(total, high, low)


def in_blocks(x, dim, size):
    before, after = (x.shape[:dim], x.shape[dim + 1 :])
    return jnp.moveaxis(x.reshape(*before, size, -1, *after), dim, 0)


def summed_on_arrival(x, axis, dim):
    parts = in_blocks(x, dim, lax.axis_size(axis))
    arrived = lax.all_to_all(parts, axis, split_axis=0, concat_axis=0, tiled=True)
    return arrived.sum(axis=0)


def sum_by_axis(x, axes, dim):
    far, near = axes
    own = summed_on_arrival(in_blocks(x, dim, lax.axis_size(far)), near, dim + 1)
    return jnp.sum(lax.all_to_all(own, far, 0, 0, tiled=True), axis=0)


def rows_for(lines, size):
    spare = -lines.shape[0] % size
    if not spare:
        return lines
    return jnp.concatenate([lines, jnp.zeros((spare, *lines.shape[1:]), lines.dtype)])


def sent_to_all(x, axis):
    copies = jnp.broadcast_to(x, (lax.axis_size(axis), *x.shape))
    return lax.all_to_all(copies, axis, split_axis=0, concat_axis=0, tiled=True)


def laid_out(parts, dim):
    parts = jnp.moveaxis(parts, 0, dim)
    dims = parts.shape
    return parts.reshape(*dims[:dim], dims[dim] * dims[dim + 1], *dims[dim + 2 :])


def whole_of(x, axes, dim):
    far, near = axes
    first = sent_to_all(x, far)
    parts = jnp.swapaxes(sent_to_all(first, near), 0, 1)
    return laid_out(parts.reshape(-1, *x.shape), dim)


def nested_sum(x, axes):
    own = sum_by_axis(rows_for(x, lax.axis_size(axes[0]) * lax.axis_size(axes[1])), axes, 0)
    whole = whole_of(own, axes, 0)
    return whole[: len(x)].reshape(x.shape)


def fdot(left, right):
    return jnp.dot(left, right, precision=lax.Precision.HIGHEST, preferred_element_type=F32)


def explicit(trial, resid, energy, shift, count):
    def total(v):
        return nested_sum(v.reshape(-1), (("x", "core"), ("y", "z"))).reshape(v.shape)

    work = resid / (energy[:, None] - shift[None, :])
    work = lax.fori_loop(0, 2, lambda _, w: w - fdot(trial, total(fdot(trial.T, w)) / count), work)
    lower = jnp.linalg.cholesky(total(fdot(work.T, work)) / count)
    return jax.scipy.linalg.solve_triangular(lower, work.T, lower=True).T


def per_device(trial, resid, energy, shift):
    count = ROWS * 512
    total, high, low = gram(trial, resid, energy, shift)
    basis, steady = finish(total, high, low, count)
    return lax.cond(
        steady[0, 0] > 0.5, lambda: basis, lambda: explicit(trial, resid, energy, shift, count)
    )


def solution(mesh):
    split = Mesh(mesh.devices.reshape(4, 2, 8, 8), AXES)
    in_specs = (P(AXES, None), P(AXES, None), P(AXES), P())
    return jax.shard_map(
        per_device, mesh=split, in_specs=in_specs, out_specs=P(AXES, None), check_vma=False
    )
```
